128 devices in a mesh: row: 8 (over x, core), col: 16 (over z, y).
Axes of the slice: x: 4, y: 4, z: 4, core: 2. Of those that a mesh axis runs over, the one named last changes fastest.
Arguments:
- matrix: float32 [8192, 8192], P('row', 'col'), as said below
- start_vectors: float32 [8192, 512], P(('col', 'row')), may hold values from -6 to 6
- interval: float32 [2], replicated, as said below
Outputs:
- ortho_basis: float32 [8192, 512], P(('col', 'row'))
- projected: float32 [512, 512], replicated
- residual: float32 [8192, 512], P(('col', 'row'))
The draws below stay inside these ranges and needn't reach their ends.
Inputs may be any that keep to these rules, and one draw needn't show every extreme that they name: matrix is exactly symmetric (entry (r, c) equals entry (c, r)); its eigenvalues lie within about -1.45 to 1.45. interval[0] lies in [-1.2, -0.7] and interval[1] in [1.45, 1.9].
All inputs are finite; a program needn't handle non-finite values.
Results may differ from the reference program's by a relative error of at most 0.0003.
Values sent between devices are 32-bit elements.
A program may use at most 128 MiB of HBM per device.

```python
import math
import jax
import jax.numpy as jnp
from jax import lax

K = 512
FILTER_DEG = 3
OUTER = 2
N = 8192


def draw_matrix(key, part):
    entries = jax.random.normal(key, (N, N), jnp.float32)
    return ((entries + entries.T) * (0.5 / math.sqrt(N))).astype(jnp.float32)


def draw_interval(key, part):
    low_key = jax.random.fold_in(key, 11)
    high_key = jax.random.fold_in(key, 23)
    low_end = jax.random.uniform(low_key, (), jnp.float32, -1.2, -0.7)
    high_end = jax.random.uniform(high_key, (), jnp.float32, 1.45, 1.9)
    return jnp.stack([low_end, high_end]).astype(jnp.float32)


def shard_levels(rng, extent, split, least, high):
    def one(axis_at, blocks):
        steps = jax.random.uniform(jax.random.fold_in(jax.random.fold_in(rng, 6), axis_at), (blocks,), jnp.float32, least / len(split), high / len(split))
        return jnp.repeat(jnp.exp(steps), extent[axis_at] // blocks).reshape((-1,) + (1,) * (len(extent) - axis_at - 1))

    gain = one(*split[0])
    for cut in split[1:]:
        gain = gain * one(*cut)
    return gain


def gaussian(rng, extent, deviation, limit, cuts=(), kind=jnp.bfloat16):
    values = jax.random.normal(rng, extent, jnp.float32) * deviation
    if len(cuts) > 0:
        values = shard_levels(rng, extent, cuts, -0.22, 0.18) * values
    return jnp.clip(values, min=-limit, max=limit).astype(kind)


def setup_inputs(seed: int = 0) -> dict:
    keys = jax.random.split(jax.random.key(seed), 4)
    matrix = draw_matrix(jax.random.fold_in(keys[3], 71), 0)
    start_vectors = gaussian(keys[1], (N, K), 1.0, 6.0, ((0, 128),), jnp.float32)
    interval = draw_interval(jax.random.fold_in(keys[3], 71), 0)
    return dict(matrix=matrix, start_vectors=start_vectors, interval=interval)


def product(left, right):
    return jnp.dot(left, right, precision=lax.Precision.HIGHEST, preferred_element_type=jnp.float32)


def tri_solve(factor, values):
    return jax.scipy.linalg.solve_triangular(factor, values, lower=True)


def reference(matrix, start_vectors, interval):
    center = 0.5 * (interval[0] + interval[1])
    half_width = 0.5 * (interval[1] - interval[0])
    total_rows = matrix.shape[0]
    positions = lax.iota(jnp.int32, total_rows)
    diagonal = positions[:, None] == positions[None, :]
    operator = jnp.where(diagonal, matrix - center, matrix) / half_width
    current_start = start_vectors
    for sweep_index in range(OUTER):
        previous = current_start
        current = product(operator, current_start)
        for degree in range(2, FILTER_DEG + 1):
            previous, current = current, 2.0 * product(operator, current) - previous
        mapped = product(operator, current)
        gram_matrix = product(current.T, current) / total_rows
        cross_terms = product(current.T, mapped) / total_rows
        factor = jnp.linalg.cholesky(gram_matrix)
        ortho_basis = tri_solve(factor, current.T).T
        partial_value = tri_solve(factor, cross_terms)
        projected = tri_solve(factor, partial_value.T).T
        current_start = ortho_basis
    residual = tri_solve(factor, mapped.T).T - product(ortho_basis, projected)
    return ortho_basis, projected, residual
```

```python
import functools

import jax
import jax.numpy as jnp
from jax import lax
from jax.experimental import pallas as pl
from jax.experimental.pallas import tpu as pltpu
from jax.sharding import PartitionSpec as P

FILTER_DEG = 3
OUTER = 2
PANEL = 8
MESH = pl.DeviceIdType.MESH
CHUNK = 128


def product(left, right, precision=lax.Precision.HIGHEST):
    return jnp.dot(left, right, precision=precision, preferred_element_type=jnp.float32)


def contract(left, right, left_dim, right_dim):
    return lax.dot_general(
        left,
        right,
        (((left_dim,), (right_dim,)), ((), ())),
        precision=lax.Precision.HIGHEST,
        preferred_element_type=jnp.float32,
    )


def factor_panel(panel, first):
    rows = panel.shape[0]
    row_at = lax.broadcasted_iota(jnp.int32, panel.shape, 0)
    pivots = jnp.ones((rows, 1), jnp.float32)
    pivot_at = lax.broadcasted_iota(jnp.int32, (rows, 1), 0)
    for step in range(rows):
        column = panel[:, first + step : first + step + 1]
        pivot = column[step : step + 1, :]
        pivots = jnp.where(pivot_at == step, pivot, pivots)
        if step < rows - 1:
            multiplier = column / pivot
            change = multiplier * panel[step : step + 1, :]
            panel = jnp.where(row_at > step, panel - change, panel)
    return panel * lax.rsqrt(pivots)


def factor_kernel(block, gram_ref, inverse_ref, work, tile):
    order = gram_ref.shape[0]
    work[...] = gram_ref[...]
    at_row = lax.broadcasted_iota(jnp.int32, (order, order), 0)
    at_col = lax.broadcasted_iota(jnp.int32, (order, order), 1)
    inverse_ref[...] = (at_row == at_col).astype(jnp.float32)
    unit = (
        lax.broadcasted_iota(jnp.int32, (block, block), 0)
        == lax.broadcasted_iota(jnp.int32, (block, block), 1)
    ).astype(jnp.float32)
    for start in range(0, order, block):
        stop = start + block
        tile[:, :block] = work[start:stop, start:stop]
        tile[:, block:] = unit
        for first in range(0, block, PANEL):
            last = first + PANEL
            done = factor_panel(tile[first:last, :], first)
            tile[first:last, :] = done
            if last < block:
                tile[last:, :] -= contract(done[:, :block], done, 0, 0)[last:, :]
        small = tile[:, block:]
        solved = product(small, inverse_ref[start:stop, :])
        inverse_ref[start:stop, :] = solved
        if stop < order:
            below = contract(work[stop:, start:stop], small, 1, 1)
            work[stop:, stop:] -= contract(below, below, 1, 1)
            inverse_ref[stop:, :] -= product(below, solved)
    inverse_ref[...] = jnp.where(at_row >= at_col, inverse_ref[...], 0.0)


def inverse_factor(gram_matrix):
    order = gram_matrix.shape[0]
    block = min(128, order)
    return pl.pallas_call(
        functools.partial(factor_kernel, block),
        out_shape=jax.ShapeDtypeStruct((order, order), jnp.float32),
        in_specs=[pl.BlockSpec(memory_space=pltpu.VMEM)],
        out_specs=pl.BlockSpec(memory_space=pltpu.VMEM),
        scratch_shapes=[
            pltpu.VMEM((order, order), jnp.float32),
            pltpu.VMEM((block, 2 * block), jnp.float32),
        ],
        cost_estimate=pl.CostEstimate(flops=2 * order**3, bytes_accessed=8 * order**2, transcendentals=order),
    )(gram_matrix)


class Copies:
    def __init__(self, send, recv):
        self.send, self.recv, self.used = send, recv, 0

    def reserve(self, count):
        first = self.used
        self.used += count
        return first

    def make(self, source, target, slot, device):
        return pltpu.make_async_remote_copy(
            src_ref=source,
            dst_ref=target,
            send_sem=self.send.at[slot],
            recv_sem=self.recv.at[slot],
            device_id=device,
            device_id_type=MESH,
        )


class Scatter:
    def __init__(self, copies, slot, place, ring, part, land):
        self.place, self.part, self.land = place, part, land
        left, right = ring
        ahead, behind, across = (place + 1) % 4, (place + 3) % 4, (place + 2) % 4
        self.ahead, self.behind = ahead, behind
        plan = (
            (part(across, 0), right),
            (part(across, 1), left),
            (part(ahead, 1), right),
            (part(behind, 0), left),
            (part(ahead, 0), right),
            (part(behind, 1), left),
        )
        self.copies = [
            copies.make(source, land(i), slot + i, device) for i, (source, device) in enumerate(plan)
        ]

    def start(self):
        for copy in self.copies[:4]:
            copy.start()

    def relay(self):
        for first, half, target in ((0, 0, self.ahead), (1, 1, self.behind)):
            self.copies[first].wait_recv()
            mine = self.part(target, half)
            mine[...] += self.land(first)[...]
            self.copies[4 + first].start()

    def finish(self):
        for copy in self.copies[2:]:
            copy.wait_recv()
        for half, terms in ((0, (3, 4)), (1, (2, 5))):
            mine = self.part(self.place, half)
            mine[...] += self.land(terms[0])[...] + self.land(terms[1])[...]
        for copy in self.copies:
            copy.wait_send()


class Gather:
    def __init__(self, copies, slot, place, ring, part):
        left, right = ring
        ahead, behind = (place + 1) % 4, (place + 3) % 4
        self.copies = [
            copies.make(part(place, None), part(place, None), slot, right),
            copies.make(part(place, None), part(place, None), slot + 1, left),
            copies.make(part(behind, 0), part(behind, 0), slot + 2, right),
            copies.make(part(ahead, 1), part(ahead, 1), slot + 3, left),
        ]

    def start(self):
        for copy in self.copies[:2]:
            copy.start()

    def forward(self):
        for first in range(2):
            self.copies[first].wait_recv()
            self.copies[2 + first].start()

    def finish(self):
        for copy in self.copies[2:]:
            copy.wait_recv()
        for copy in self.copies:
            copy.wait_send()


def split(value):
    high = value.astype(jnp.bfloat16)
    return high, (value - high.astype(jnp.float32)).astype(jnp.bfloat16)


def three_pass(left, right, dims):
    def one(a, b):
        return lax.dot_general(a, b, (dims, ((), ())), preferred_element_type=jnp.float32)

    return one(left[0], right[0]) + (one(left[0], right[1]) + one(left[1], right[0]))


def filter_kernel(
    scale_ref, block_ref, start_ref, first_ref, last_ref, image_ref,
    other, high, low, rows, row_parts, cols, col_parts, vec_high, vec_low,
    land_big, land_small, land_col, row_prev, col_prev, first_part,
    start_land, first_land, last_land, image_land, send, recv,
):
    r, c = lax.axis_index("row"), lax.axis_index("col")
    core, x, y, z = r % 2, r // 2, c % 4, c // 4
    copies = Copies(send, recv)

    def device(x, core, y, z):
        return (2 * x + core, 4 * z + y)

    mate = device(x, 1 - core, y, z)
    ring_x = device((x + 3) % 4, core, y, z), device((x + 1) % 4, core, y, z)
    ring_y = device(x, core, (y + 3) % 4, z), device(x, core, (y + 1) % 4, z)
    ring_z = device(x, core, y, (z + 3) % 4), device(x, core, y, (z + 1) % 4)
    crossed = x != z

    barrier = pltpu.get_barrier_semaphore()

    def greet(who):
        pl.semaphore_signal(barrier, inc=1, device_id=who, device_id_type=MESH)

    for who in (mate, *ring_x, *ring_y, *ring_z):
        greet(who)

    @pl.when(crossed)
    def _():
        greet(device(z, core, y, x))
        greet(device(z, 1 - core, y, x))

    pl.semaphore_wait(barrier, jnp.where(crossed, 9, 7))

    block_rows, block_cols = block_ref.shape
    slab = start_ref.shape[0]
    width = start_ref.shape[1] // 2
    mine_cols = pl.ds(pl.multiple_of(core * width, width), width)
    mate_cols = pl.ds(pl.multiple_of((1 - core) * width, width), width)

    start_copy = copies.make(start_ref.at[:, mate_cols], start_land, copies.reserve(1), mate)
    start_copy.start()
    block_copy = copies.make(block_ref, other, copies.reserve(1), mate)
    block_copy.start()

    center, inverse_width = scale_ref[0], scale_ref[1]

    def prepare(source, which):
        base = which * block_rows
        step = 256

        @pl.loop(0, block_rows // step)
        def _(i):
            at = pl.multiple_of(i * step, step)
            value = source[pl.ds(at, step), :]
            row = lax.broadcasted_iota(jnp.int32, value.shape, 0) + (2 * x * block_rows + base + at)
            col = lax.broadcasted_iota(jnp.int32, value.shape, 1) + c * block_cols
            value = jnp.where(row == col, value - center, value) * inverse_width
            big, small = split(value)
            to = pl.ds(pl.multiple_of(base + at, step), step)
            high[to, :] = big
            low[to, :] = small

    prepare(block_ref, core)

    start_copy.wait_recv()
    half = width // 2
    own = start_ref[:, mine_cols]
    theirs = start_land[...]
    lower = jnp.where(core == 0, own, theirs)
    upper = jnp.where(core == 0, theirs, own)
    piece = jnp.concatenate([lower, upper], axis=0).T
    cols[x] = piece
    col_prev[...] = piece
    row_prev[...] = jnp.zeros_like(row_prev)
    start_copy.wait_send()

    def col_slice(ref):
        def part(t, side):
            if side is None:
                return ref.at[t]
            return ref.at[t, pl.ds(side * half, half), :]
        return part

    def plane_slice(ref, colour, axis):
        def part(t, side):
            size = half if side is None else half // 2
            at = pl.ds(colour * half + (0 if side is None else side * size), size)
            return ref.at[:, t, at, :] if axis == "z" else ref.at[t, :, at, :]
        return part

    def line_slice(ref, colour, axis):
        def part(t, side):
            size = half if side is None else half // 2
            at = pl.ds(colour * half + (0 if side is None else side * size), size)
            return ref.at[y, t, at, :] if axis == "z" else ref.at[t, z, at, :]
        return part

    places = {"y": y, "z": z}
    rings = {"y": ring_y, "z": ring_z}
    orders = (("z", "y"), ("y", "z"))

    scatter_slots = [[copies.reserve(6) for _ in range(2)] for _ in range(2)]
    gather_slots = [[copies.reserve(4) for _ in range(2)] for _ in range(2)]
    col_slots = copies.reserve(6), copies.reserve(4)

    def scatter_stage(colour, stage):
        axis = orders[colour][stage]
        ref_slice = (plane_slice if stage == 0 else line_slice)(row_parts, colour, axis)
        land = (lambda i: land_big.at[colour, i]) if stage == 0 else (lambda i: land_small.at[colour, i])
        return Scatter(copies, scatter_slots[colour][stage], places[axis], rings[axis], ref_slice, land)

    def gather_stage(colour, stage):
        axis = orders[colour][1 - stage]
        ref_slice = (line_slice if stage == 0 else plane_slice)(rows, colour, axis)
        return Gather(copies, gather_slots[colour][stage], places[axis], rings[axis], ref_slice)

    col_gather = Gather(copies, col_slots[1], x, ring_x, col_slice(cols))
    col_scatter = Scatter(copies, col_slots[0], x, ring_x, col_slice(col_parts), lambda i: land_col.at[i])

    col_gather.start()
    col_gather.forward()
    col_gather.finish()

    block_copy.wait_recv()
    prepare(other, 1 - core)
    block_copy.wait_send()

    def to_rows():
        for q in range(4):
            big, small = split(cols[q])
            vec_high[:, q * CHUNK : (q + 1) * CHUNK] = big
            vec_low[:, q * CHUNK : (q + 1) * CHUNK] = small

        @pl.loop(0, 8)
        def _(i):
            at = pl.ds(pl.multiple_of(i * 256, 256), 256)
            out = three_pass((vec_high[...], vec_low[...]), (high[at, :], low[at, :]), ((1,), (1,)))
            row_parts[i // 2, 2 * (i % 2)] = out[:, :CHUNK]
            row_parts[i // 2, 2 * (i % 2) + 1] = out[:, CHUNK:]

        stages = [scatter_stage(0, 0), scatter_stage(1, 0)]
        for stage in stages:
            stage.start()
        for stage in stages:
            stage.relay()
        seconds = [scatter_stage(0, 1), scatter_stage(1, 1)]
        for stage, second in zip(stages, seconds):
            stage.finish()
            second.start()
        for second in seconds:
            second.relay()
        return seconds

    def sweep(step, carry):
        factor = jnp.where(step == 0, 1.0, 2.0)
        weight = jnp.where(step == 0, 0.0, 1.0)
        seconds = to_rows()
        gathers = []
        for colour, second in enumerate(seconds):
            second.finish()
            at = pl.ds(colour * half, half)
            value = factor * row_parts[y, z, at, :] - weight * row_prev[at, :]
            rows[y, z, at, :] = value
            row_prev[at, :] = value
            first = gather_stage(colour, 0)
            first.start()
            gathers.append(first)

        @pl.when(step == 1)
        def _():
            first_part[...] = row_prev[...]

        for first in gathers:
            first.forward()
        lasts = []
        for colour, first in enumerate(gathers):
            first.finish()
            last = gather_stage(colour, 1)
            last.start()
            lasts.append(last)
        for last in lasts:
            last.forward()
        for last in lasts:
            last.finish()

        for q in range(4):
            col_parts[q] = jnp.zeros((width, CHUNK), jnp.float32)

        @pl.loop(0, 8)
        def _(i):
            at = pl.ds(pl.multiple_of(i * 256, 256), 256)
            vec = jnp.concatenate([rows[i // 2, 2 * (i % 2)], rows[i // 2, 2 * (i % 2) + 1]], axis=1)
            out = three_pass(split(vec), (high[at, :], low[at, :]), ((1,), (0,)))
            for q in range(4):
                col_parts[q] += out[:, q * CHUNK : (q + 1) * CHUNK]

        col_scatter.start()
        col_scatter.relay()
        col_scatter.finish()
        again = jnp.where(step == 1, 1.0, 2.0)
        minus = jnp.where(step == 1, 0.0, 1.0)
        value = again * col_parts[x] - minus * col_prev[...]
        cols[x] = value
        col_prev[...] = value
        col_gather.start()
        col_gather.forward()
        col_gather.finish()
        return carry

    lax.fori_loop(0, 3, sweep, 0)
    for second in to_rows():
        second.finish()

    def trade(piece, land, out_ref):
        turned = piece.T
        land[1] = turned
        copy = copies.make(
            land.at[1, pl.ds(pl.multiple_of((1 - core) * slab, slab), slab), :],
            land.at[0, pl.ds(pl.multiple_of((1 - core) * slab, slab), slab), :],
            copies.reserve(1),
            mate,
        )
        copy.start()
        return copy

    first_copy = trade(first_part[...], first_land, first_ref)
    last_copy = trade(col_prev[...], last_land, last_ref)

    image_land[2, :, :] = row_parts[y, z].T
    image_slots = copies.reserve(2)

    same = copies.make(
        image_land.at[2, pl.ds(pl.multiple_of(core * slab, slab), slab), :],
        image_land.at[0, pl.ds(0, slab), :],
        image_slots,
        device(z, core, y, x),
    )
    cross = copies.make(
        image_land.at[2, pl.ds(pl.multiple_of((1 - core) * slab, slab), slab), :],
        image_land.at[1, pl.ds(0, slab), :],
        image_slots + 1,
        device(z, 1 - core, y, x),
    )
    cross.start()

    @pl.when(crossed)
    def _():
        same.start()
        same.wait()

    @pl.when(jnp.logical_not(crossed))
    def _():
        image_land[0, pl.ds(0, slab), :] = image_land[2, pl.ds(pl.multiple_of(core * slab, slab), slab), :]

    keep = pl.ds(pl.multiple_of(core * slab, slab), slab)
    for copy, land, out_ref in ((first_copy, first_land, first_ref), (last_copy, last_land, last_ref)):
        copy.wait()
        out_ref[:, mine_cols] = land[1, keep, :]
        out_ref[:, mate_cols] = land[0, keep, :]
    cross.wait()
    image_ref[:, mine_cols] = image_land[0, pl.ds(0, slab), :]
    image_ref[:, mate_cols] = image_land[1, pl.ds(0, slab), :]


def filtered_blocks(matrix, start_vectors, scale):
    block_rows, block_cols = matrix.shape
    slab, vectors = start_vectors.shape
    width = vectors // 2
    half = width // 2
    f32, bf16 = jnp.float32, jnp.bfloat16
    vmem = pl.BlockSpec(memory_space=pltpu.VMEM)
    return pl.pallas_call(
        filter_kernel,
        out_shape=[jax.ShapeDtypeStruct((slab, vectors), f32)] * 3,
        in_specs=[pl.BlockSpec(memory_space=pltpu.SMEM), vmem, vmem],
        out_specs=[vmem] * 3,
        scratch_shapes=[
            pltpu.VMEM((block_rows, block_cols), f32),
            pltpu.VMEM((2 * block_rows, block_cols), bf16),
            pltpu.VMEM((2 * block_rows, block_cols), bf16),
            pltpu.VMEM((4, 4, width, CHUNK), f32),
            pltpu.VMEM((4, 4, width, CHUNK), f32),
            pltpu.VMEM((4, width, CHUNK), f32),
            pltpu.VMEM((4, width, CHUNK), f32),
            pltpu.VMEM((width, block_cols), bf16),
            pltpu.VMEM((width, block_cols), bf16),
            pltpu.VMEM((2, 6, 4, half // 2, CHUNK), f32),
            pltpu.VMEM((2, 6, half // 2, CHUNK), f32),
            pltpu.VMEM((6, half, CHUNK), f32),
            pltpu.VMEM((width, CHUNK), f32),
            pltpu.VMEM((width, CHUNK), f32),
            pltpu.VMEM((width, CHUNK), f32),
            pltpu.VMEM((slab, width), f32),
            pltpu.VMEM((2, CHUNK, width), f32),
            pltpu.VMEM((2, CHUNK, width), f32),
            pltpu.VMEM((3, CHUNK, width), f32),
            pltpu.SemaphoreType.DMA((64,)),
            pltpu.SemaphoreType.DMA((64,)),
        ],
        compiler_params=pltpu.CompilerParams(
            collective_id=0, has_side_effects=True, vmem_limit_bytes=40 * 2**20
        ),
        cost_estimate=pl.CostEstimate(flops=10**10, bytes_accessed=4 * 10**6, transcendentals=0),
    )(scale, matrix, start_vectors)


def on_device(matrix, start_vectors, interval):
    slab_rows, vectors = start_vectors.shape
    total_rows = slab_rows * lax.axis_size("row") * lax.axis_size("col")
    center = 0.5 * (interval[0] + interval[1])
    half_width = 0.5 * (interval[1] - interval[0])
    scale = jnp.stack([center, 1.0 / half_width])
    early, slab, mapped = filtered_blocks(matrix, start_vectors, scale)

    gram = lax.psum(contract(early, early, 0, 0), ("row", "col")) / total_rows
    before = inverse_factor(gram)
    slab = contract(slab, before, 1, 1)
    mapped = contract(mapped, before, 1, 1)
    pair = jnp.concatenate([slab, mapped], axis=1)
    sums = lax.psum(contract(slab, pair, 0, 0), ("row", "col")) / total_rows
    gram, cross = sums[:, :vectors], sums[:, vectors:]
    inverse = inverse_factor(gram)
    basis = contract(slab, inverse, 1, 1)
    projected = contract(product(inverse, cross), inverse, 1, 1)
    residual = contract(mapped, inverse, 1, 1) - product(basis, projected)
    return basis, projected, residual


def solution(mesh):
    return jax.shard_map(
        on_device,
        mesh=mesh,
        in_specs=(P("row", "col"), P(("col", "row"), None), P()),
        out_specs=(P(("col", "row"), None), P(), P(("col", "row"), None)),
        check_vma=False,
    )
```

```python
import functools

import jax
import jax.numpy as jnp
from jax import lax
from jax.experimental import pallas as pl
from jax.experimental.pallas import tpu as pltpu
from jax.sharding import PartitionSpec as P

FILTER_DEG = 3
OUTER = 2
PANEL = 8
MESH = pl.DeviceIdType.MESH
CHUNK = 128


def product(left, right, precision=lax.Precision.HIGHEST):
    return jnp.dot(left, right, precision=precision, preferred_element_type=jnp.float32)


def contract(left, right, left_dim, right_dim):
    return lax.dot_general(
        left,
        right,
        (((left_dim,), (right_dim,)), ((), ())),
        precision=lax.Precision.HIGHEST,
        preferred_element_type=jnp.float32,
    )


def factor_panel(panel, first):
    rows = panel.shape[0]
    row_at = lax.broadcasted_iota(jnp.int32, panel.shape, 0)
    pivots = jnp.ones((rows, 1), jnp.float32)
    pivot_at = lax.broadcasted_iota(jnp.int32, (rows, 1), 0)
    for step in range(rows):
        column = panel[:, first + step : first + step + 1]
        pivot = column[step : step + 1, :]
        pivots = jnp.where(pivot_at == step, pivot, pivots)
        if step < rows - 1:
            multiplier = column / pivot
            change = multiplier * panel[step : step + 1, :]
            panel = jnp.where(row_at > step, panel - change, panel)
    return panel * lax.rsqrt(pivots)


def factor_kernel(block, gram_ref, inverse_ref, work, tile):
    order = gram_ref.shape[0]
    work[...] = gram_ref[...]
    at_row = lax.broadcasted_iota(jnp.int32, (order, order), 0)
    at_col = lax.broadcasted_iota(jnp.int32, (order, order), 1)
    inverse_ref[...] = (at_row == at_col).astype(jnp.float32)
    unit = (
        lax.broadcasted_iota(jnp.int32, (block, block), 0)
        == lax.broadcasted_iota(jnp.int32, (block, block), 1)
    ).astype(jnp.float32)
    for start in range(0, order, block):
        stop = start + block
        tile[:, :block] = work[start:stop, start:stop]
        tile[:, block:] = unit
        for first in range(0, block, PANEL):
            last = first + PANEL
            done = factor_panel(tile[first:last, :], first)
            tile[first:last, :] = done
            if last < block:
                tile[last:, :] -= contract(done[:, :block], done, 0, 0)[last:, :]
        small = tile[:, block:]
        solved = product(small, inverse_ref[start:stop, :])
        inverse_ref[start:stop, :] = solved
        if stop < order:
            below = contract(work[stop:, start:stop], small, 1, 1)
            work[stop:, stop:] -= contract(below, below, 1, 1)
            inverse_ref[stop:, :] -= product(below, solved)
    inverse_ref[...] = jnp.where(at_row >= at_col, inverse_ref[...], 0.0)


class Copies:
    def __init__(self, send, recv):
        self.send, self.recv, self.used = send, recv, 0

    def reserve(self, count):
        first = self.used
        self.used += count
        return first

    def make(self, source, target, slot, device):
        return pltpu.make_async_remote_copy(
            src_ref=source,
            dst_ref=target,
            send_sem=self.send.at[slot],
            recv_sem=self.recv.at[slot],
            device_id=device,
            device_id_type=MESH,
        )


class Scatter:
    def __init__(self, copies, slot, place, ring, part, land):
        self.place, self.part, self.land = place, part, land
        left, right = ring
        ahead, behind, across = (place + 1) % 4, (place + 3) % 4, (place + 2) % 4
        self.ahead, self.behind = ahead, behind
        plan = (
            (part(across, 0), right),
            (part(across, 1), left),
            (part(ahead, 1), right),
            (part(behind, 0), left),
            (part(ahead, 0), right),
            (part(behind, 1), left),
        )
        self.copies = [
            copies.make(source, land(i), slot + i, device) for i, (source, device) in enumerate(plan)
        ]

    def start(self):
        for copy in self.copies[:4]:
            copy.start()

    def relay(self):
        for first, half, target in ((0, 0, self.ahead), (1, 1, self.behind)):
            self.copies[first].wait_recv()
            mine = self.part(target, half)
            mine[...] += self.land(first)[...]
            self.copies[4 + first].start()

    def finish(self):
        for copy in self.copies[2:]:
            copy.wait_recv()
        for half, terms in ((0, (3, 4)), (1, (2, 5))):
            mine = self.part(self.place, half)
            mine[...] += self.land(terms[0])[...] + self.land(terms[1])[...]
        for copy in self.copies:
            copy.wait_send()


class Gather:
    def __init__(self, copies, slot, place, ring, part):
        left, right = ring
        ahead, behind = (place + 1) % 4, (place + 3) % 4
        self.copies = [
            copies.make(part(place, None), part(place, None), slot, right),
            copies.make(part(place, None), part(place, None), slot + 1, left),
            copies.make(part(behind, 0), part(behind, 0), slot + 2, right),
            copies.make(part(ahead, 1), part(ahead, 1), slot + 3, left),
        ]

    def start(self):
        for copy in self.copies[:2]:
            copy.start()

    def forward(self):
        for first in range(2):
            self.copies[first].wait_recv()
            self.copies[2 + first].start()

    def finish(self):
        for copy in self.copies[2:]:
            copy.wait_recv()
        for copy in self.copies:
            copy.wait_send()


def split(value):
    high = value.astype(jnp.bfloat16)
    return high, (value - high.astype(jnp.float32)).astype(jnp.bfloat16)


def three_pass(left, right, dims):
    def one(a, b):
        return lax.dot_general(a, b, (dims, ((), ())), preferred_element_type=jnp.float32)

    return one(left[0], right[0]) + (one(left[0], right[1]) + one(left[1], right[0]))


def filter_kernel(
    scale_ref, block_ref, start_ref, first_ref, last_ref, image_ref,
    other, high, low, rows, row_parts, cols, col_parts, vec_high, vec_low,
    land_big, land_small, land_col, row_prev, col_prev, first_part,
    start_land, first_land, last_land, image_land, send, recv,
):
    r, c = lax.axis_index("row"), lax.axis_index("col")
    core, x, y, z = r % 2, r // 2, c % 4, c // 4
    copies = Copies(send, recv)

    def device(x, core, y, z):
        return (2 * x + core, 4 * z + y)

    mate = device(x, 1 - core, y, z)
    ring_x = device((x + 3) % 4, core, y, z), device((x + 1) % 4, core, y, z)
    ring_y = device(x, core, (y + 3) % 4, z), device(x, core, (y + 1) % 4, z)
    ring_z = device(x, core, y, (z + 3) % 4), device(x, core, y, (z + 1) % 4)
    crossed = x != z

    barrier = pltpu.get_barrier_semaphore()

    def greet(who):
        pl.semaphore_signal(barrier, inc=1, device_id=who, device_id_type=MESH)

    for who in (mate, *ring_x, *ring_y, *ring_z):
        greet(who)

    @pl.when(crossed)
    def _():
        greet(device(z, core, y, x))
        greet(device(z, 1 - core, y, x))

    pl.semaphore_wait(barrier, jnp.where(crossed, 9, 7))

    block_rows, block_cols = block_ref.shape
    slab = start_ref.shape[0]
    width = start_ref.shape[1] // 2
    mine_cols = pl.ds(pl.multiple_of(core * width, width), width)
    mate_cols = pl.ds(pl.multiple_of((1 - core) * width, width), width)

    start_copy = copies.make(start_ref.at[:, mate_cols], start_land, copies.reserve(1), mate)
    start_copy.start()
    block_copy = copies.make(block_ref, other, copies.reserve(1), mate)
    block_copy.start()

    center, inverse_width = scale_ref[0], scale_ref[1]

    def prepare(source, which):
        base = which * block_rows
        step = 256

        @pl.loop(0, block_rows // step)
        def _(i):
            at = pl.multiple_of(i * step, step)
            value = source[pl.ds(at, step), :]
            row = lax.broadcasted_iota(jnp.int32, value.shape, 0) + (2 * x * block_rows + base + at)
            col = lax.broadcasted_iota(jnp.int32, value.shape, 1) + c * block_cols
            value = jnp.where(row == col, value - center, value) * inverse_width
            big, small = split(value)
            to = pl.ds(pl.multiple_of(base + at, step), step)
            high[to, :] = big
            low[to, :] = small

    prepare(block_ref, core)

    start_copy.wait_recv()
    half = width // 2
    own = start_ref[:, mine_cols]
    theirs = start_land[...]
    lower = jnp.where(core == 0, own, theirs)
    upper = jnp.where(core == 0, theirs, own)
    piece = jnp.concatenate([lower, upper], axis=0).T
    cols[x] = piece
    col_prev[...] = piece
    row_prev[...] = jnp.zeros_like(row_prev)
    start_copy.wait_send()

    def col_slice(ref):
        def part(t, side):
            if side is None:
                return ref.at[t]
            return ref.at[t, pl.ds(side * half, half), :]
        return part

    def plane_slice(ref, colour, axis):
        def part(t, side):
            size = half if side is None else half // 2
            at = pl.ds(colour * half + (0 if side is None else side * size), size)
            return ref.at[:, t, at, :] if axis == "z" else ref.at[t, :, at, :]
        return part

    def line_slice(ref, colour, axis):
        def part(t, side):
            size = half if side is None else half // 2
            at = pl.ds(colour * half + (0 if side is None else side * size), size)
            return ref.at[y, t, at, :] if axis == "z" else ref.at[t, z, at, :]
        return part

    places = {"y": y, "z": z}
    rings = {"y": ring_y, "z": ring_z}
    orders = (("z", "y"), ("y", "z"))

    scatter_slots = [[copies.reserve(6) for _ in range(2)] for _ in range(2)]
    gather_slots = [[copies.reserve(4) for _ in range(2)] for _ in range(2)]
    col_slots = copies.reserve(6), copies.reserve(4)

    def scatter_stage(colour, stage):
        axis = orders[colour][stage]
        ref_slice = (plane_slice if stage == 0 else line_slice)(row_parts, colour, axis)
        land = (lambda i: land_big.at[colour, i]) if stage == 0 else (lambda i: land_small.at[colour, i])
        return Scatter(copies, scatter_slots[colour][stage], places[axis], rings[axis], ref_slice, land)

    def gather_stage(colour, stage):
        axis = orders[colour][1 - stage]
        ref_slice = (line_slice if stage == 0 else plane_slice)(rows, colour, axis)
        return Gather(copies, gather_slots[colour][stage], places[axis], rings[axis], ref_slice)

    col_gather = Gather(copies, col_slots[1], x, ring_x, col_slice(cols))
    col_scatter = Scatter(copies, col_slots[0], x, ring_x, col_slice(col_parts), lambda i: land_col.at[i])

    col_gather.start()
    col_gather.forward()
    col_gather.finish()

    block_copy.wait_recv()
    prepare(other, 1 - core)
    block_copy.wait_send()

    def to_rows():
        for q in range(4):
            big, small = split(cols[q])
            vec_high[:, q * CHUNK : (q + 1) * CHUNK] = big
            vec_low[:, q * CHUNK : (q + 1) * CHUNK] = small

        @pl.loop(0, 8)
        def _(i):
            at = pl.ds(pl.multiple_of(i * 256, 256), 256)
            out = three_pass((vec_high[...], vec_low[...]), (high[at, :], low[at, :]), ((1,), (1,)))
            row_parts[i // 2, 2 * (i % 2)] = out[:, :CHUNK]
            row_parts[i // 2, 2 * (i % 2) + 1] = out[:, CHUNK:]

        stages = [scatter_stage(0, 0), scatter_stage(1, 0)]
        for stage in stages:
            stage.start()
        for stage in stages:
            stage.relay()
        seconds = [scatter_stage(0, 1), scatter_stage(1, 1)]
        for stage, second in zip(stages, seconds):
            stage.finish()
            second.start()
        for second in seconds:
            second.relay()
        return seconds

    def sweep(step, carry):
        factor = jnp.where(step == 0, 1.0, 2.0)
        weight = jnp.where(step == 0, 0.0, 1.0)
        seconds = to_rows()
        gathers = []
        for colour, second in enumerate(seconds):
            second.finish()
            at = pl.ds(colour * half, half)
            value = factor * row_parts[y, z, at, :] - weight * row_prev[at, :]
            rows[y, z, at, :] = value
            row_prev[at, :] = value
            first = gather_stage(colour, 0)
            first.start()
            gathers.append(first)

        @pl.when(step == 1)
        def _():
            first_part[...] = row_prev[...]

        for first in gathers:
            first.forward()
        lasts = []
        for colour, first in enumerate(gathers):
            first.finish()
            last = gather_stage(colour, 1)
            last.start()
            lasts.append(last)
        for last in lasts:
            last.forward()
        for last in lasts:
            last.finish()

        for q in range(4):
            col_parts[q] = jnp.zeros((width, CHUNK), jnp.float32)

        @pl.loop(0, 8)
        def _(i):
            at = pl.ds(pl.multiple_of(i * 256, 256), 256)
            vec = jnp.concatenate([rows[i // 2, 2 * (i % 2)], rows[i // 2, 2 * (i % 2) + 1]], axis=1)
            out = three_pass(split(vec), (high[at, :], low[at, :]), ((1,), (0,)))
            for q in range(4):
                col_parts[q] += out[:, q * CHUNK : (q + 1) * CHUNK]

        col_scatter.start()
        col_scatter.relay()
        col_scatter.finish()
        again = jnp.where(step == 1, 1.0, 2.0)
        minus = jnp.where(step == 1, 0.0, 1.0)
        value = again * col_parts[x] - minus * col_prev[...]
        cols[x] = value
        col_prev[...] = value
        col_gather.start()
        col_gather.forward()
        col_gather.finish()
        return carry

    lax.fori_loop(0, 3, sweep, 0)
    for second in to_rows():
        second.finish()

    def trade(piece, land, out_ref):
        turned = piece.T
        land[1] = turned
        copy = copies.make(
            land.at[1, pl.ds(pl.multiple_of((1 - core) * slab, slab), slab), :],
            land.at[0, pl.ds(pl.multiple_of((1 - core) * slab, slab), slab), :],
            copies.reserve(1),
            mate,
        )
        copy.start()
        return copy

    first_copy = trade(first_part[...], first_land, first_ref)
    last_copy = trade(col_prev[...], last_land, last_ref)

    image_land[2, :, :] = row_parts[y, z].T
    image_slots = copies.reserve(2)

    same = copies.make(
        image_land.at[2, pl.ds(pl.multiple_of(core * slab, slab), slab), :],
        image_land.at[0, pl.ds(0, slab), :],
        image_slots,
        device(z, core, y, x),
    )
    cross = copies.make(
        image_land.at[2, pl.ds(pl.multiple_of((1 - core) * slab, slab), slab), :],
        image_land.at[1, pl.ds(0, slab), :],
        image_slots + 1,
        device(z, 1 - core, y, x),
    )
    cross.start()

    @pl.when(crossed)
    def _():
        same.start()
        same.wait()

    @pl.when(jnp.logical_not(crossed))
    def _():
        image_land[0, pl.ds(0, slab), :] = image_land[2, pl.ds(pl.multiple_of(core * slab, slab), slab), :]

    keep = pl.ds(pl.multiple_of(core * slab, slab), slab)
    for copy, land, out_ref in ((first_copy, first_land, first_ref), (last_copy, last_land, last_ref)):
        copy.wait()
        out_ref[:, mine_cols] = land[1, keep, :]
        out_ref[:, mate_cols] = land[0, keep, :]
    cross.wait()
    image_ref[:, mine_cols] = image_land[0, pl.ds(0, slab), :]
    image_ref[:, mate_cols] = image_land[1, pl.ds(0, slab), :]


def filtered_blocks(matrix, start_vectors, scale):
    block_rows, block_cols = matrix.shape
    slab, vectors = start_vectors.shape
    width = vectors // 2
    half = width // 2
    f32, bf16 = jnp.float32, jnp.bfloat16
    vmem = pl.BlockSpec(memory_space=pltpu.VMEM)
    return pl.pallas_call(
        filter_kernel,
        out_shape=[jax.ShapeDtypeStruct((slab, vectors), f32)] * 3,
        in_specs=[pl.BlockSpec(memory_space=pltpu.SMEM), vmem, vmem],
        out_specs=[vmem] * 3,
        scratch_shapes=[
            pltpu.VMEM((block_rows, block_cols), f32),
            pltpu.VMEM((2 * block_rows, block_cols), bf16),
            pltpu.VMEM((2 * block_rows, block_cols), bf16),
            pltpu.VMEM((4, 4, width, CHUNK), f32),
            pltpu.VMEM((4, 4, width, CHUNK), f32),
            pltpu.VMEM((4, width, CHUNK), f32),
            pltpu.VMEM((4, width, CHUNK), f32),
            pltpu.VMEM((width, block_cols), bf16),
            pltpu.VMEM((width, block_cols), bf16),
            pltpu.VMEM((2, 6, 4, half // 2, CHUNK), f32),
            pltpu.VMEM((2, 6, half // 2, CHUNK), f32),
            pltpu.VMEM((6, half, CHUNK), f32),
            pltpu.VMEM((width, CHUNK), f32),
            pltpu.VMEM((width, CHUNK), f32),
            pltpu.VMEM((width, CHUNK), f32),
            pltpu.VMEM((slab, width), f32),
            pltpu.VMEM((2, CHUNK, width), f32),
            pltpu.VMEM((2, CHUNK, width), f32),
            pltpu.VMEM((3, CHUNK, width), f32),
            pltpu.SemaphoreType.DMA((64,)),
            pltpu.SemaphoreType.DMA((64,)),
        ],
        compiler_params=pltpu.CompilerParams(
            collective_id=0, has_side_effects=True, vmem_limit_bytes=40 * 2**20
        ),
        cost_estimate=pl.CostEstimate(flops=10**10, bytes_accessed=4 * 10**6, transcendentals=0),
    )(scale, matrix, start_vectors)


class Places:
    def __init__(self):
        self.r, self.c = lax.axis_index("row"), lax.axis_index("col")
        self.core, self.x = self.r % 2, self.r // 2
        self.y, self.z = self.c % 4, self.c // 4
        self.mate = (2 * self.x + 1 - self.core, self.c)
        self.ring_x = ((self.r + 6) % 8, self.c), ((self.r + 2) % 8, self.c)

    def peer(self, offset):
        return self.r, (self.c + offset) % 16


def all_sum(copies, at, total, result, land_core, land_x, land_plane):
    order, width = total.shape
    half, quarter = order // 2, order // 8

    def rows(first, count, ref=total):
        return ref.at[pl.ds(pl.multiple_of(first, 8), count), :]

    mine, theirs = rows(at.core * half, half), rows((1 - at.core) * half, half)
    swap = copies.make(theirs, land_core, copies.reserve(1), at.mate)
    swap.start()
    swap.wait_recv()
    mine[...] += land_core[...]

    def part(t, side, ref=total):
        size = quarter if side is None else quarter // 2
        return rows(at.core * half + t * quarter + (0 if side is None else side * size), size, ref)

    scatter = Scatter(copies, copies.reserve(6), at.x, at.ring_x, part, lambda i: land_x.at[i])
    scatter.start()
    scatter.relay()
    scatter.finish()

    def piece(t, ref=total):
        first = at.core * half + at.x * quarter + 8 * (t // 2)
        lanes = pl.ds(pl.multiple_of((t % 2) * (width // 2), 128), width // 2)
        return ref.at[pl.ds(pl.multiple_of(first, 8), 8), lanes]

    slots = copies.reserve(15), copies.reserve(15)
    sent = []
    for offset in range(1, 16):
        to = (at.c + offset) % 16
        copy = copies.make(piece(to), land_plane.at[offset], slots[0] + offset - 1, at.peer(offset))
        copy.start()
        sent.append(copy)
    own = piece(at.c)
    value = own[...]
    for offset, copy in enumerate(sent, 1):
        copy.wait_recv()
        value = value + land_plane[offset]
    own = piece(at.c, result)
    own[...] = value
    back = []
    for offset in range(1, 16):
        copy = copies.make(own, own, slots[1] + offset - 1, at.peer(offset))
        copy.start()
        back.append(copy)
    for copy in back:
        copy.wait_recv()
    gather = Gather(copies, copies.reserve(4), at.x, at.ring_x, lambda t, side: part(t, side, result))
    gather.start()
    gather.forward()
    gather.finish()
    mine = rows(at.core * half, half, result)
    give = copies.make(mine, mine, copies.reserve(1), at.mate)
    give.start()
    for copy in (swap, *sent, *back):
        copy.wait_send()
    give.wait()


def greet_all(at):
    barrier = pltpu.get_barrier_semaphore()
    others = [at.mate, *at.ring_x] + [at.peer(offset) for offset in range(1, 16)]
    for who in others:
        pl.semaphore_signal(barrier, inc=1, device_id=who, device_id_type=MESH)
    pl.semaphore_wait(barrier, len(others))


def sum_scratch(order, width):
    f32 = jnp.float32
    return [
        pltpu.VMEM((order, width), f32),
        pltpu.VMEM((order, width), f32),
        pltpu.VMEM((order // 2, width), f32),
        pltpu.VMEM((6, order // 16, width), f32),
        pltpu.VMEM((16, 8, width // 2), f32),
        pltpu.VMEM((order, order), f32),
        pltpu.VMEM((128, 256), f32),
        pltpu.SemaphoreType.DMA((64,)),
        pltpu.SemaphoreType.DMA((64,)),
    ]


def early_kernel(count, slab_ref, inverse_ref, total, result, land_core, land_x, land_plane, work, tile, send, recv):
    at = Places()
    greet_all(at)
    slab = slab_ref[...]
    total[...] = contract(slab, slab, 0, 0)
    all_sum(Copies(send, recv), at, total, result, land_core, land_x, land_plane)
    result[...] = result[...] / count
    factor_kernel(128, result, inverse_ref, work, tile)


def late_kernel(
    count, slab_ref, image_ref, before_ref, basis_ref, projected_ref, residual_ref,
    inverse_ref, total, result, land_core, land_x, land_plane, work, tile, send, recv,
):
    at = Places()
    greet_all(at)
    order = slab_ref.shape[1]
    slab = contract(slab_ref[...], before_ref[...], 1, 1)
    image = contract(image_ref[...], before_ref[...], 1, 1)
    total[:, :order] = contract(slab, slab, 0, 0)
    total[:, order:] = contract(slab, image, 0, 0)
    all_sum(Copies(send, recv), at, total, result, land_core, land_x, land_plane)
    result[...] = result[...] / count
    factor_kernel(128, result.at[:, :order], inverse_ref, work, tile)
    inverse = inverse_ref[...]
    basis = contract(slab, inverse, 1, 1)
    basis_ref[...] = basis
    projected = contract(product(inverse, result[:, order:]), inverse, 1, 1)
    projected_ref[...] = projected
    residual_ref[...] = contract(image, inverse, 1, 1) - product(basis, projected)


def on_device(matrix, start_vectors, interval):
    slab_rows, vectors = start_vectors.shape
    total_rows = slab_rows * lax.axis_size("row") * lax.axis_size("col")
    center = 0.5 * (interval[0] + interval[1])
    half_width = 0.5 * (interval[1] - interval[0])
    scale = jnp.stack([center, 1.0 / half_width])
    early, slab, mapped = filtered_blocks(matrix, start_vectors, scale)

    f32 = jnp.float32
    vmem = pl.BlockSpec(memory_space=pltpu.VMEM)
    square = jax.ShapeDtypeStruct((vectors, vectors), f32)
    tall = jax.ShapeDtypeStruct((slab_rows, vectors), f32)
    cost = pl.CostEstimate(flops=2 * vectors**3, bytes_accessed=8 * vectors**2, transcendentals=vectors)
    before = pl.pallas_call(
        functools.partial(early_kernel, total_rows),
        out_shape=square,
        in_specs=[vmem],
        out_specs=vmem,
        scratch_shapes=sum_scratch(vectors, vectors),
        compiler_params=pltpu.CompilerParams(collective_id=1, has_side_effects=True, vmem_limit_bytes=40 * 2**20),
        cost_estimate=cost,
    )(early)
    return pl.pallas_call(
        functools.partial(late_kernel, total_rows),
        out_shape=(tall, square, tall),
        in_specs=[vmem] * 3,
        out_specs=(vmem,) * 3,
        scratch_shapes=[pltpu.VMEM((vectors, vectors), f32)] + sum_scratch(vectors, 2 * vectors),
        compiler_params=pltpu.CompilerParams(collective_id=2, has_side_effects=True, vmem_limit_bytes=40 * 2**20),
        cost_estimate=cost,
    )(slab, mapped, before)


def solution(mesh):
    return jax.shard_map(
        on_device,
        mesh=mesh,
        in_specs=(P("row", "col"), P(("col", "row"), None), P()),
        out_specs=(P(("col", "row"), None), P(), P(("col", "row"), None)),
        check_vma=False,
    )
```

```python
import functools

import jax
import jax.numpy as jnp
from jax import lax
from jax.experimental import pallas as pl
from jax.experimental.pallas import tpu as pltpu
from jax.sharding import PartitionSpec as P

FILTER_DEG = 3
OUTER = 2
PANEL = 8
MESH = pl.DeviceIdType.MESH
CHUNK = 128


def product(left, right, precision=lax.Precision.HIGHEST):
    return jnp.dot(left, right, precision=precision, preferred_element_type=jnp.float32)


def contract(left, right, left_dim, right_dim):
    return lax.dot_general(
        left,
        right,
        (((left_dim,), (right_dim,)), ((), ())),
        precision=lax.Precision.HIGHEST,
        preferred_element_type=jnp.float32,
    )


def lane_columns(rows, first):
    narrow = rows[:, :128]
    lanes = jnp.zeros((PANEL, 128), jnp.int32) + first
    return [jnp.take_along_axis(narrow, lanes + j, axis=1) for j in range(PANEL)]


def row_of(value, step):
    return jnp.broadcast_to(value[step : step + 1, :], value.shape)


def factor_block(tile, pending):
    block = tile.shape[1] // 2
    sub = lax.broadcasted_iota(jnp.int32, (PANEL, 128), 0)
    lane = lax.broadcasted_iota(jnp.int32, (PANEL, block), 1)
    pending[...] = jnp.zeros_like(pending)

    def panel(p, carry):
        first = pl.multiple_of(p * PANEL, PANEL)
        here, after = pl.ds(first, PANEL), pl.ds(pl.multiple_of(first + PANEL, PANEL), PANEL)
        rows = tile[here, :]
        late = pending[...]
        tile[:block, :] -= contract(jnp.where(lane >= first + PANEL, late[:, :block], 0.0), late, 0, 0)

        columns = lane_columns(rows, first)
        left, right = rows[:, :block], rows[:, block:]
        inverses = []
        pivots = jnp.ones((PANEL, 128), jnp.float32)
        for s in range(PANEL):
            pivot = row_of(columns[s], s)
            pivots = jnp.where(sub == s, pivot, pivots)
            inverse = 1.0 / pivot
            inverses.append(inverse)
            if s < PANEL - 1:
                ratio = jnp.where(sub > s, columns[s] * inverse, 0.0)
                for j in range(s + 1, PANEL):
                    columns[j] = columns[j] - ratio * row_of(columns[j], s)
                left = left - ratio * row_of(left, s)
                right = right - ratio * row_of(right, s)

        following = tile[after, :]
        others = lane_columns(following, first)
        next_left, next_right = following[:, :block], following[:, block:]
        for s in range(PANEL):
            ratio = others[s] * inverses[s]
            for j in range(s + 1, PANEL):
                others[j] = others[j] - ratio * row_of(columns[j], s)
            next_left = next_left - ratio * row_of(left, s)
            next_right = next_right - ratio * row_of(right, s)
        tile[after, :block] = next_left
        tile[after, block:] = next_right
        scale = lax.rsqrt(pivots)
        left, right = left * scale, right * scale
        tile[here, :block] = left
        tile[here, block:] = right
        pending[:, :block] = left
        pending[:, block:] = right
        return carry

    lax.fori_loop(0, block // PANEL, panel, 0)


def factor_kernel(block, gram_ref, inverse_ref, work, tile, pending):
    order = gram_ref.shape[0]
    work[...] = gram_ref[...]
    at_row = lax.broadcasted_iota(jnp.int32, (order, order), 0)
    at_col = lax.broadcasted_iota(jnp.int32, (order, order), 1)
    inverse_ref[...] = (at_row == at_col).astype(jnp.float32)
    unit = (
        lax.broadcasted_iota(jnp.int32, (block, block), 0)
        == lax.broadcasted_iota(jnp.int32, (block, block), 1)
    ).astype(jnp.float32)

    def one(b, carry):
        start = pl.multiple_of(b * block, block)
        tile[:block, :block] = work[pl.ds(start, block), pl.ds(start, block)]
        tile[:block, block:] = unit
        tile[block:, :] = jnp.zeros((PANEL, 2 * block), jnp.float32)
        factor_block(tile, pending)
        for k in range(order // block):
            @pl.when(b == k)
            def _():
                at, stop = k * block, (k + 1) * block
                row = lax.broadcasted_iota(jnp.int32, (block, block), 0)
                col = lax.broadcasted_iota(jnp.int32, (block, block), 1)
                small = jnp.where(row >= col, tile[:block, block:], 0.0)
                solved = product(small, inverse_ref[at:stop, :stop])
                inverse_ref[at:stop, :stop] = solved
                if stop < order:
                    below = contract(work[stop:, at:stop], small, 1, 1)
                    work[stop:, stop:] -= contract(below, below, 1, 1)
                    inverse_ref[stop:, :stop] -= product(below, solved)
        return carry

    lax.fori_loop(0, order // block, one, 0)


class Copies:
    def __init__(self, send, recv):
        self.send, self.recv, self.used = send, recv, 0

    def reserve(self, count):
        first = self.used
        self.used += count
        return first

    def make(self, source, target, slot, device):
        return pltpu.make_async_remote_copy(
            src_ref=source,
            dst_ref=target,
            send_sem=self.send.at[slot],
            recv_sem=self.recv.at[slot],
            device_id=device,
            device_id_type=MESH,
        )


class Scatter:
    def __init__(self, copies, slot, place, ring, part, land):
        self.place, self.part, self.land = place, part, land
        left, right = ring
        ahead, behind, across = (place + 1) % 4, (place + 3) % 4, (place + 2) % 4
        self.ahead, self.behind = ahead, behind
        plan = (
            (part(across, 0), right),
            (part(across, 1), left),
            (part(ahead, 1), right),
            (part(behind, 0), left),
            (part(ahead, 0), right),
            (part(behind, 1), left),
        )
        self.copies = [
            copies.make(source, land(i), slot + i, device) for i, (source, device) in enumerate(plan)
        ]

    def start(self):
        for copy in self.copies[:4]:
            copy.start()

    def relay(self):
        for first, half, target in ((0, 0, self.ahead), (1, 1, self.behind)):
            self.copies[first].wait_recv()
            mine = self.part(target, half)
            mine[...] += self.land(first)[...]
            self.copies[4 + first].start()

    def finish(self):
        for copy in self.copies[2:]:
            copy.wait_recv()
        for half, terms in ((0, (3, 4)), (1, (2, 5))):
            mine = self.part(self.place, half)
            mine[...] += self.land(terms[0])[...] + self.land(terms[1])[...]
        for copy in self.copies:
            copy.wait_send()


class Gather:
    def __init__(self, copies, slot, place, ring, part):
        left, right = ring
        ahead, behind = (place + 1) % 4, (place + 3) % 4
        self.copies = [
            copies.make(part(place, None), part(place, None), slot, right),
            copies.make(part(place, None), part(place, None), slot + 1, left),
            copies.make(part(behind, 0), part(behind, 0), slot + 2, right),
            copies.make(part(ahead, 1), part(ahead, 1), slot + 3, left),
        ]

    def start(self):
        for copy in self.copies[:2]:
            copy.start()

    def forward(self):
        for first in range(2):
            self.copies[first].wait_recv()
            self.copies[2 + first].start()

    def finish(self):
        for copy in self.copies[2:]:
            copy.wait_recv()
        for copy in self.copies:
            copy.wait_send()


def split(value):
    high = value.astype(jnp.bfloat16)
    return high, (value - high.astype(jnp.float32)).astype(jnp.bfloat16)


def three_pass(left, right, dims):
    def one(a, b):
        return lax.dot_general(a, b, (dims, ((), ())), preferred_element_type=jnp.float32)

    return one(left[0], right[0]) + (one(left[0], right[1]) + one(left[1], right[0]))


def filter_kernel(
    scale_ref, block_ref, start_ref, first_ref, last_ref, image_ref,
    other, high, low, rows, row_parts, cols, col_parts, vec_high, vec_low,
    land_big, land_small, land_col, row_prev, col_prev, first_part,
    start_land, first_land, last_land, image_land, send, recv,
):
    r, c = lax.axis_index("row"), lax.axis_index("col")
    core, x, y, z = r % 2, r // 2, c % 4, c // 4
    copies = Copies(send, recv)

    def device(x, core, y, z):
        return (2 * x + core, 4 * z + y)

    mate = device(x, 1 - core, y, z)
    ring_x = device((x + 3) % 4, core, y, z), device((x + 1) % 4, core, y, z)
    ring_y = device(x, core, (y + 3) % 4, z), device(x, core, (y + 1) % 4, z)
    ring_z = device(x, core, y, (z + 3) % 4), device(x, core, y, (z + 1) % 4)
    crossed = x != z

    barrier = pltpu.get_barrier_semaphore()

    def greet(who):
        pl.semaphore_signal(barrier, inc=1, device_id=who, device_id_type=MESH)

    for who in (mate, *ring_x, *ring_y, *ring_z):
        greet(who)

    @pl.when(crossed)
    def _():
        greet(device(z, core, y, x))
        greet(device(z, 1 - core, y, x))

    pl.semaphore_wait(barrier, jnp.where(crossed, 9, 7))

    block_rows, block_cols = block_ref.shape
    slab = start_ref.shape[0]
    width = start_ref.shape[1] // 2
    mine_cols = pl.ds(pl.multiple_of(core * width, width), width)
    mate_cols = pl.ds(pl.multiple_of((1 - core) * width, width), width)

    start_copy = copies.make(start_ref.at[:, mate_cols], start_land, copies.reserve(1), mate)
    start_copy.start()
    block_copy = copies.make(block_ref, other, copies.reserve(1), mate)
    block_copy.start()

    center, inverse_width = scale_ref[0], scale_ref[1]

    def prepare(source, which):
        base = which * block_rows
        step = 256

        @pl.loop(0, block_rows // step)
        def _(i):
            at = pl.multiple_of(i * step, step)
            value = source[pl.ds(at, step), :]
            row = lax.broadcasted_iota(jnp.int32, value.shape, 0) + (2 * x * block_rows + base + at)
            col = lax.broadcasted_iota(jnp.int32, value.shape, 1) + c * block_cols
            value = jnp.where(row == col, value - center, value) * inverse_width
            big, small = split(value)
            to = pl.ds(pl.multiple_of(base + at, step), step)
            high[to, :] = big
            low[to, :] = small

    prepare(block_ref, core)

    start_copy.wait_recv()
    half = width // 2
    own = start_ref[:, mine_cols]
    theirs = start_land[...]
    lower = jnp.where(core == 0, own, theirs)
    upper = jnp.where(core == 0, theirs, own)
    piece = jnp.concatenate([lower, upper], axis=0).T
    cols[x] = piece
    col_prev[...] = piece
    row_prev[...] = jnp.zeros_like(row_prev)
    start_copy.wait_send()

    def col_slice(ref):
        def part(t, side):
            if side is None:
                return ref.at[t]
            return ref.at[t, pl.ds(side * half, half), :]
        return part

    def plane_slice(ref, colour, axis):
        def part(t, side):
            size = half if side is None else half // 2
            at = pl.ds(colour * half + (0 if side is None else side * size), size)
            return ref.at[:, t, at, :] if axis == "z" else ref.at[t, :, at, :]
        return part

    def line_slice(ref, colour, axis):
        def part(t, side):
            size = half if side is None else half // 2
            at = pl.ds(colour * half + (0 if side is None else side * size), size)
            return ref.at[y, t, at, :] if axis == "z" else ref.at[t, z, at, :]
        return part

    places = {"y": y, "z": z}
    rings = {"y": ring_y, "z": ring_z}
    orders = (("z", "y"), ("y", "z"))

    scatter_slots = [[copies.reserve(6) for _ in range(2)] for _ in range(2)]
    gather_slots = [[copies.reserve(4) for _ in range(2)] for _ in range(2)]
    col_slots = copies.reserve(6), copies.reserve(4)

    def scatter_stage(colour, stage):
        axis = orders[colour][stage]
        ref_slice = (plane_slice if stage == 0 else line_slice)(row_parts, colour, axis)
        land = (lambda i: land_big.at[colour, i]) if stage == 0 else (lambda i: land_small.at[colour, i])
        return Scatter(copies, scatter_slots[colour][stage], places[axis], rings[axis], ref_slice, land)

    def gather_stage(colour, stage):
        axis = orders[colour][1 - stage]
        ref_slice = (line_slice if stage == 0 else plane_slice)(rows, colour, axis)
        return Gather(copies, gather_slots[colour][stage], places[axis], rings[axis], ref_slice)

    col_gather = Gather(copies, col_slots[1], x, ring_x, col_slice(cols))
    col_scatter = Scatter(copies, col_slots[0], x, ring_x, col_slice(col_parts), lambda i: land_col.at[i])

    col_gather.start()
    col_gather.forward()
    col_gather.finish()

    block_copy.wait_recv()
    prepare(other, 1 - core)
    block_copy.wait_send()

    def to_rows():
        for q in range(4):
            big, small = split(cols[q])
            vec_high[:, q * CHUNK : (q + 1) * CHUNK] = big
            vec_low[:, q * CHUNK : (q + 1) * CHUNK] = small

        @pl.loop(0, 8)
        def _(i):
            at = pl.ds(pl.multiple_of(i * 256, 256), 256)
            out = three_pass((vec_high[...], vec_low[...]), (high[at, :], low[at, :]), ((1,), (1,)))
            row_parts[i // 2, 2 * (i % 2)] = out[:, :CHUNK]
            row_parts[i // 2, 2 * (i % 2) + 1] = out[:, CHUNK:]

        stages = [scatter_stage(0, 0), scatter_stage(1, 0)]
        for stage in stages:
            stage.start()
        for stage in stages:
            stage.relay()
        seconds = [scatter_stage(0, 1), scatter_stage(1, 1)]
        for stage, second in zip(stages, seconds):
            stage.finish()
            second.start()
        for second in seconds:
            second.relay()
        return seconds

    def sweep(step, carry):
        factor = jnp.where(step == 0, 1.0, 2.0)
        weight = jnp.where(step == 0, 0.0, 1.0)
        seconds = to_rows()
        gathers = []
        for colour, second in enumerate(seconds):
            second.finish()
            at = pl.ds(colour * half, half)
            value = factor * row_parts[y, z, at, :] - weight * row_prev[at, :]
            rows[y, z, at, :] = value
            row_prev[at, :] = value
            first = gather_stage(colour, 0)
            first.start()
            gathers.append(first)

        @pl.when(step == 1)
        def _():
            first_part[...] = row_prev[...]

        for first in gathers:
            first.forward()
        lasts = []
        for colour, first in enumerate(gathers):
            first.finish()
            last = gather_stage(colour, 1)
            last.start()
            lasts.append(last)
        for last in lasts:
            last.forward()
        for last in lasts:
            last.finish()

        for q in range(4):
            col_parts[q] = jnp.zeros((width, CHUNK), jnp.float32)

        @pl.loop(0, 8)
        def _(i):
            at = pl.ds(pl.multiple_of(i * 256, 256), 256)
            vec = jnp.concatenate([rows[i // 2, 2 * (i % 2)], rows[i // 2, 2 * (i % 2) + 1]], axis=1)
            out = three_pass(split(vec), (high[at, :], low[at, :]), ((1,), (0,)))
            for q in range(4):
                col_parts[q] += out[:, q * CHUNK : (q + 1) * CHUNK]

        col_scatter.start()
        col_scatter.relay()
        col_scatter.finish()
        again = jnp.where(step == 1, 1.0, 2.0)
        minus = jnp.where(step == 1, 0.0, 1.0)
        value = again * col_parts[x] - minus * col_prev[...]
        cols[x] = value
        col_prev[...] = value
        col_gather.start()
        col_gather.forward()
        col_gather.finish()
        return carry

    lax.fori_loop(0, 3, sweep, 0)
    for second in to_rows():
        second.finish()

    def trade(piece, land, out_ref):
        turned = piece.T
        land[1] = turned
        copy = copies.make(
            land.at[1, pl.ds(pl.multiple_of((1 - core) * slab, slab), slab), :],
            land.at[0, pl.ds(pl.multiple_of((1 - core) * slab, slab), slab), :],
            copies.reserve(1),
            mate,
        )
        copy.start()
        return copy

    first_copy = trade(first_part[...], first_land, first_ref)
    last_copy = trade(col_prev[...], last_land, last_ref)

    image_land[2, :, :] = row_parts[y, z].T
    image_slots = copies.reserve(2)

    same = copies.make(
        image_land.at[2, pl.ds(pl.multiple_of(core * slab, slab), slab), :],
        image_land.at[0, pl.ds(0, slab), :],
        image_slots,
        device(z, core, y, x),
    )
    cross = copies.make(
        image_land.at[2, pl.ds(pl.multiple_of((1 - core) * slab, slab), slab), :],
        image_land.at[1, pl.ds(0, slab), :],
        image_slots + 1,
        device(z, 1 - core, y, x),
    )
    cross.start()

    @pl.when(crossed)
    def _():
        same.start()
        same.wait()

    @pl.when(jnp.logical_not(crossed))
    def _():
        image_land[0, pl.ds(0, slab), :] = image_land[2, pl.ds(pl.multiple_of(core * slab, slab), slab), :]

    keep = pl.ds(pl.multiple_of(core * slab, slab), slab)
    for copy, land, out_ref in ((first_copy, first_land, first_ref), (last_copy, last_land, last_ref)):
        copy.wait()
        out_ref[:, mine_cols] = land[1, keep, :]
        out_ref[:, mate_cols] = land[0, keep, :]
    cross.wait()
    image_ref[:, mine_cols] = image_land[0, pl.ds(0, slab), :]
    image_ref[:, mate_cols] = image_land[1, pl.ds(0, slab), :]


def filtered_blocks(matrix, start_vectors, scale):
    block_rows, block_cols = matrix.shape
    slab, vectors = start_vectors.shape
    width = vectors // 2
    half = width // 2
    f32, bf16 = jnp.float32, jnp.bfloat16
    vmem = pl.BlockSpec(memory_space=pltpu.VMEM)
    return pl.pallas_call(
        filter_kernel,
        out_shape=[jax.ShapeDtypeStruct((slab, vectors), f32)] * 3,
        in_specs=[pl.BlockSpec(memory_space=pltpu.SMEM), vmem, vmem],
        out_specs=[vmem] * 3,
        scratch_shapes=[
            pltpu.VMEM((block_rows, block_cols), f32),
            pltpu.VMEM((2 * block_rows, block_cols), bf16),
            pltpu.VMEM((2 * block_rows, block_cols), bf16),
            pltpu.VMEM((4, 4, width, CHUNK), f32),
            pltpu.VMEM((4, 4, width, CHUNK), f32),
            pltpu.VMEM((4, width, CHUNK), f32),
            pltpu.VMEM((4, width, CHUNK), f32),
            pltpu.VMEM((width, block_cols), bf16),
            pltpu.VMEM((width, block_cols), bf16),
            pltpu.VMEM((2, 6, 4, half // 2, CHUNK), f32),
            pltpu.VMEM((2, 6, half // 2, CHUNK), f32),
            pltpu.VMEM((6, half, CHUNK), f32),
            pltpu.VMEM((width, CHUNK), f32),
            pltpu.VMEM((width, CHUNK), f32),
            pltpu.VMEM((width, CHUNK), f32),
            pltpu.VMEM((slab, width), f32),
            pltpu.VMEM((2, CHUNK, width), f32),
            pltpu.VMEM((2, CHUNK, width), f32),
            pltpu.VMEM((3, CHUNK, width), f32),
            pltpu.SemaphoreType.DMA((64,)),
            pltpu.SemaphoreType.DMA((64,)),
        ],
        compiler_params=pltpu.CompilerParams(
            collective_id=0, has_side_effects=True, vmem_limit_bytes=40 * 2**20
        ),
        cost_estimate=pl.CostEstimate(flops=10**10, bytes_accessed=4 * 10**6, transcendentals=0),
    )(scale, matrix, start_vectors)


class Places:
    def __init__(self):
        self.r, self.c = lax.axis_index("row"), lax.axis_index("col")
        self.core, self.x = self.r % 2, self.r // 2
        self.y, self.z = self.c % 4, self.c // 4
        self.mate = (2 * self.x + 1 - self.core, self.c)
        self.ring_x = ((self.r + 6) % 8, self.c), ((self.r + 2) % 8, self.c)

    def peer(self, offset):
        return self.r, (self.c + offset) % 16


def all_sum(copies, at, total, result, land_core, land_x, land_plane):
    order, width = total.shape
    half, quarter = order // 2, order // 8

    def rows(first, count, ref=total):
        return ref.at[pl.ds(pl.multiple_of(first, 8), count), :]

    mine, theirs = rows(at.core * half, half), rows((1 - at.core) * half, half)
    swap = copies.make(theirs, land_core, copies.reserve(1), at.mate)
    swap.start()
    swap.wait_recv()
    mine[...] += land_core[...]

    def part(t, side, ref=total):
        size = quarter if side is None else quarter // 2
        return rows(at.core * half + t * quarter + (0 if side is None else side * size), size, ref)

    scatter = Scatter(copies, copies.reserve(6), at.x, at.ring_x, part, lambda i: land_x.at[i])
    scatter.start()
    scatter.relay()
    scatter.finish()

    def piece(t, ref=total):
        first = at.core * half + at.x * quarter + 8 * (t // 2)
        lanes = pl.ds(pl.multiple_of((t % 2) * (width // 2), 128), width // 2)
        return ref.at[pl.ds(pl.multiple_of(first, 8), 8), lanes]

    slots = copies.reserve(15), copies.reserve(15)
    sent = []
    for offset in range(1, 16):
        to = (at.c + offset) % 16
        copy = copies.make(piece(to), land_plane.at[offset], slots[0] + offset - 1, at.peer(offset))
        copy.start()
        sent.append(copy)
    own = piece(at.c)
    value = own[...]
    for offset, copy in enumerate(sent, 1):
        copy.wait_recv()
        value = value + land_plane[offset]
    own = piece(at.c, result)
    own[...] = value
    back = []
    for offset in range(1, 16):
        copy = copies.make(own, own, slots[1] + offset - 1, at.peer(offset))
        copy.start()
        back.append(copy)
    for copy in back:
        copy.wait_recv()
    gather = Gather(copies, copies.reserve(4), at.x, at.ring_x, lambda t, side: part(t, side, result))
    gather.start()
    gather.forward()
    gather.finish()
    mine = rows(at.core * half, half, result)
    give = copies.make(mine, mine, copies.reserve(1), at.mate)
    give.start()
    for copy in (swap, *sent, *back):
        copy.wait_send()
    give.wait()


def greet_all(at):
    barrier = pltpu.get_barrier_semaphore()
    others = [at.mate, *at.ring_x] + [at.peer(offset) for offset in range(1, 16)]
    for who in others:
        pl.semaphore_signal(barrier, inc=1, device_id=who, device_id_type=MESH)
    pl.semaphore_wait(barrier, len(others))


def sum_scratch(order, width):
    f32 = jnp.float32
    return [
        pltpu.VMEM((order, width), f32),
        pltpu.VMEM((order, width), f32),
        pltpu.VMEM((order // 2, width), f32),
        pltpu.VMEM((6, order // 16, width), f32),
        pltpu.VMEM((16, 8, width // 2), f32),
        pltpu.VMEM((order, order), f32),
        pltpu.VMEM((128 + PANEL, 256), f32),
        pltpu.VMEM((PANEL, 256), f32),
        pltpu.SemaphoreType.DMA((64,)),
        pltpu.SemaphoreType.DMA((64,)),
    ]


def early_kernel(count, slab_ref, inverse_ref, total, result, land_core, land_x, land_plane, work, tile, pending, send, recv):
    at = Places()
    greet_all(at)
    slab = slab_ref[...]
    total[...] = contract(slab, slab, 0, 0)
    all_sum(Copies(send, recv), at, total, result, land_core, land_x, land_plane)
    result[...] = result[...] / count
    factor_kernel(128, result, inverse_ref, work, tile, pending)


def late_kernel(
    count, slab_ref, image_ref, before_ref, basis_ref, projected_ref, residual_ref,
    inverse_ref, total, result, land_core, land_x, land_plane, work, tile, pending, send, recv,
):
    at = Places()
    greet_all(at)
    order = slab_ref.shape[1]
    slab = contract(slab_ref[...], before_ref[...], 1, 1)
    image = contract(image_ref[...], before_ref[...], 1, 1)
    total[:, :order] = contract(slab, slab, 0, 0)
    total[:, order:] = contract(slab, image, 0, 0)
    all_sum(Copies(send, recv), at, total, result, land_core, land_x, land_plane)
    result[...] = result[...] / count
    factor_kernel(128, result.at[:, :order], inverse_ref, work, tile, pending)
    inverse = inverse_ref[...]
    basis = contract(slab, inverse, 1, 1)
    basis_ref[...] = basis
    projected = contract(product(inverse, result[:, order:]), inverse, 1, 1)
    projected_ref[...] = projected
    residual_ref[...] = contract(image, inverse, 1, 1) - product(basis, projected)


def on_device(matrix, start_vectors, interval):
    slab_rows, vectors = start_vectors.shape
    total_rows = slab_rows * lax.axis_size("row") * lax.axis_size("col")
    center = 0.5 * (interval[0] + interval[1])
    half_width = 0.5 * (interval[1] - interval[0])
    scale = jnp.stack([center, 1.0 / half_width])
    early, slab, mapped = filtered_blocks(matrix, start_vectors, scale)

    f32 = jnp.float32
    vmem = pl.BlockSpec(memory_space=pltpu.VMEM)
    square = jax.ShapeDtypeStruct((vectors, vectors), f32)
    tall = jax.ShapeDtypeStruct((slab_rows, vectors), f32)
    cost = pl.CostEstimate(flops=2 * vectors**3, bytes_accessed=8 * vectors**2, transcendentals=vectors)
    before = pl.pallas_call(
        functools.partial(early_kernel, total_rows),
        out_shape=square,
        in_specs=[vmem],
        out_specs=vmem,
        scratch_shapes=sum_scratch(vectors, vectors),
        compiler_params=pltpu.CompilerParams(collective_id=1, has_side_effects=True, vmem_limit_bytes=40 * 2**20),
        cost_estimate=cost,
    )(early)
    return pl.pallas_call(
        functools.partial(late_kernel, total_rows),
        out_shape=(tall, square, tall),
        in_specs=[vmem] * 3,
        out_specs=(vmem,) * 3,
        scratch_shapes=[pltpu.VMEM((vectors, vectors), f32)] + sum_scratch(vectors, 2 * vectors),
        compiler_params=pltpu.CompilerParams(collective_id=2, has_side_effects=True, vmem_limit_bytes=40 * 2**20),
        cost_estimate=cost,
    )(slab, mapped, before)


def solution(mesh):
    return jax.shard_map(
        on_device,
        mesh=mesh,
        in_specs=(P("row", "col"), P(("col", "row"), None), P()),
        out_specs=(P(("col", "row"), None), P(), P(("col", "row"), None)),
        check_vma=False,
    )
```

```python
import functools

import jax
import jax.numpy as jnp
from jax import lax
from jax.experimental import pallas as pl
from jax.experimental.pallas import tpu as pltpu
from jax.sharding import PartitionSpec as P

FILTER_DEG = 3
OUTER = 2
PANEL = 8
MESH = pl.DeviceIdType.MESH
CHUNK = 128


def product(left, right, precision=lax.Precision.HIGHEST):
    return jnp.dot(left, right, precision=precision, preferred_element_type=jnp.float32)


def contract(left, right, left_dim, right_dim):
    return lax.dot_general(
        left,
        right,
        (((left_dim,), (right_dim,)), ((), ())),
        precision=lax.Precision.HIGHEST,
        preferred_element_type=jnp.float32,
    )


def lane_columns(rows, first):
    narrow = rows[:, :128]
    lanes = jnp.zeros((PANEL, 128), jnp.int32) + first
    return [jnp.take_along_axis(narrow, lanes + j, axis=1) for j in range(PANEL)]


def row_of(value, step):
    return jnp.broadcast_to(value[step : step + 1, :], value.shape)


def factor_block(tile, pending):
    block = tile.shape[1] // 2
    sub = lax.broadcasted_iota(jnp.int32, (PANEL, 128), 0)
    lane = lax.broadcasted_iota(jnp.int32, (PANEL, block), 1)
    pending[...] = jnp.zeros_like(pending)

    def panel(p, carry):
        first = pl.multiple_of(p * PANEL, PANEL)
        here, after = pl.ds(first, PANEL), pl.ds(pl.multiple_of(first + PANEL, PANEL), PANEL)
        rows = tile[here, :]
        late = pending[...]
        tile[:block, :] -= contract(jnp.where(lane >= first + PANEL, late[:, :block], 0.0), late, 0, 0)

        columns = lane_columns(rows, first)
        left, right = rows[:, :block], rows[:, block:]
        inverses = []
        pivots = jnp.ones((PANEL, 128), jnp.float32)
        for s in range(PANEL):
            pivot = row_of(columns[s], s)
            pivots = jnp.where(sub == s, pivot, pivots)
            inverse = 1.0 / pivot
            inverses.append(inverse)
            if s < PANEL - 1:
                ratio = jnp.where(sub > s, columns[s] * inverse, 0.0)
                for j in range(s + 1, PANEL):
                    columns[j] = columns[j] - ratio * row_of(columns[j], s)
                left = left - ratio * row_of(left, s)
                right = right - ratio * row_of(right, s)

        following = tile[after, :]
        others = lane_columns(following, first)
        next_left, next_right = following[:, :block], following[:, block:]
        for s in range(PANEL):
            ratio = others[s] * inverses[s]
            for j in range(s + 1, PANEL):
                others[j] = others[j] - ratio * row_of(columns[j], s)
            next_left = next_left - ratio * row_of(left, s)
            next_right = next_right - ratio * row_of(right, s)
        tile[after, :block] = next_left
        tile[after, block:] = next_right
        scale = lax.rsqrt(pivots)
        left, right = left * scale, right * scale
        tile[here, :block] = left
        tile[here, block:] = right
        pending[:, :block] = left
        pending[:, block:] = right
        return carry

    lax.fori_loop(0, block // PANEL, panel, 0)


def factor_kernel(block, gram_ref, inverse_ref, work, tile, pending):
    order = gram_ref.shape[0]
    work[...] = gram_ref[...]
    at_row = lax.broadcasted_iota(jnp.int32, (order, order), 0)
    at_col = lax.broadcasted_iota(jnp.int32, (order, order), 1)
    inverse_ref[...] = (at_row == at_col).astype(jnp.float32)
    unit = (
        lax.broadcasted_iota(jnp.int32, (block, block), 0)
        == lax.broadcasted_iota(jnp.int32, (block, block), 1)
    ).astype(jnp.float32)

    def one(b, carry):
        start = pl.multiple_of(b * block, block)
        tile[:block, :block] = work[pl.ds(start, block), pl.ds(start, block)]
        tile[:block, block:] = unit
        tile[block:, :] = jnp.zeros((PANEL, 2 * block), jnp.float32)
        factor_block(tile, pending)
        for k in range(order // block):
            @pl.when(b == k)
            def _():
                at, stop = k * block, (k + 1) * block
                row = lax.broadcasted_iota(jnp.int32, (block, block), 0)
                col = lax.broadcasted_iota(jnp.int32, (block, block), 1)
                small = jnp.where(row >= col, tile[:block, block:], 0.0)
                solved = product(small, inverse_ref[at:stop, :stop])
                inverse_ref[at:stop, :stop] = solved
                if stop < order:
                    below = contract(work[stop:, at:stop], small, 1, 1)
                    work[stop:, stop:] -= contract(below, below, 1, 1)
                    inverse_ref[stop:, :stop] -= product(below, solved)
        return carry

    lax.fori_loop(0, order // block, one, 0)


class Copies:
    def __init__(self, send, recv):
        self.send, self.recv, self.used = send, recv, 0

    def reserve(self, count):
        first = self.used
        self.used += count
        return first

    def make(self, source, target, slot, device):
        return pltpu.make_async_remote_copy(
            src_ref=source,
            dst_ref=target,
            send_sem=self.send.at[slot],
            recv_sem=self.recv.at[slot],
            device_id=device,
            device_id_type=MESH,
        )


class Scatter:
    def __init__(self, copies, slot, place, ring, part, land):
        self.place, self.part, self.land = place, part, land
        left, right = ring
        ahead, behind, across = (place + 1) % 4, (place + 3) % 4, (place + 2) % 4
        self.ahead, self.behind = ahead, behind
        plan = (
            (part(across, 0), right),
            (part(across, 1), left),
            (part(ahead, 1), right),
            (part(behind, 0), left),
            (part(ahead, 0), right),
            (part(behind, 1), left),
        )
        self.copies = [
            copies.make(source, land(i), slot + i, device) for i, (source, device) in enumerate(plan)
        ]

    def start(self):
        for copy in self.copies[:4]:
            copy.start()

    def relay(self):
        for first, half, target in ((0, 0, self.ahead), (1, 1, self.behind)):
            self.copies[first].wait_recv()
            mine = self.part(target, half)
            mine[...] += self.land(first)[...]
            self.copies[4 + first].start()

    def finish(self):
        for copy in self.copies[2:]:
            copy.wait_recv()
        for half, terms in ((0, (3, 4)), (1, (2, 5))):
            mine = self.part(self.place, half)
            mine[...] += self.land(terms[0])[...] + self.land(terms[1])[...]
        for copy in self.copies:
            copy.wait_send()


class Gather:
    def __init__(self, copies, slot, place, ring, part):
        left, right = ring
        ahead, behind = (place + 1) % 4, (place + 3) % 4
        self.copies = [
            copies.make(part(place, None), part(place, None), slot, right),
            copies.make(part(place, None), part(place, None), slot + 1, left),
            copies.make(part(behind, 0), part(behind, 0), slot + 2, right),
            copies.make(part(ahead, 1), part(ahead, 1), slot + 3, left),
        ]

    def start(self):
        for copy in self.copies[:2]:
            copy.start()

    def forward(self):
        for first in range(2):
            self.copies[first].wait_recv()
            self.copies[2 + first].start()

    def finish(self):
        for copy in self.copies[2:]:
            copy.wait_recv()
        for copy in self.copies:
            copy.wait_send()


def split(value):
    high = value.astype(jnp.bfloat16)
    return high, (value - high.astype(jnp.float32)).astype(jnp.bfloat16)


def three_pass(left, right, dims):
    def one(a, b):
        return lax.dot_general(a, b, (dims, ((), ())), preferred_element_type=jnp.float32)

    return one(left[0], right[0]) + (one(left[0], right[1]) + one(left[1], right[0]))


STREAMS = 2
LEAD = 6


def filter_kernel(
    interval_ref, block_ref, start_ref, first_ref, last_ref, image_ref,
    block, other, high, low, rows, row_parts, cols, col_parts, vec_high, vec_low,
    land_big, land_small, land_col, row_prev, col_prev, first_part,
    start_land, first_land, last_land, image_land, send, recv, local_sem,
):
    r, c = lax.axis_index("row"), lax.axis_index("col")
    core, x, y, z = r % 2, r // 2, c % 4, c // 4
    copies = Copies(send, recv)

    def device(x, core, y, z):
        return (2 * x + core, 4 * z + y)

    mate = device(x, 1 - core, y, z)
    ring_x = device((x + 3) % 4, core, y, z), device((x + 1) % 4, core, y, z)
    ring_y = device(x, core, (y + 3) % 4, z), device(x, core, (y + 1) % 4, z)
    ring_z = device(x, core, y, (z + 3) % 4), device(x, core, y, (z + 1) % 4)
    crossed = x != z

    local = pltpu.make_async_copy(block_ref, block, local_sem)
    local.start()
    barrier = pltpu.get_barrier_semaphore()

    def greet(who):
        pl.semaphore_signal(barrier, inc=1, device_id=who, device_id_type=MESH)

    for who in (mate, *ring_x, *ring_y, *ring_z):
        greet(who)

    @pl.when(crossed)
    def _():
        greet(device(z, core, y, x))
        greet(device(z, 1 - core, y, x))

    pl.semaphore_wait(barrier, jnp.where(crossed, 9, 7))

    block_rows, block_cols = block.shape
    slab = start_ref.shape[0]
    width = start_ref.shape[1] // 2
    mine_cols = pl.ds(pl.multiple_of(core * width, width), width)
    mate_cols = pl.ds(pl.multiple_of((1 - core) * width, width), width)

    start_copy = copies.make(start_ref.at[:, mate_cols], start_land, copies.reserve(1), mate)
    start_copy.start()
    block_copy = copies.make(block_ref, other, copies.reserve(1), mate)
    block_copy.start()

    lower_end = jnp.full((1, block_cols), interval_ref[0], jnp.float32)
    upper_end = jnp.full((1, block_cols), interval_ref[1], jnp.float32)
    center = 0.5 * (lower_end + upper_end)
    inverse_width = 1.0 / (0.5 * (upper_end - lower_end))

    def prepare(source, which):
        base = which * block_rows
        step = 256

        @pl.loop(0, block_rows // step)
        def _(i):
            at = pl.multiple_of(i * step, step)
            value = source[pl.ds(at, step), :]
            row = lax.broadcasted_iota(jnp.int32, value.shape, 0) + (2 * x * block_rows + base + at)
            col = lax.broadcasted_iota(jnp.int32, value.shape, 1) + c * block_cols
            value = jnp.where(row == col, value - center, value) * inverse_width
            big, small = split(value)
            to = pl.ds(pl.multiple_of(base + at, step), step)
            high[to, :] = big
            low[to, :] = small

    start_copy.wait_recv()
    own = start_ref[:, mine_cols]
    theirs = start_land[...]
    lower = jnp.where(core == 0, own, theirs)
    upper = jnp.where(core == 0, theirs, own)
    piece = jnp.concatenate([lower, upper], axis=0).T
    cols[x] = piece
    col_prev[...] = piece

    places = {"y": y, "z": z}
    rings = {"y": ring_y, "z": ring_z}
    orders = (("z", "y"), ("y", "z"))
    share = width // STREAMS
    half = share // 2

    class Stream:
        def __init__(self, index):
            self.base = index * share
            self.all = pl.ds(self.base, share)
            slots = [[copies.reserve(6) for _ in range(2)] for _ in range(2)]
            self.scatters = [[self.scatter(index, u, stage, slots[u][stage]) for stage in range(2)] for u in range(2)]
            slots = [[copies.reserve(4) for _ in range(2)] for _ in range(2)]
            self.gathers = [[self.gather(u, stage, slots[u][stage]) for stage in range(2)] for u in range(2)]
            self.col_scatter = Scatter(
                copies, copies.reserve(6), x, ring_x, self.col_slice(col_parts), lambda i: land_col.at[index, i]
            )
            self.col_gather = Gather(copies, copies.reserve(4), x, ring_x, self.col_slice(cols))

        def span(self, colour, side):
            size = half if side is None else half // 2
            return pl.ds(self.base + colour * half + (0 if side is None else side * size), size)

        def col_slice(self, ref):
            def part(t, side):
                return ref.at[t, self.all if side is None else self.span(side, None), :]
            return part

        def plane(self, ref, colour, axis):
            def part(t, side):
                at = self.span(colour, side)
                return ref.at[:, t, at, :] if axis == "z" else ref.at[t, :, at, :]
            return part

        def line(self, ref, colour, axis):
            def part(t, side):
                at = self.span(colour, side)
                return ref.at[y, t, at, :] if axis == "z" else ref.at[t, z, at, :]
            return part

        def scatter(self, index, colour, stage, slot):
            axis = orders[colour][stage]
            part = (self.plane if stage == 0 else self.line)(row_parts, colour, axis)
            landing = land_big if stage == 0 else land_small
            return Scatter(copies, slot, places[axis], rings[axis], part, lambda i: landing.at[index, colour, i])

        def gather(self, colour, stage, slot):
            axis = orders[colour][1 - stage]
            part = (self.line if stage == 0 else self.plane)(rows, colour, axis)
            return Gather(copies, slot, places[axis], rings[axis], part)

        def multiply(self):
            for q in range(4):
                big, small = split(cols[q, self.all, :])
                vec_high[self.all, q * CHUNK : (q + 1) * CHUNK] = big
                vec_low[self.all, q * CHUNK : (q + 1) * CHUNK] = small

            @pl.loop(0, 8)
            def _(i):
                at = pl.ds(pl.multiple_of(i * 256, 256), 256)
                left = vec_high[self.all, :], vec_low[self.all, :]
                out = three_pass(left, (high[at, :], low[at, :]), ((1,), (1,)))
                row_parts[i // 2, 2 * (i % 2), self.all, :] = out[:, :CHUNK]
                row_parts[i // 2, 2 * (i % 2) + 1, self.all, :] = out[:, CHUNK:]

        def multiply_turned(self):
            for q in range(4):
                col_parts[q, self.all, :] = jnp.zeros((share, CHUNK), jnp.float32)

            @pl.loop(0, 8)
            def _(i):
                at = pl.ds(pl.multiple_of(i * 256, 256), 256)
                pair = [rows[i // 2, 2 * (i % 2) + k, self.all, :] for k in range(2)]
                out = three_pass(split(jnp.concatenate(pair, axis=1)), (high[at, :], low[at, :]), ((1,), (0,)))
                for q in range(4):
                    col_parts[q, self.all, :] += out[:, q * CHUNK : (q + 1) * CHUNK]

        def to_rows(self):
            self.multiply()
            firsts = [self.scatters[0][0], self.scatters[1][0]]
            seconds = [self.scatters[0][1], self.scatters[1][1]]
            for first in firsts:
                first.start()
            yield
            for first in firsts:
                first.relay()
            yield
            for first, second in zip(firsts, seconds):
                first.finish()
                second.start()
            yield
            for second in seconds:
                second.relay()
            yield

        def run(self):
            for step in range(3):
                yield from self.to_rows()
                for colour in range(2):
                    self.scatters[colour][1].finish()
                    at = self.span(colour, None)
                    value = row_parts[y, z, at, :]
                    if step > 0:
                        value = 2.0 * value - row_prev[at, :]
                    rows[y, z, at, :] = value
                    row_prev[at, :] = value
                    if step == 1:
                        first_part[at, :] = value
                    self.gathers[colour][0].start()
                yield
                for colour in range(2):
                    self.gathers[colour][0].forward()
                yield
                for colour in range(2):
                    self.gathers[colour][0].finish()
                    self.gathers[colour][1].start()
                yield
                for colour in range(2):
                    self.gathers[colour][1].forward()
                yield
                for colour in range(2):
                    self.gathers[colour][1].finish()
                self.multiply_turned()
                self.col_scatter.start()
                yield
                self.col_scatter.relay()
                yield
                self.col_scatter.finish()
                value = col_parts[x, self.all, :]
                if step != 1:
                    value = 2.0 * value - col_prev[self.all, :]
                cols[x, self.all, :] = value
                col_prev[self.all, :] = value
                self.col_gather.start()
                yield
                self.col_gather.forward()
                yield
                self.col_gather.finish()
            yield from self.to_rows()
            for colour in range(2):
                self.scatters[colour][1].finish()

    streams = [Stream(index) for index in range(STREAMS)]
    for stream in streams:
        stream.col_gather.start()
    local.wait()
    prepare(block, core)
    for stream in streams:
        stream.col_gather.forward()
    start_copy.wait_send()
    block_copy.wait_recv()
    prepare(other, 1 - core)
    block_copy.wait_send()
    for stream in streams:
        stream.col_gather.finish()

    runs = [stream.run() for stream in streams]
    for _ in range(LEAD):
        next(runs[0])
    going = True
    while going:
        going = False
        for run in runs:
            if next(run, "end") != "end":
                going = True

    def trade(piece, land):
        land[1] = piece.T
        rows_there = pl.ds(pl.multiple_of((1 - core) * slab, slab), slab)
        copy = copies.make(land.at[1, rows_there, :], land.at[0, rows_there, :], copies.reserve(1), mate)
        copy.start()
        return copy

    first_copy = trade(first_part[...], first_land)
    last_copy = trade(col_prev[...], last_land)

    image_land[2, :, :] = row_parts[y, z].T
    image_slots = copies.reserve(2)
    keep = pl.ds(pl.multiple_of(core * slab, slab), slab)
    give = pl.ds(pl.multiple_of((1 - core) * slab, slab), slab)
    top = pl.ds(0, slab)
    same = copies.make(image_land.at[2, keep, :], image_land.at[0, top, :], image_slots, device(z, core, y, x))
    cross = copies.make(image_land.at[2, give, :], image_land.at[1, top, :], image_slots + 1, device(z, 1 - core, y, x))
    cross.start()

    @pl.when(crossed)
    def _():
        same.start()
        same.wait()

    @pl.when(jnp.logical_not(crossed))
    def _():
        image_land[0, top, :] = image_land[2, keep, :]

    for copy, land, out_ref in ((first_copy, first_land, first_ref), (last_copy, last_land, last_ref)):
        copy.wait()
        out_ref[:, mine_cols] = land[1, keep, :]
        out_ref[:, mate_cols] = land[0, keep, :]
    cross.wait()
    image_ref[:, mine_cols] = image_land[0, top, :]
    image_ref[:, mate_cols] = image_land[1, top, :]


def filtered_blocks(matrix, start_vectors, interval):
    block_rows, block_cols = matrix.shape
    slab, vectors = start_vectors.shape
    width = vectors // 2
    share = width // STREAMS
    f32, bf16 = jnp.float32, jnp.bfloat16
    vmem = pl.BlockSpec(memory_space=pltpu.VMEM)
    return pl.pallas_call(
        filter_kernel,
        out_shape=[jax.ShapeDtypeStruct((slab, vectors), f32)] * 3,
        in_specs=[pl.BlockSpec(memory_space=pltpu.SMEM), pl.BlockSpec(memory_space=pl.ANY), vmem],
        out_specs=[vmem] * 3,
        scratch_shapes=[
            pltpu.VMEM((block_rows, block_cols), f32),
            pltpu.VMEM((block_rows, block_cols), f32),
            pltpu.VMEM((2 * block_rows, block_cols), bf16),
            pltpu.VMEM((2 * block_rows, block_cols), bf16),
            pltpu.VMEM((4, 4, width, CHUNK), f32),
            pltpu.VMEM((4, 4, width, CHUNK), f32),
            pltpu.VMEM((4, width, CHUNK), f32),
            pltpu.VMEM((4, width, CHUNK), f32),
            pltpu.VMEM((width, block_cols), bf16),
            pltpu.VMEM((width, block_cols), bf16),
            pltpu.VMEM((STREAMS, 2, 6, 4, share // 4, CHUNK), f32),
            pltpu.VMEM((STREAMS, 2, 6, share // 4, CHUNK), f32),
            pltpu.VMEM((STREAMS, 6, share // 2, CHUNK), f32),
            pltpu.VMEM((width, CHUNK), f32),
            pltpu.VMEM((width, CHUNK), f32),
            pltpu.VMEM((width, CHUNK), f32),
            pltpu.VMEM((slab, width), f32),
            pltpu.VMEM((2, CHUNK, width), f32),
            pltpu.VMEM((2, CHUNK, width), f32),
            pltpu.VMEM((3, CHUNK, width), f32),
            pltpu.SemaphoreType.DMA((112,)),
            pltpu.SemaphoreType.DMA((112,)),
            pltpu.SemaphoreType.DMA,
        ],
        compiler_params=pltpu.CompilerParams(
            collective_id=0, has_side_effects=True, vmem_limit_bytes=50 * 2**20
        ),
        cost_estimate=pl.CostEstimate(flops=10**10, bytes_accessed=4 * 10**6, transcendentals=0),
    )(interval, matrix, start_vectors)


class Places:
    def __init__(self):
        self.r, self.c = lax.axis_index("row"), lax.axis_index("col")
        self.core, self.x = self.r % 2, self.r // 2
        self.y, self.z = self.c % 4, self.c // 4
        self.mate = (2 * self.x + 1 - self.core, self.c)
        self.ring_x = ((self.r + 6) % 8, self.c), ((self.r + 2) % 8, self.c)

    def peer(self, offset):
        return self.r, (self.c + offset) % 16


def all_sum(copies, at, total, result, land_core, land_x, land_plane):
    order, width = total.shape
    half, quarter = order // 2, order // 8

    def rows(first, count, ref=total):
        return ref.at[pl.ds(pl.multiple_of(first, 8), count), :]

    mine, theirs = rows(at.core * half, half), rows((1 - at.core) * half, half)
    swap = copies.make(theirs, land_core, copies.reserve(1), at.mate)
    swap.start()
    swap.wait_recv()
    mine[...] += land_core[...]

    def part(t, side, ref=total):
        size = quarter if side is None else quarter // 2
        return rows(at.core * half + t * quarter + (0 if side is None else side * size), size, ref)

    scatter = Scatter(copies, copies.reserve(6), at.x, at.ring_x, part, lambda i: land_x.at[i])
    scatter.start()
    scatter.relay()
    scatter.finish()

    def piece(t, ref=total):
        first = at.core * half + at.x * quarter + 8 * (t // 2)
        lanes = pl.ds(pl.multiple_of((t % 2) * (width // 2), 128), width // 2)
        return ref.at[pl.ds(pl.multiple_of(first, 8), 8), lanes]

    slots = copies.reserve(15), copies.reserve(15)
    sent = []
    for offset in range(1, 16):
        to = (at.c + offset) % 16
        copy = copies.make(piece(to), land_plane.at[offset], slots[0] + offset - 1, at.peer(offset))
        copy.start()
        sent.append(copy)
    own = piece(at.c)
    value = own[...]
    for offset, copy in enumerate(sent, 1):
        copy.wait_recv()
        value = value + land_plane[offset]
    own = piece(at.c, result)
    own[...] = value
    back = []
    for offset in range(1, 16):
        copy = copies.make(own, own, slots[1] + offset - 1, at.peer(offset))
        copy.start()
        back.append(copy)
    for copy in back:
        copy.wait_recv()
    gather = Gather(copies, copies.reserve(4), at.x, at.ring_x, lambda t, side: part(t, side, result))
    gather.start()
    gather.forward()
    gather.finish()
    mine = rows(at.core * half, half, result)
    give = copies.make(mine, mine, copies.reserve(1), at.mate)
    give.start()
    for copy in (swap, *sent, *back):
        copy.wait_send()
    give.wait()


def greet_all(at):
    barrier = pltpu.get_barrier_semaphore()
    others = [at.mate, *at.ring_x] + [at.peer(offset) for offset in range(1, 16)]
    for who in others:
        pl.semaphore_signal(barrier, inc=1, device_id=who, device_id_type=MESH)
    pl.semaphore_wait(barrier, len(others))


def sum_scratch(order, width):
    f32 = jnp.float32
    return [
        pltpu.VMEM((order, width), f32),
        pltpu.VMEM((order, width), f32),
        pltpu.VMEM((order // 2, width), f32),
        pltpu.VMEM((6, order // 16, width), f32),
        pltpu.VMEM((16, 8, width // 2), f32),
        pltpu.VMEM((order, order), f32),
        pltpu.VMEM((128 + PANEL, 256), f32),
        pltpu.VMEM((PANEL, 256), f32),
        pltpu.SemaphoreType.DMA((64,)),
        pltpu.SemaphoreType.DMA((64,)),
    ]


def early_kernel(count, slab_ref, inverse_ref, total, result, land_core, land_x, land_plane, work, tile, pending, send, recv):
    at = Places()
    greet_all(at)
    slab = slab_ref[...]
    total[...] = contract(slab, slab, 0, 0)
    all_sum(Copies(send, recv), at, total, result, land_core, land_x, land_plane)
    result[...] = result[...] / count
    factor_kernel(128, result, inverse_ref, work, tile, pending)


def late_kernel(
    count, slab_ref, image_ref, before_ref, basis_ref, projected_ref, residual_ref,
    inverse_ref, total, result, land_core, land_x, land_plane, work, tile, pending, send, recv,
):
    at = Places()
    greet_all(at)
    order = slab_ref.shape[1]
    slab = contract(slab_ref[...], before_ref[...], 1, 1)
    image = contract(image_ref[...], before_ref[...], 1, 1)
    total[:, :order] = contract(slab, slab, 0, 0)
    total[:, order:] = contract(slab, image, 0, 0)
    all_sum(Copies(send, recv), at, total, result, land_core, land_x, land_plane)
    result[...] = result[...] / count
    factor_kernel(128, result.at[:, :order], inverse_ref, work, tile, pending)
    inverse = inverse_ref[...]
    basis = contract(slab, inverse, 1, 1)
    basis_ref[...] = basis
    projected = contract(product(inverse, result[:, order:]), inverse, 1, 1)
    projected_ref[...] = projected
    residual_ref[...] = contract(image, inverse, 1, 1) - product(basis, projected)


def on_device(matrix, start_vectors, interval):
    slab_rows, vectors = start_vectors.shape
    total_rows = slab_rows * lax.axis_size("row") * lax.axis_size("col")
    early, slab, mapped = filtered_blocks(matrix, start_vectors, interval)

    f32 = jnp.float32
    vmem = pl.BlockSpec(memory_space=pltpu.VMEM)
    square = jax.ShapeDtypeStruct((vectors, vectors), f32)
    tall = jax.ShapeDtypeStruct((slab_rows, vectors), f32)
    cost = pl.CostEstimate(flops=2 * vectors**3, bytes_accessed=8 * vectors**2, transcendentals=vectors)
    before = pl.pallas_call(
        functools.partial(early_kernel, total_rows),
        out_shape=square,
        in_specs=[vmem],
        out_specs=vmem,
        scratch_shapes=sum_scratch(vectors, vectors),
        compiler_params=pltpu.CompilerParams(collective_id=1, has_side_effects=True, vmem_limit_bytes=40 * 2**20),
        cost_estimate=cost,
    )(early)
    return pl.pallas_call(
        functools.partial(late_kernel, total_rows),
        out_shape=(tall, square, tall),
        in_specs=[vmem] * 3,
        out_specs=(vmem,) * 3,
        scratch_shapes=[pltpu.VMEM((vectors, vectors), f32)] + sum_scratch(vectors, 2 * vectors),
        compiler_params=pltpu.CompilerParams(collective_id=2, has_side_effects=True, vmem_limit_bytes=40 * 2**20),
        cost_estimate=cost,
    )(slab, mapped, before)


def solution(mesh):
    return jax.shard_map(
        on_device,
        mesh=mesh,
        in_specs=(P("row", "col"), P(("col", "row"), None), P()),
        out_specs=(P(("col", "row"), None), P(), P(("col", "row"), None)),
        check_vma=False,
    )
```

```python
import functools

import jax
import jax.numpy as jnp
from jax import lax
from jax.experimental import pallas as pl
from jax.experimental.pallas import tpu as pltpu
from jax.sharding import PartitionSpec as P

FILTER_DEG = 3
OUTER = 2
PANEL = 8
BLOCK = 128
MESH = pl.DeviceIdType.MESH
CHUNK = 128


def product(left, right, precision=lax.Precision.HIGHEST):
    return jnp.dot(left, right, precision=precision, preferred_element_type=jnp.float32)


def contract(left, right, left_dim, right_dim):
    return lax.dot_general(
        left,
        right,
        (((left_dim,), (right_dim,)), ((), ())),
        precision=lax.Precision.HIGHEST,
        preferred_element_type=jnp.float32,
    )


def lane_columns(rows, first):
    narrow = rows[:, :128]
    lanes = jnp.zeros((PANEL, 128), jnp.int32) + first
    return [jnp.take_along_axis(narrow, lanes + j, axis=1) for j in range(PANEL)]


def row_of(value, step):
    return jnp.broadcast_to(value[step : step + 1, :], value.shape)


def factor_panels(tile, pending, begin, end):
    block = tile.shape[1] // 2
    sub = lax.broadcasted_iota(jnp.int32, (PANEL, 128), 0)
    lane = lax.broadcasted_iota(jnp.int32, (PANEL, block), 1)

    def panel(p, carry):
        first = pl.multiple_of(p * PANEL, PANEL)
        here, after = pl.ds(first, PANEL), pl.ds(pl.multiple_of(first + PANEL, PANEL), PANEL)
        rows = tile[here, :]
        late = pending[...]
        tile[:block, :] -= contract(jnp.where(lane >= first + PANEL, late[:, :block], 0.0), late, 0, 0)

        columns = lane_columns(rows, first)
        left, right = rows[:, :block], rows[:, block:]
        inverses = []
        pivots = jnp.ones((PANEL, 128), jnp.float32)
        for s in range(PANEL):
            pivot = row_of(columns[s], s)
            pivots = jnp.where(sub == s, pivot, pivots)
            inverse = 1.0 / pivot
            inverses.append(inverse)
            if s < PANEL - 1:
                ratio = jnp.where(sub > s, columns[s] * inverse, 0.0)
                for j in range(s + 1, PANEL):
                    columns[j] = columns[j] - ratio * row_of(columns[j], s)
                left = left - ratio * row_of(left, s)
                right = right - ratio * row_of(right, s)

        following = tile[after, :]
        others = lane_columns(following, first)
        next_left, next_right = following[:, :block], following[:, block:]
        for s in range(PANEL):
            ratio = others[s] * inverses[s]
            for j in range(s + 1, PANEL):
                others[j] = others[j] - ratio * row_of(columns[j], s)
            next_left = next_left - ratio * row_of(left, s)
            next_right = next_right - ratio * row_of(right, s)
        tile[after, :block] = next_left
        tile[after, block:] = next_right
        scale = lax.rsqrt(pivots)
        left, right = left * scale, right * scale
        tile[here, :block] = left
        tile[here, block:] = right
        pending[:, :block] = left
        pending[:, block:] = right
        return carry

    lax.fori_loop(begin, end, panel, 0)


def factor_steps(pieces, work, inverse_ref, tile, pending):
    order, block = work.shape[0], BLOCK
    at_row = lax.broadcasted_iota(jnp.int32, (order, order), 0)
    at_col = lax.broadcasted_iota(jnp.int32, (order, order), 1)
    inverse_ref[...] = (at_row == at_col).astype(jnp.float32)
    row = lax.broadcasted_iota(jnp.int32, (block, block), 0)
    col = lax.broadcasted_iota(jnp.int32, (block, block), 1)
    panels = block // PANEL
    for at in range(0, order, block):
        stop = at + block
        tile[:block, :block] = work[at:stop, at:stop]
        tile[:block, block:] = (row == col).astype(jnp.float32)
        tile[block:, :] = jnp.zeros((PANEL, 2 * block), jnp.float32)
        pending[...] = jnp.zeros_like(pending)
        for piece in range(pieces):
            factor_panels(tile, pending, piece * panels // pieces, (piece + 1) * panels // pieces)
            yield
        small = jnp.where(row >= col, tile[:block, block:], 0.0)
        solved = product(small, inverse_ref[at:stop, :stop])
        inverse_ref[at:stop, :stop] = solved
        if stop < order:
            below = contract(work[stop:, at:stop], small, 1, 1)
            work[stop:, stop:] -= contract(below, below, 1, 1)
            inverse_ref[stop:, :stop] -= product(below, solved)
            yield


class Copies:
    def __init__(self, send, recv):
        self.send, self.recv, self.used = send, recv, 0

    def reserve(self, count):
        first = self.used
        self.used += count
        return first

    def make(self, source, target, slot, device):
        return pltpu.make_async_remote_copy(
            src_ref=source,
            dst_ref=target,
            send_sem=self.send.at[slot],
            recv_sem=self.recv.at[slot],
            device_id=device,
            device_id_type=MESH,
        )


class Scatter:
    def __init__(self, copies, slot, place, ring, part, land):
        self.place, self.part, self.land = place, part, land
        left, right = ring
        ahead, behind, across = (place + 1) % 4, (place + 3) % 4, (place + 2) % 4
        self.ahead, self.behind = ahead, behind
        plan = (
            (part(across, 0), right),
            (part(across, 1), left),
            (part(ahead, 1), right),
            (part(behind, 0), left),
            (part(ahead, 0), right),
            (part(behind, 1), left),
        )
        self.copies = [
            copies.make(source, land(i), slot + i, device) for i, (source, device) in enumerate(plan)
        ]

    def start(self):
        for copy in self.copies[:4]:
            copy.start()

    def relay(self):
        for first, half, target in ((0, 0, self.ahead), (1, 1, self.behind)):
            self.copies[first].wait_recv()
            mine = self.part(target, half)
            mine[...] += self.land(first)[...]
            self.copies[4 + first].start()

    def finish(self):
        for copy in self.copies[2:]:
            copy.wait_recv()
        for half, terms in ((0, (3, 4)), (1, (2, 5))):
            mine = self.part(self.place, half)
            mine[...] += self.land(terms[0])[...] + self.land(terms[1])[...]
        for copy in self.copies:
            copy.wait_send()


class Gather:
    def __init__(self, copies, slot, place, ring, part):
        left, right = ring
        ahead, behind = (place + 1) % 4, (place + 3) % 4
        self.copies = [
            copies.make(part(place, None), part(place, None), slot, right),
            copies.make(part(place, None), part(place, None), slot + 1, left),
            copies.make(part(behind, 0), part(behind, 0), slot + 2, right),
            copies.make(part(ahead, 1), part(ahead, 1), slot + 3, left),
        ]

    def start(self):
        for copy in self.copies[:2]:
            copy.start()

    def forward(self):
        for first in range(2):
            self.copies[first].wait_recv()
            self.copies[2 + first].start()

    def finish(self):
        for copy in self.copies[2:]:
            copy.wait_recv()
        for copy in self.copies:
            copy.wait_send()


def split(value):
    high = value.astype(jnp.bfloat16)
    return high, (value - high.astype(jnp.float32)).astype(jnp.bfloat16)


def three_pass(left, right, dims):
    def one(a, b):
        return lax.dot_general(a, b, (dims, ((), ())), preferred_element_type=jnp.float32)

    return one(left[0], right[0]) + (one(left[0], right[1]) + one(left[1], right[0]))


class TotalSum:
    def __init__(self, copies, position, mate, ring_x, peers, buffers):
        core, x, c = position
        self.total, self.result, self.land_core, land_x, self.land_plane = buffers
        order, width = self.total.shape
        half, quarter = order // 2, order // 8

        def rows(ref, first, count):
            return ref.at[pl.ds(pl.multiple_of(first, 8), count), :]

        def part(ref):
            def one(t, side):
                size = quarter if side is None else quarter // 2
                return rows(ref, core * half + t * quarter + (0 if side is None else side * size), size)
            return one

        def piece(ref, t):
            first = core * half + x * quarter + 8 * (t // 2)
            lanes = pl.ds(pl.multiple_of((t % 2) * (width // 2), 128), width // 2)
            return ref.at[pl.ds(pl.multiple_of(first, 8), 8), lanes]

        self.mine = rows(self.total, core * half, half)
        self.swap = copies.make(rows(self.total, (1 - core) * half, half), self.land_core, copies.reserve(1), mate)
        self.scatter = Scatter(copies, copies.reserve(6), x, ring_x, part(self.total), lambda i: land_x.at[i])
        self.own, self.summed = piece(self.total, c), piece(self.result, c)
        self.there, self.back = [], []
        for offset, peer in peers:
            source, target = piece(self.total, (c + offset) % 16), self.land_plane.at[offset]
            self.there.append(copies.make(source, target, copies.reserve(1), peer))
            self.back.append(copies.make(self.summed, self.summed, copies.reserve(1), peer))
        self.gather = Gather(copies, copies.reserve(4), x, ring_x, part(self.result))
        whole = rows(self.result, core * half, half)
        self.give = copies.make(whole, whole, copies.reserve(1), mate)

    def steps(self):
        self.swap.start()
        yield
        self.swap.wait_recv()
        self.mine[...] += self.land_core[...]
        self.scatter.start()
        yield
        self.scatter.relay()
        yield
        self.scatter.finish()
        for copy in self.there:
            copy.start()
        yield
        value = self.own[...]
        for offset, copy in enumerate(self.there, 1):
            copy.wait_recv()
            value = value + self.land_plane[offset]
        self.summed[...] = value
        for copy in self.back:
            copy.start()
        yield
        for copy in self.back:
            copy.wait_recv()
        self.gather.start()
        yield
        self.gather.forward()
        yield
        self.gather.finish()
        self.give.start()
        for copy in (self.swap, *self.there, *self.back):
            copy.wait_send()
        yield
        self.give.wait()


STREAMS = 2


def whole_kernel(
    count, interval_ref, block_ref, start_ref, basis_ref, projected_ref, residual_ref,
    block, other, high, low, rows, row_parts, cols, col_parts, vec_high, vec_low,
    land_big, land_small, land_col, row_prev, col_prev, first_part,
    start_land, first_land, last_land, image_land, slab_ref, image_ref, before_ref, inverse_ref,
    *rest,
):
    sum_buffers = [rest[5 * k : 5 * k + 5] for k in range(3)]
    tile, pending, send, recv, local_sem = rest[15:]
    r, c = lax.axis_index("row"), lax.axis_index("col")
    core, x, y, z = r % 2, r // 2, c % 4, c // 4
    copies = Copies(send, recv)

    def device(x, core, y, z):
        return (2 * x + core, 4 * z + y)

    mate = device(x, 1 - core, y, z)
    ring_x = device((x + 3) % 4, core, y, z), device((x + 1) % 4, core, y, z)
    ring_y = device(x, core, (y + 3) % 4, z), device(x, core, (y + 1) % 4, z)
    ring_z = device(x, core, y, (z + 3) % 4), device(x, core, y, (z + 1) % 4)
    crossed = x != z

    local = pltpu.make_async_copy(block_ref, block, local_sem)
    local.start()
    barrier = pltpu.get_barrier_semaphore()

    def greet(who):
        pl.semaphore_signal(barrier, inc=1, device_id=who, device_id_type=MESH)

    peers = [(offset, (r, (c + offset) % 16)) for offset in range(1, 16)]
    for who in (mate, *ring_x, *(peer for _, peer in peers)):
        greet(who)

    @pl.when(crossed)
    def _():
        greet(device(z, core, y, x))
        greet(device(z, 1 - core, y, x))

    pl.semaphore_wait(barrier, jnp.where(crossed, 20, 18))

    block_rows, block_cols = block.shape
    slab = start_ref.shape[0]
    width = start_ref.shape[1] // 2
    mine_cols = pl.ds(pl.multiple_of(core * width, width), width)
    mate_cols = pl.ds(pl.multiple_of((1 - core) * width, width), width)

    start_copy = copies.make(start_ref.at[:, mate_cols], start_land, copies.reserve(1), mate)
    start_copy.start()
    block_copy = copies.make(block_ref, other, copies.reserve(1), mate)
    block_copy.start()

    lower_end = jnp.full((1, block_cols), interval_ref[0], jnp.float32)
    upper_end = jnp.full((1, block_cols), interval_ref[1], jnp.float32)
    center = 0.5 * (lower_end + upper_end)
    inverse_width = 1.0 / (0.5 * (upper_end - lower_end))

    def prepare(source, which):
        base = which * block_rows
        step = 256

        @pl.loop(0, block_rows // step)
        def _(i):
            at = pl.multiple_of(i * step, step)
            value = source[pl.ds(at, step), :]
            row = lax.broadcasted_iota(jnp.int32, value.shape, 0) + (2 * x * block_rows + base + at)
            col = lax.broadcasted_iota(jnp.int32, value.shape, 1) + c * block_cols
            value = jnp.where(row == col, value - center, value) * inverse_width
            big, small = split(value)
            to = pl.ds(pl.multiple_of(base + at, step), step)
            high[to, :] = big
            low[to, :] = small

    start_copy.wait_recv()
    own = start_ref[:, mine_cols]
    theirs = start_land[...]
    lower = jnp.where(core == 0, own, theirs)
    upper = jnp.where(core == 0, theirs, own)
    piece = jnp.concatenate([lower, upper], axis=0).T
    cols[x] = piece
    col_prev[...] = piece

    places = {"y": y, "z": z}
    rings = {"y": ring_y, "z": ring_z}
    orders = (("z", "y"), ("y", "z"))
    share = width // STREAMS
    half = share // 2

    class Stream:
        def __init__(self, index):
            self.base = index * share
            self.at_first = self.at_last = False
            self.all = pl.ds(self.base, share)
            slots = [[copies.reserve(6) for _ in range(2)] for _ in range(2)]
            self.scatters = [[self.scatter(index, u, stage, slots[u][stage]) for stage in range(2)] for u in range(2)]
            slots = [[copies.reserve(4) for _ in range(2)] for _ in range(2)]
            self.gathers = [[self.gather(u, stage, slots[u][stage]) for stage in range(2)] for u in range(2)]
            self.col_scatter = Scatter(
                copies, copies.reserve(6), x, ring_x, self.col_slice(col_parts), lambda i: land_col.at[index, i]
            )
            self.col_gather = Gather(copies, copies.reserve(4), x, ring_x, self.col_slice(cols))

        def span(self, colour, side):
            size = half if side is None else half // 2
            return pl.ds(self.base + colour * half + (0 if side is None else side * size), size)

        def col_slice(self, ref):
            def part(t, side):
                return ref.at[t, self.all if side is None else self.span(side, None), :]
            return part

        def plane(self, ref, colour, axis):
            def part(t, side):
                at = self.span(colour, side)
                return ref.at[:, t, at, :] if axis == "z" else ref.at[t, :, at, :]
            return part

        def line(self, ref, colour, axis):
            def part(t, side):
                at = self.span(colour, side)
                return ref.at[y, t, at, :] if axis == "z" else ref.at[t, z, at, :]
            return part

        def scatter(self, index, colour, stage, slot):
            axis = orders[colour][stage]
            part = (self.plane if stage == 0 else self.line)(row_parts, colour, axis)
            landing = land_big if stage == 0 else land_small
            return Scatter(copies, slot, places[axis], rings[axis], part, lambda i: landing.at[index, colour, i])

        def gather(self, colour, stage, slot):
            axis = orders[colour][1 - stage]
            part = (self.line if stage == 0 else self.plane)(rows, colour, axis)
            return Gather(copies, slot, places[axis], rings[axis], part)

        def multiply(self):
            for q in range(4):
                big, small = split(cols[q, self.all, :])
                vec_high[self.all, q * CHUNK : (q + 1) * CHUNK] = big
                vec_low[self.all, q * CHUNK : (q + 1) * CHUNK] = small

            @pl.loop(0, 8)
            def _(i):
                at = pl.ds(pl.multiple_of(i * 256, 256), 256)
                left = vec_high[self.all, :], vec_low[self.all, :]
                out = three_pass(left, (high[at, :], low[at, :]), ((1,), (1,)))
                row_parts[i // 2, 2 * (i % 2), self.all, :] = out[:, :CHUNK]
                row_parts[i // 2, 2 * (i % 2) + 1, self.all, :] = out[:, CHUNK:]

        def multiply_turned(self):
            for q in range(4):
                col_parts[q, self.all, :] = jnp.zeros((share, CHUNK), jnp.float32)

            @pl.loop(0, 8)
            def _(i):
                at = pl.ds(pl.multiple_of(i * 256, 256), 256)
                pair = [rows[i // 2, 2 * (i % 2) + k, self.all, :] for k in range(2)]
                out = three_pass(split(jnp.concatenate(pair, axis=1)), (high[at, :], low[at, :]), ((1,), (0,)))
                for q in range(4):
                    col_parts[q, self.all, :] += out[:, q * CHUNK : (q + 1) * CHUNK]

        def to_rows(self):
            self.multiply()
            firsts = [self.scatters[0][0], self.scatters[1][0]]
            seconds = [self.scatters[0][1], self.scatters[1][1]]
            for first in firsts:
                first.start()
            yield
            for first in firsts:
                first.relay()
            yield
            for first, second in zip(firsts, seconds):
                first.finish()
                second.start()
            yield
            for second in seconds:
                second.relay()
            yield

        def run(self):
            for step in range(3):
                yield from self.to_rows()
                for colour in range(2):
                    self.scatters[colour][1].finish()
                    at = self.span(colour, None)
                    value = row_parts[y, z, at, :]
                    if step > 0:
                        value = 2.0 * value - row_prev[at, :]
                    rows[y, z, at, :] = value
                    row_prev[at, :] = value
                    if step == 1:
                        first_part[at, :] = value
                    self.gathers[colour][0].start()
                self.at_first = step >= 1
                yield
                for colour in range(2):
                    self.gathers[colour][0].forward()
                yield
                for colour in range(2):
                    self.gathers[colour][0].finish()
                    self.gathers[colour][1].start()
                yield
                for colour in range(2):
                    self.gathers[colour][1].forward()
                yield
                for colour in range(2):
                    self.gathers[colour][1].finish()
                self.multiply_turned()
                self.col_scatter.start()
                yield
                self.col_scatter.relay()
                yield
                self.col_scatter.finish()
                value = col_parts[x, self.all, :]
                if step != 1:
                    value = 2.0 * value - col_prev[self.all, :]
                cols[x, self.all, :] = value
                col_prev[self.all, :] = value
                self.col_gather.start()
                self.at_last = step == 2
                yield
                self.col_gather.forward()
                yield
                self.col_gather.finish()
            yield from self.to_rows()
            for colour in range(2):
                self.scatters[colour][1].finish()

    streams = [Stream(index) for index in range(STREAMS)]
    for stream in streams:
        stream.col_gather.start()
    local.wait()
    prepare(block, core)
    for stream in streams:
        stream.col_gather.forward()
    start_copy.wait_send()
    block_copy.wait_recv()
    prepare(other, 1 - core)
    block_copy.wait_send()
    for stream in streams:
        stream.col_gather.finish()

    keep = pl.ds(pl.multiple_of(core * slab, slab), slab)
    give = pl.ds(pl.multiple_of((1 - core) * slab, slab), slab)
    top = pl.ds(0, slab)
    sums = [TotalSum(copies, (core, x, c), mate, ring_x, peers, buffers) for buffers in sum_buffers]

    def trade(piece, land, target):
        land[1] = piece.T
        copy = copies.make(land.at[1, give, :], land.at[0, give, :], copies.reserve(1), mate)
        copy.start()
        yield
        copy.wait()
        target[:, mine_cols] = land[1, keep, :]
        target[:, mate_cols] = land[0, keep, :]

    def first_chain():
        yield from trade(first_part[...], first_land, slab_ref)
        sums[0].total[...] = contract(slab_ref[...], slab_ref[...], 0, 0)
        yield from sums[0].steps()
        sums[0].total[...] = sums[0].result[...] / count
        yield from factor_steps(2, sums[0].total, before_ref, tile, pending)

    def last_chain():
        yield from trade(col_prev[...], last_land, slab_ref)
        slab_ref[...] = contract(slab_ref[...], before_ref[...], 1, 1)
        sums[1].total[...] = contract(slab_ref[...], slab_ref[...], 0, 0)
        yield from sums[1].steps()
        sums[1].total[...] = sums[1].result[...] / count
        yield from factor_steps(2, sums[1].total, inverse_ref, tile, pending)

    def image_chain():
        image_land[2, :, :] = row_parts[y, z].T
        slots = copies.reserve(2)
        same = copies.make(image_land.at[2, keep, :], image_land.at[0, top, :], slots, device(z, core, y, x))
        cross = copies.make(image_land.at[2, give, :], image_land.at[1, top, :], slots + 1, device(z, 1 - core, y, x))
        cross.start()

        @pl.when(crossed)
        def _():
            same.start()

        yield

        @pl.when(crossed)
        def _():
            same.wait()

        @pl.when(jnp.logical_not(crossed))
        def _():
            image_land[0, top, :] = image_land[2, keep, :]

        cross.wait()
        image_ref[:, mine_cols] = image_land[0, top, :]
        image_ref[:, mate_cols] = image_land[1, top, :]
        image_ref[...] = contract(image_ref[...], before_ref[...], 1, 1)
        sums[2].total[...] = contract(slab_ref[...], image_ref[...], 0, 0)
        yield from sums[2].steps()

    def advance(chain):
        return next(chain, "end") != "end"

    runs = [stream.run() for stream in streams]
    chains, begun = [], 0
    going = True
    while going:
        going = False
        for run in runs:
            going = advance(run) or going
            if chains and not advance(chains[0]):
                chains.pop(0)
        if begun == 0 and all(stream.at_first for stream in streams):
            chains.append(first_chain())
            begun = 1
        if begun == 1 and all(stream.at_last for stream in streams):
            chains.append(last_chain())
            begun = 2
    while len(chains) > 1:
        if not advance(chains[0]):
            chains.pop(0)
    chains.append(image_chain())
    while chains:
        chains = [chain for chain in reversed(chains) if advance(chain)][::-1]

    inverse = inverse_ref[...]
    basis = contract(slab_ref[...], inverse, 1, 1)
    basis_ref[...] = basis
    projected = contract(product(inverse, sums[2].result[...] / count), inverse, 1, 1)
    projected_ref[...] = projected
    residual_ref[...] = contract(image_ref[...], inverse, 1, 1) - product(basis, projected)


def on_device(matrix, start_vectors, interval):
    block_rows, block_cols = matrix.shape
    slab, vectors = start_vectors.shape
    total_rows = slab * lax.axis_size("row") * lax.axis_size("col")
    width = vectors // 2
    share = width // STREAMS
    f32, bf16 = jnp.float32, jnp.bfloat16
    vmem = pl.BlockSpec(memory_space=pltpu.VMEM)
    tall = jax.ShapeDtypeStruct((slab, vectors), f32)
    square = jax.ShapeDtypeStruct((vectors, vectors), f32)
    one_sum = [
        pltpu.VMEM((vectors, vectors), f32),
        pltpu.VMEM((vectors, vectors), f32),
        pltpu.VMEM((vectors // 2, vectors), f32),
        pltpu.VMEM((6, vectors // 16, vectors), f32),
        pltpu.VMEM((16, 8, vectors // 2), f32),
    ]
    return pl.pallas_call(
        functools.partial(whole_kernel, total_rows),
        out_shape=(tall, square, tall),
        in_specs=[pl.BlockSpec(memory_space=pltpu.SMEM), pl.BlockSpec(memory_space=pl.ANY), vmem],
        out_specs=(vmem,) * 3,
        scratch_shapes=[
            pltpu.VMEM((block_rows, block_cols), f32),
            pltpu.VMEM((block_rows, block_cols), f32),
            pltpu.VMEM((2 * block_rows, block_cols), bf16),
            pltpu.VMEM((2 * block_rows, block_cols), bf16),
            pltpu.VMEM((4, 4, width, CHUNK), f32),
            pltpu.VMEM((4, 4, width, CHUNK), f32),
            pltpu.VMEM((4, width, CHUNK), f32),
            pltpu.VMEM((4, width, CHUNK), f32),
            pltpu.VMEM((width, block_cols), bf16),
            pltpu.VMEM((width, block_cols), bf16),
            pltpu.VMEM((STREAMS, 2, 6, 4, share // 4, CHUNK), f32),
            pltpu.VMEM((STREAMS, 2, 6, share // 4, CHUNK), f32),
            pltpu.VMEM((STREAMS, 6, share // 2, CHUNK), f32),
            pltpu.VMEM((width, CHUNK), f32),
            pltpu.VMEM((width, CHUNK), f32),
            pltpu.VMEM((width, CHUNK), f32),
            pltpu.VMEM((slab, width), f32),
            pltpu.VMEM((2, CHUNK, width), f32),
            pltpu.VMEM((2, CHUNK, width), f32),
            pltpu.VMEM((3, CHUNK, width), f32),
            pltpu.VMEM((slab, vectors), f32),
            pltpu.VMEM((slab, vectors), f32),
            pltpu.VMEM((vectors, vectors), f32),
            pltpu.VMEM((vectors, vectors), f32),
            *(one_sum * 3),
            pltpu.VMEM((BLOCK + PANEL, 2 * BLOCK), f32),
            pltpu.VMEM((PANEL, 2 * BLOCK), f32),
            pltpu.SemaphoreType.DMA((256,)),
            pltpu.SemaphoreType.DMA((256,)),
            pltpu.SemaphoreType.DMA,
        ],
        compiler_params=pltpu.CompilerParams(
            collective_id=0, has_side_effects=True, vmem_limit_bytes=56 * 2**20
        ),
        cost_estimate=pl.CostEstimate(flops=10**10, bytes_accessed=4 * 10**6, transcendentals=0),
    )(interval, matrix, start_vectors)


def solution(mesh):
    return jax.shard_map(
        on_device,
        mesh=mesh,
        in_specs=(P("row", "col"), P(("col", "row"), None), P()),
        out_specs=(P(("col", "row"), None), P(), P(("col", "row"), None)),
        check_vma=False,
    )
```

```python
import functools

import jax
import jax.numpy as jnp
from jax import lax
from jax.experimental import pallas as pl
from jax.experimental.pallas import tpu as pltpu
from jax.sharding import PartitionSpec as P

FILTER_DEG = 3
OUTER = 2
PANEL = 16
BLOCK = 128
MESH = pl.DeviceIdType.MESH
CHUNK = 128


def product(left, right, precision=lax.Precision.HIGHEST):
    return jnp.dot(left, right, precision=precision, preferred_element_type=jnp.float32)


def contract(left, right, left_dim, right_dim):
    return lax.dot_general(
        left,
        right,
        (((left_dim,), (right_dim,)), ((), ())),
        precision=lax.Precision.HIGHEST,
        preferred_element_type=jnp.float32,
    )


def lane_columns(rows, first):
    narrow = rows[:, :128]
    lanes = jnp.zeros(narrow.shape, jnp.int32) + first
    return [jnp.take_along_axis(narrow, lanes + j, axis=1) for j in range(PANEL)]


def row_of(value, step):
    return jnp.broadcast_to(value[step : step + 1, :], value.shape)


def three_parts(value):
    high = value.astype(jnp.bfloat16).astype(jnp.float32)
    rest = value - high
    middle = rest.astype(jnp.bfloat16).astype(jnp.float32)
    return high, middle, rest - middle


def factor_panels(tile, pend_left, pend_right, begin, end):
    block = tile.shape[1] // 2
    sub = lax.broadcasted_iota(jnp.int32, (PANEL, 128), 0)
    lane = lax.broadcasted_iota(jnp.int32, (PANEL, block), 1)

    def panel(p, carry):
        first = pl.multiple_of(p * PANEL, PANEL)
        here, after = pl.ds(first, PANEL), pl.ds(pl.multiple_of(first + PANEL, PANEL), PANEL)
        rows = tile[here, :]
        tile[:block, :] -= jnp.dot(pend_left[...], pend_right[...], preferred_element_type=jnp.float32)

        columns = lane_columns(rows, first)
        left, right = rows[:, :block], rows[:, block:]
        inverses = []
        pivots = jnp.ones((PANEL, 128), jnp.float32)
        for s in range(PANEL):
            pivot = row_of(columns[s], s)
            pivots = jnp.where(sub == s, pivot, pivots)
            inverse = 1.0 / pivot
            inverses.append(inverse)
            if s < PANEL - 1:
                ratio = jnp.where(sub > s, columns[s] * inverse, 0.0)
                for j in range(s + 1, PANEL):
                    columns[j] = columns[j] - ratio * row_of(columns[j], s)
                left = left - ratio * row_of(left, s)
                right = right - ratio * row_of(right, s)

        scale = lax.rsqrt(pivots)
        done_left, done_right = left * scale, right * scale
        tile[here, :block] = done_left
        tile[here, block:] = done_right
        a = three_parts(jnp.where(lane >= first + 2 * PANEL, done_left, 0.0))
        pend_left[...] = jnp.concatenate([a[0], a[0], a[1], a[1], a[0], a[2]], axis=0).T.astype(jnp.bfloat16)
        b = three_parts(jnp.concatenate([done_left, done_right], axis=1))
        pend_right[...] = jnp.concatenate([b[0], b[1], b[0], b[1], b[2], b[0]], axis=0).astype(jnp.bfloat16)

        following = tile[after, :]
        others = lane_columns(following, first)
        next_left, next_right = following[:, :block], following[:, block:]
        for s in range(PANEL):
            ratio = others[s] * inverses[s]
            for j in range(s + 1, PANEL):
                others[j] = others[j] - ratio * row_of(columns[j], s)
            next_left = next_left - ratio * row_of(left, s)
            next_right = next_right - ratio * row_of(right, s)
        tile[after, :block] = next_left
        tile[after, block:] = next_right
        return carry

    lax.fori_loop(begin, end, panel, 0)


def factor_steps(pieces, work, inverse_ref, tile, pend_left, pend_right):
    order, block = work.shape[0], BLOCK
    at_row = lax.broadcasted_iota(jnp.int32, (order, order), 0)
    at_col = lax.broadcasted_iota(jnp.int32, (order, order), 1)
    inverse_ref[...] = (at_row == at_col).astype(jnp.float32)
    row = lax.broadcasted_iota(jnp.int32, (block, block), 0)
    col = lax.broadcasted_iota(jnp.int32, (block, block), 1)
    panels = block // PANEL
    for at in range(0, order, block):
        stop = at + block
        tile[:block, :block] = work[at:stop, at:stop]
        tile[:block, block:] = (row == col).astype(jnp.float32)
        tile[block:, :] = jnp.zeros((PANEL, 2 * block), jnp.float32)
        pend_left[...] = jnp.zeros_like(pend_left)
        pend_right[...] = jnp.zeros_like(pend_right)
        for piece in range(pieces):
            factor_panels(tile, pend_left, pend_right, piece * panels // pieces, (piece + 1) * panels // pieces)
            yield
        small = jnp.where(row >= col, tile[:block, block:], 0.0)
        solved = product(small, inverse_ref[at:stop, :stop])
        inverse_ref[at:stop, :stop] = solved
        if stop < order:
            below = contract(work[stop:, at:stop], small, 1, 1)
            work[stop:, stop:] -= contract(below, below, 1, 1)
            inverse_ref[stop:, :stop] -= product(below, solved)
            yield


class Copies:
    def __init__(self, send, recv):
        self.send, self.recv, self.used = send, recv, 0

    def reserve(self, count):
        first = self.used
        self.used += count
        return first

    def make(self, source, target, slot, device):
        return pltpu.make_async_remote_copy(
            src_ref=source,
            dst_ref=target,
            send_sem=self.send.at[slot],
            recv_sem=self.recv.at[slot],
            device_id=device,
            device_id_type=MESH,
        )


class Scatter:
    def __init__(self, copies, slot, place, ring, part, land):
        self.place, self.part, self.land = place, part, land
        left, right = ring
        ahead, behind, across = (place + 1) % 4, (place + 3) % 4, (place + 2) % 4
        self.ahead, self.behind = ahead, behind
        plan = (
            (part(across, 0), right),
            (part(across, 1), left),
            (part(ahead, 1), right),
            (part(behind, 0), left),
            (part(ahead, 0), right),
            (part(behind, 1), left),
        )
        self.copies = [
            copies.make(source, land(i), slot + i, device) for i, (source, device) in enumerate(plan)
        ]

    def start(self):
        for copy in self.copies[:4]:
            copy.start()

    def relay(self):
        for first, half, target in ((0, 0, self.ahead), (1, 1, self.behind)):
            self.copies[first].wait_recv()
            mine = self.part(target, half)
            mine[...] += self.land(first)[...]
            self.copies[4 + first].start()

    def finish(self):
        for copy in self.copies[2:]:
            copy.wait_recv()
        for half, terms in ((0, (3, 4)), (1, (2, 5))):
            mine = self.part(self.place, half)
            mine[...] += self.land(terms[0])[...] + self.land(terms[1])[...]
        for copy in self.copies:
            copy.wait_send()


class Gather:
    def __init__(self, copies, slot, place, ring, part):
        left, right = ring
        ahead, behind = (place + 1) % 4, (place + 3) % 4
        self.copies = [
            copies.make(part(place, None), part(place, None), slot, right),
            copies.make(part(place, None), part(place, None), slot + 1, left),
            copies.make(part(behind, 0), part(behind, 0), slot + 2, right),
            copies.make(part(ahead, 1), part(ahead, 1), slot + 3, left),
        ]

    def start(self):
        for copy in self.copies[:2]:
            copy.start()

    def forward(self):
        for first in range(2):
            self.copies[first].wait_recv()
            self.copies[2 + first].start()

    def finish(self):
        for copy in self.copies[2:]:
            copy.wait_recv()
        for copy in self.copies:
            copy.wait_send()


def split(value):
    high = value.astype(jnp.bfloat16)
    return high, (value - high.astype(jnp.float32)).astype(jnp.bfloat16)


def three_pass(left, right, dims):
    def one(a, b):
        return lax.dot_general(a, b, (dims, ((), ())), preferred_element_type=jnp.float32)

    count = left.shape[0] // 2
    both = one(left, right[0])
    return both[:count] + (both[count:] + one(left[:count], right[1]))


class TotalSum:
    def __init__(self, copies, position, mate, ring_x, peers, buffers):
        core, x, c = position
        self.total, self.result, self.land_core, land_x, self.land_plane = buffers
        order, width = self.total.shape
        half, quarter = order // 2, order // 8

        def rows(ref, first, count):
            return ref.at[pl.ds(pl.multiple_of(first, 8), count), :]

        def part(ref):
            def one(t, side):
                size = quarter if side is None else quarter // 2
                return rows(ref, core * half + t * quarter + (0 if side is None else side * size), size)
            return one

        def piece(ref, t):
            first = core * half + x * quarter + 8 * (t // 2)
            lanes = pl.ds(pl.multiple_of((t % 2) * (width // 2), 128), width // 2)
            return ref.at[pl.ds(pl.multiple_of(first, 8), 8), lanes]

        self.mine = rows(self.total, core * half, half)
        self.swap = copies.make(rows(self.total, (1 - core) * half, half), self.land_core, copies.reserve(1), mate)
        self.scatter = Scatter(copies, copies.reserve(6), x, ring_x, part(self.total), lambda i: land_x.at[i])
        self.own, self.summed = piece(self.total, c), piece(self.result, c)
        self.there, self.back = [], []
        for offset, peer in peers:
            source, target = piece(self.total, (c + offset) % 16), self.land_plane.at[offset]
            self.there.append(copies.make(source, target, copies.reserve(1), peer))
            self.back.append(copies.make(self.summed, self.summed, copies.reserve(1), peer))
        self.gather = Gather(copies, copies.reserve(4), x, ring_x, part(self.result))
        whole = rows(self.result, core * half, half)
        self.give = copies.make(whole, whole, copies.reserve(1), mate)

    def steps(self):
        self.swap.start()
        yield
        self.swap.wait_recv()
        self.mine[...] += self.land_core[...]
        self.scatter.start()
        yield
        self.scatter.relay()
        yield
        self.scatter.finish()
        for copy in self.there:
            copy.start()
        yield
        value = self.own[...]
        for offset, copy in enumerate(self.there, 1):
            copy.wait_recv()
            value = value + self.land_plane[offset]
        self.summed[...] = value
        for copy in self.back:
            copy.start()
        yield
        for copy in self.back:
            copy.wait_recv()
        self.gather.start()
        yield
        self.gather.forward()
        yield
        self.gather.finish()
        self.give.start()
        for copy in (self.swap, *self.there, *self.back):
            copy.wait_send()
        yield
        self.give.wait()


STREAMS = 2


def whole_kernel(
    count, interval_ref, block_ref, start_ref, basis_ref, projected_ref, residual_ref,
    block, other, high, low, rows, row_parts, cols, col_parts, vec,
    land_big, land_small, land_col, row_prev, col_prev, first_part,
    start_land, first_land, last_land, image_land, slab_ref, image_ref, before_ref, inverse_ref,
    *rest,
):
    sum_buffers = [rest[5 * k : 5 * k + 5] for k in range(3)]
    tile, pend_left, pend_right, send, recv, local_sem = rest[15:]
    r, c = lax.axis_index("row"), lax.axis_index("col")
    core, x, y, z = r % 2, r // 2, c % 4, c // 4
    copies = Copies(send, recv)

    def device(x, core, y, z):
        return (2 * x + core, 4 * z + y)

    mate = device(x, 1 - core, y, z)
    ring_x = device((x + 3) % 4, core, y, z), device((x + 1) % 4, core, y, z)
    ring_y = device(x, core, (y + 3) % 4, z), device(x, core, (y + 1) % 4, z)
    ring_z = device(x, core, y, (z + 3) % 4), device(x, core, y, (z + 1) % 4)
    crossed = x != z

    local = pltpu.make_async_copy(block_ref, block, local_sem)
    local.start()
    barrier = pltpu.get_barrier_semaphore()

    def greet(who):
        pl.semaphore_signal(barrier, inc=1, device_id=who, device_id_type=MESH)

    peers = [(offset, (r, (c + offset) % 16)) for offset in range(1, 16)]
    for who in (mate, *ring_x, *(peer for _, peer in peers)):
        greet(who)

    @pl.when(crossed)
    def _():
        greet(device(z, core, y, x))
        greet(device(z, 1 - core, y, x))

    pl.semaphore_wait(barrier, jnp.where(crossed, 20, 18))

    block_rows, block_cols = block.shape
    slab = start_ref.shape[0]
    width = start_ref.shape[1] // 2
    mine_cols = pl.ds(pl.multiple_of(core * width, width), width)
    mate_cols = pl.ds(pl.multiple_of((1 - core) * width, width), width)

    start_copy = copies.make(start_ref.at[:, mate_cols], start_land, copies.reserve(1), mate)
    start_copy.start()
    block_copy = copies.make(block_ref, other, copies.reserve(1), mate)
    block_copy.start()

    lower_end = jnp.full((1, block_cols), interval_ref[0], jnp.float32)
    upper_end = jnp.full((1, block_cols), interval_ref[1], jnp.float32)
    center = 0.5 * (lower_end + upper_end)
    inverse_width = 1.0 / (0.5 * (upper_end - lower_end))

    def prepare(source, which):
        base = which * block_rows
        step = 256

        @pl.loop(0, block_rows // step)
        def _(i):
            at = pl.multiple_of(i * step, step)
            value = source[pl.ds(at, step), :]
            row = lax.broadcasted_iota(jnp.int32, value.shape, 0) + (2 * x * block_rows + base + at)
            col = lax.broadcasted_iota(jnp.int32, value.shape, 1) + c * block_cols
            value = jnp.where(row == col, value - center, value) * inverse_width
            big, small = split(value)
            to = pl.ds(pl.multiple_of(base + at, step), step)
            high[to, :] = big
            low[to, :] = small

    start_copy.wait_recv()
    own = start_ref[:, mine_cols]
    theirs = start_land[...]
    lower = jnp.where(core == 0, own, theirs)
    upper = jnp.where(core == 0, theirs, own)
    piece = jnp.concatenate([lower, upper], axis=0).T
    cols[x] = piece
    col_prev[...] = piece

    places = {"y": y, "z": z}
    rings = {"y": ring_y, "z": ring_z}
    orders = (("z", "y"), ("y", "z"))
    share = width // STREAMS
    half = share // 2

    class Stream:
        def __init__(self, index):
            self.base = index * share
            self.at_first = self.at_last = False
            self.all = pl.ds(self.base, share)
            slots = [[copies.reserve(6) for _ in range(2)] for _ in range(2)]
            self.scatters = [[self.scatter(index, u, stage, slots[u][stage]) for stage in range(2)] for u in range(2)]
            slots = [[copies.reserve(4) for _ in range(2)] for _ in range(2)]
            self.gathers = [[self.gather(u, stage, slots[u][stage]) for stage in range(2)] for u in range(2)]
            self.col_scatter = Scatter(
                copies, copies.reserve(6), x, ring_x, self.col_slice(col_parts), lambda i: land_col.at[index, i]
            )
            self.col_gather = Gather(copies, copies.reserve(4), x, ring_x, self.col_slice(cols))

        def span(self, colour, side):
            size = half if side is None else half // 2
            return pl.ds(self.base + colour * half + (0 if side is None else side * size), size)

        def col_slice(self, ref):
            def part(t, side):
                return ref.at[t, self.all if side is None else self.span(side, None), :]
            return part

        def plane(self, ref, colour, axis):
            def part(t, side):
                at = self.span(colour, side)
                return ref.at[:, t, at, :] if axis == "z" else ref.at[t, :, at, :]
            return part

        def line(self, ref, colour, axis):
            def part(t, side):
                at = self.span(colour, side)
                return ref.at[y, t, at, :] if axis == "z" else ref.at[t, z, at, :]
            return part

        def scatter(self, index, colour, stage, slot):
            axis = orders[colour][stage]
            part = (self.plane if stage == 0 else self.line)(row_parts, colour, axis)
            landing = land_big if stage == 0 else land_small
            return Scatter(copies, slot, places[axis], rings[axis], part, lambda i: landing.at[index, colour, i])

        def gather(self, colour, stage, slot):
            axis = orders[colour][1 - stage]
            part = (self.line if stage == 0 else self.plane)(rows, colour, axis)
            return Gather(copies, slot, places[axis], rings[axis], part)

        def multiply(self):
            for q in range(4):
                big, small = split(cols[q, self.all, :])
                vec[:share, q * CHUNK : (q + 1) * CHUNK] = big
                vec[share:, q * CHUNK : (q + 1) * CHUNK] = small

            @pl.loop(0, 8, unroll=4)
            def _(i):
                at = pl.ds(pl.multiple_of(i * 256, 256), 256)
                out = three_pass(vec[...], (high[at, :], low[at, :]), ((1,), (1,)))
                row_parts[i // 2, 2 * (i % 2), self.all, :] = out[:, :CHUNK]
                row_parts[i // 2, 2 * (i % 2) + 1, self.all, :] = out[:, CHUNK:]

        def multiply_turned(self):
            def one(i):
                at = pl.ds(pl.multiple_of(i * 1024, 1024), 1024)
                wide = jnp.concatenate([rows[2 * i + k // 4, k % 4, self.all, :] for k in range(8)], axis=1)
                left = jnp.concatenate(split(wide), axis=0)
                return three_pass(left, (high[at, :], low[at, :]), ((1,), (0,)))

            out = one(0) + one(1)
            for q in range(4):
                col_parts[q, self.all, :] = out[:, q * CHUNK : (q + 1) * CHUNK]

        def to_rows(self):
            self.multiply()
            firsts = [self.scatters[0][0], self.scatters[1][0]]
            seconds = [self.scatters[0][1], self.scatters[1][1]]
            for first in firsts:
                first.start()
            yield
            for first in firsts:
                first.relay()
            yield
            for first, second in zip(firsts, seconds):
                first.finish()
                second.start()
            yield
            for second in seconds:
                second.relay()
            yield

        def run(self):
            for step in range(3):
                yield from self.to_rows()
                for colour in range(2):
                    self.scatters[colour][1].finish()
                    at = self.span(colour, None)
                    value = row_parts[y, z, at, :]
                    if step > 0:
                        value = 2.0 * value - row_prev[at, :]
                    rows[y, z, at, :] = value
                    row_prev[at, :] = value
                    if step == 1:
                        first_part[at, :] = value
                    self.gathers[colour][0].start()
                self.at_first = step >= 1
                yield
                for colour in range(2):
                    self.gathers[colour][0].forward()
                yield
                for colour in range(2):
                    self.gathers[colour][0].finish()
                    self.gathers[colour][1].start()
                yield
                for colour in range(2):
                    self.gathers[colour][1].forward()
                yield
                for colour in range(2):
                    self.gathers[colour][1].finish()
                self.multiply_turned()
                self.col_scatter.start()
                yield
                self.col_scatter.relay()
                yield
                self.col_scatter.finish()
                value = col_parts[x, self.all, :]
                if step != 1:
                    value = 2.0 * value - col_prev[self.all, :]
                cols[x, self.all, :] = value
                col_prev[self.all, :] = value
                self.col_gather.start()
                self.at_last = step == 2
                yield
                self.col_gather.forward()
                yield
                self.col_gather.finish()
            yield from self.to_rows()
            for colour in range(2):
                self.scatters[colour][1].finish()

    streams = [Stream(index) for index in range(STREAMS)]
    for stream in streams:
        stream.col_gather.start()
    local.wait()
    prepare(block, core)
    for stream in streams:
        stream.col_gather.forward()
    start_copy.wait_send()
    block_copy.wait_recv()
    prepare(other, 1 - core)
    block_copy.wait_send()
    for stream in streams:
        stream.col_gather.finish()

    keep = pl.ds(pl.multiple_of(core * slab, slab), slab)
    give = pl.ds(pl.multiple_of((1 - core) * slab, slab), slab)
    top = pl.ds(0, slab)
    sums = [TotalSum(copies, (core, x, c), mate, ring_x, peers, buffers) for buffers in sum_buffers]

    def trade(piece, land, target):
        land[1] = piece.T
        copy = copies.make(land.at[1, give, :], land.at[0, give, :], copies.reserve(1), mate)
        copy.start()
        yield
        copy.wait()
        target[:, mine_cols] = land[1, keep, :]
        target[:, mate_cols] = land[0, keep, :]

    def first_chain():
        yield from trade(first_part[...], first_land, slab_ref)
        sums[0].total[...] = contract(slab_ref[...], slab_ref[...], 0, 0)
        yield from sums[0].steps()
        sums[0].total[...] = sums[0].result[...] / count
        yield from factor_steps(2, sums[0].total, before_ref, tile, pend_left, pend_right)

    def last_chain():
        yield from trade(col_prev[...], last_land, slab_ref)
        slab_ref[...] = contract(slab_ref[...], before_ref[...], 1, 1)
        sums[1].total[...] = contract(slab_ref[...], slab_ref[...], 0, 0)
        yield from sums[1].steps()
        sums[1].total[...] = sums[1].result[...] / count
        yield from factor_steps(2, sums[1].total, inverse_ref, tile, pend_left, pend_right)

    def image_chain():
        image_land[2, :, :] = row_parts[y, z].T
        slots = copies.reserve(2)
        same = copies.make(image_land.at[2, keep, :], image_land.at[0, top, :], slots, device(z, core, y, x))
        cross = copies.make(image_land.at[2, give, :], image_land.at[1, top, :], slots + 1, device(z, 1 - core, y, x))
        cross.start()

        @pl.when(crossed)
        def _():
            same.start()

        yield

        @pl.when(crossed)
        def _():
            same.wait()

        @pl.when(jnp.logical_not(crossed))
        def _():
            image_land[0, top, :] = image_land[2, keep, :]

        cross.wait()
        image_ref[:, mine_cols] = image_land[0, top, :]
        image_ref[:, mate_cols] = image_land[1, top, :]
        image_ref[...] = contract(image_ref[...], before_ref[...], 1, 1)
        sums[2].total[...] = contract(slab_ref[...], image_ref[...], 0, 0)
        yield from sums[2].steps()

    def advance(chain):
        return next(chain, "end") != "end"

    runs = [stream.run() for stream in streams]
    chains, begun = [], 0
    going = True
    while going:
        going = False
        for run in runs:
            going = advance(run) or going
            if chains and not advance(chains[0]):
                chains.pop(0)
        if begun == 0 and all(stream.at_first for stream in streams):
            chains.append(first_chain())
            begun = 1
        if begun == 1 and all(stream.at_last for stream in streams):
            chains.append(last_chain())
            begun = 2
    while len(chains) > 1:
        if not advance(chains[0]):
            chains.pop(0)
    chains.append(image_chain())
    while chains:
        chains = [chain for chain in reversed(chains) if advance(chain)][::-1]

    inverse = inverse_ref[...]
    basis = contract(slab_ref[...], inverse, 1, 1)
    basis_ref[...] = basis
    projected = contract(product(inverse, sums[2].result[...] / count), inverse, 1, 1)
    projected_ref[...] = projected
    residual_ref[...] = contract(image_ref[...], inverse, 1, 1) - product(basis, projected)


def on_device(matrix, start_vectors, interval):
    block_rows, block_cols = matrix.shape
    slab, vectors = start_vectors.shape
    total_rows = slab * lax.axis_size("row") * lax.axis_size("col")
    width = vectors // 2
    share = width // STREAMS
    f32, bf16 = jnp.float32, jnp.bfloat16
    vmem = pl.BlockSpec(memory_space=pltpu.VMEM)
    tall = jax.ShapeDtypeStruct((slab, vectors), f32)
    square = jax.ShapeDtypeStruct((vectors, vectors), f32)
    one_sum = [
        pltpu.VMEM((vectors, vectors), f32),
        pltpu.VMEM((vectors, vectors), f32),
        pltpu.VMEM((vectors // 2, vectors), f32),
        pltpu.VMEM((6, vectors // 16, vectors), f32),
        pltpu.VMEM((16, 8, vectors // 2), f32),
    ]
    return pl.pallas_call(
        functools.partial(whole_kernel, total_rows),
        out_shape=(tall, square, tall),
        in_specs=[pl.BlockSpec(memory_space=pltpu.SMEM), pl.BlockSpec(memory_space=pl.ANY), vmem],
        out_specs=(vmem,) * 3,
        scratch_shapes=[
            pltpu.VMEM((block_rows, block_cols), f32),
            pltpu.VMEM((block_rows, block_cols), f32),
            pltpu.VMEM((2 * block_rows, block_cols), bf16),
            pltpu.VMEM((2 * block_rows, block_cols), bf16),
            pltpu.VMEM((4, 4, width, CHUNK), f32),
            pltpu.VMEM((4, 4, width, CHUNK), f32),
            pltpu.VMEM((4, width, CHUNK), f32),
            pltpu.VMEM((4, width, CHUNK), f32),
            pltpu.VMEM((2 * share, block_cols), bf16),
            pltpu.VMEM((STREAMS, 2, 6, 4, share // 4, CHUNK), f32),
            pltpu.VMEM((STREAMS, 2, 6, share // 4, CHUNK), f32),
            pltpu.VMEM((STREAMS, 6, share // 2, CHUNK), f32),
            pltpu.VMEM((width, CHUNK), f32),
            pltpu.VMEM((width, CHUNK), f32),
            pltpu.VMEM((width, CHUNK), f32),
            pltpu.VMEM((slab, width), f32),
            pltpu.VMEM((2, CHUNK, width), f32),
            pltpu.VMEM((2, CHUNK, width), f32),
            pltpu.VMEM((3, CHUNK, width), f32),
            pltpu.VMEM((slab, vectors), f32),
            pltpu.VMEM((slab, vectors), f32),
            pltpu.VMEM((vectors, vectors), f32),
            pltpu.VMEM((vectors, vectors), f32),
            *(one_sum * 3),
            pltpu.VMEM((BLOCK + PANEL, 2 * BLOCK), f32),
            pltpu.VMEM((BLOCK, 6 * PANEL), bf16),
            pltpu.VMEM((6 * PANEL, 2 * BLOCK), bf16),
            pltpu.SemaphoreType.DMA((256,)),
            pltpu.SemaphoreType.DMA((256,)),
            pltpu.SemaphoreType.DMA,
        ],
        compiler_params=pltpu.CompilerParams(
            collective_id=0, has_side_effects=True, vmem_limit_bytes=56 * 2**20
        ),
        cost_estimate=pl.CostEstimate(flops=10**10, bytes_accessed=4 * 10**6, transcendentals=0),
    )(interval, matrix, start_vectors)


def solution(mesh):
    return jax.shard_map(
        on_device,
        mesh=mesh,
        in_specs=(P("row", "col"), P(("col", "row"), None), P()),
        out_specs=(P(("col", "row"), None), P(), P(("col", "row"), None)),
        check_vma=False,
    )
```

```python
import functools

import jax
import jax.numpy as jnp
from jax import lax
from jax.experimental import pallas as pl
from jax.experimental.pallas import tpu as pltpu
from jax.sharding import PartitionSpec as P

FILTER_DEG = 3
OUTER = 2
PANEL = 16
BLOCK = 128
MESH = pl.DeviceIdType.MESH
CHUNK = 128


def product(left, right, precision=lax.Precision.HIGHEST):
    return jnp.dot(left, right, precision=precision, preferred_element_type=jnp.float32)


def contract(left, right, left_dim, right_dim):
    return lax.dot_general(
        left,
        right,
        (((left_dim,), (right_dim,)), ((), ())),
        precision=lax.Precision.HIGHEST,
        preferred_element_type=jnp.float32,
    )


def lane_columns(rows, first):
    narrow = rows[:, :128]
    lanes = jnp.zeros(narrow.shape, jnp.int32) + first
    return [jnp.take_along_axis(narrow, lanes + j, axis=1) for j in range(PANEL)]


def row_of(value, step):
    return jnp.broadcast_to(value[step : step + 1, :], value.shape)


def three_parts(value):
    high = value.astype(jnp.bfloat16).astype(jnp.float32)
    rest = value - high
    middle = rest.astype(jnp.bfloat16).astype(jnp.float32)
    return high, middle, rest - middle


def factor_panels(tile, pend_left, pend_right, begin, end):
    block = tile.shape[1] // 2
    sub = lax.broadcasted_iota(jnp.int32, (PANEL, 128), 0)
    lane = lax.broadcasted_iota(jnp.int32, (PANEL, block), 1)

    def panel(p, carry):
        first = pl.multiple_of(p * PANEL, PANEL)
        here, after = pl.ds(first, PANEL), pl.ds(pl.multiple_of(first + PANEL, PANEL), PANEL)
        rows = tile[here, :]
        tile[:block, :] -= jnp.dot(pend_left[...], pend_right[...], preferred_element_type=jnp.float32)

        columns = lane_columns(rows, first)
        left, right = rows[:, :block], rows[:, block:]
        inverses = []
        pivots = jnp.ones((PANEL, 128), jnp.float32)
        for s in range(PANEL):
            pivot = row_of(columns[s], s)
            pivots = jnp.where(sub == s, pivot, pivots)
            inverse = 1.0 / pivot
            inverses.append(inverse)
            if s < PANEL - 1:
                ratio = jnp.where(sub > s, columns[s] * inverse, 0.0)
                for j in range(s + 1, PANEL):
                    columns[j] = columns[j] - ratio * row_of(columns[j], s)
                left = left - ratio * row_of(left, s)
                right = right - ratio * row_of(right, s)

        scale = lax.rsqrt(pivots)
        done_left, done_right = left * scale, right * scale
        tile[here, :block] = done_left
        tile[here, block:] = done_right
        a = three_parts(jnp.where(lane >= first + 2 * PANEL, done_left, 0.0))
        pend_left[...] = jnp.concatenate([a[0], a[0], a[1], a[1], a[0], a[2]], axis=0).T.astype(jnp.bfloat16)
        b = three_parts(jnp.concatenate([done_left, done_right], axis=1))
        pend_right[...] = jnp.concatenate([b[0], b[1], b[0], b[1], b[2], b[0]], axis=0).astype(jnp.bfloat16)

        following = tile[after, :]
        others = lane_columns(following, first)
        next_left, next_right = following[:, :block], following[:, block:]
        for s in range(PANEL):
            ratio = others[s] * inverses[s]
            for j in range(s + 1, PANEL):
                others[j] = others[j] - ratio * row_of(columns[j], s)
            next_left = next_left - ratio * row_of(left, s)
            next_right = next_right - ratio * row_of(right, s)
        tile[after, :block] = next_left
        tile[after, block:] = next_right
        return carry

    lax.fori_loop(begin, end, panel, 0)


def factor_steps(pieces, work, inverse_ref, tile, pend_left, pend_right):
    order, block = work.shape[0], BLOCK
    at_row = lax.broadcasted_iota(jnp.int32, (order, order), 0)
    at_col = lax.broadcasted_iota(jnp.int32, (order, order), 1)
    inverse_ref[...] = (at_row == at_col).astype(jnp.float32)
    row = lax.broadcasted_iota(jnp.int32, (block, block), 0)
    col = lax.broadcasted_iota(jnp.int32, (block, block), 1)
    panels = block // PANEL
    for at in range(0, order, block):
        stop = at + block
        tile[:block, :block] = work[at:stop, at:stop]
        tile[:block, block:] = (row == col).astype(jnp.float32)
        tile[block:, :] = jnp.zeros((PANEL, 2 * block), jnp.float32)
        pend_left[...] = jnp.zeros_like(pend_left)
        pend_right[...] = jnp.zeros_like(pend_right)
        for piece in range(pieces):
            factor_panels(tile, pend_left, pend_right, piece * panels // pieces, (piece + 1) * panels // pieces)
            yield
        small = jnp.where(row >= col, tile[:block, block:], 0.0)
        solved = product(small, inverse_ref[at:stop, :stop])
        inverse_ref[at:stop, :stop] = solved
        if stop < order:
            below = contract(work[stop:, at:stop], small, 1, 1)
            work[stop:, stop:] -= contract(below, below, 1, 1)
            inverse_ref[stop:, :stop] -= product(below, solved)
            yield


class Copies:
    def __init__(self, send, recv):
        self.send, self.recv, self.used = send, recv, 0

    def reserve(self, count):
        first = self.used
        self.used += count
        return first

    def make(self, source, target, slot, device):
        return pltpu.make_async_remote_copy(
            src_ref=source,
            dst_ref=target,
            send_sem=self.send.at[slot],
            recv_sem=self.recv.at[slot],
            device_id=device,
            device_id_type=MESH,
        )


class Scatter:
    def __init__(self, copies, slot, place, ring, part, land):
        self.place, self.part, self.land = place, part, land
        left, right = ring
        ahead, behind, across = (place + 1) % 4, (place + 3) % 4, (place + 2) % 4
        self.ahead, self.behind = ahead, behind
        plan = (
            (part(across, 0), right),
            (part(across, 1), left),
            (part(ahead, 1), right),
            (part(behind, 0), left),
            (part(ahead, 0), right),
            (part(behind, 1), left),
        )
        self.copies = [
            copies.make(source, land(i), slot + i, device) for i, (source, device) in enumerate(plan)
        ]

    def start(self):
        for copy in self.copies[:4]:
            copy.start()

    def relay(self):
        for first, half, target in ((0, 0, self.ahead), (1, 1, self.behind)):
            self.copies[first].wait_recv()
            mine = self.part(target, half)
            mine[...] += self.land(first)[...]
            self.copies[4 + first].start()

    def finish(self):
        for copy in self.copies[2:]:
            copy.wait_recv()
        for half, terms in ((0, (3, 4)), (1, (2, 5))):
            mine = self.part(self.place, half)
            mine[...] += self.land(terms[0])[...] + self.land(terms[1])[...]
        for copy in self.copies:
            copy.wait_send()


class Gather:
    def __init__(self, copies, slot, place, ring, part):
        left, right = ring
        ahead, behind = (place + 1) % 4, (place + 3) % 4
        self.copies = [
            copies.make(part(place, None), part(place, None), slot, right),
            copies.make(part(place, None), part(place, None), slot + 1, left),
            copies.make(part(behind, 0), part(behind, 0), slot + 2, right),
            copies.make(part(ahead, 1), part(ahead, 1), slot + 3, left),
        ]

    def start(self):
        for copy in self.copies[:2]:
            copy.start()

    def forward(self):
        for first in range(2):
            self.copies[first].wait_recv()
            self.copies[2 + first].start()

    def finish(self):
        for copy in self.copies[2:]:
            copy.wait_recv()
        for copy in self.copies:
            copy.wait_send()


def split(value):
    high = value.astype(jnp.bfloat16)
    return high, (value - high.astype(jnp.float32)).astype(jnp.bfloat16)


def three_pass(left, right, dims):
    def one(a, b):
        return lax.dot_general(a, b, (dims, ((), ())), preferred_element_type=jnp.float32)

    count = left.shape[0] // 2
    both = one(left, right[0])
    return both[:count] + (both[count:] + one(left[:count], right[1]))


class TotalSum:
    def __init__(self, copies, position, mate, peers, x_peers, buffers):
        core, x, c = position
        self.x = x
        self.total, self.result, self.land_core, self.land_plane, self.land_x = buffers
        half = self.total.shape[0] // 2
        size = half // 16

        def rows(ref, first, count):
            return ref.at[pl.ds(pl.multiple_of(first, size), count), :]

        def piece(ref, t):
            return rows(ref, core * half + t * size, size)

        self.mine = rows(self.total, core * half, half)
        self.swap = copies.make(rows(self.total, (1 - core) * half, half), self.land_core, copies.reserve(1), mate)
        self.own, self.summed = piece(self.total, c), piece(self.result, c)
        self.there, self.along, self.back = [], [], []
        for offset, peer in peers:
            source, target = piece(self.total, (c + offset) % 16), self.land_plane.at[offset]
            self.there.append(copies.make(source, target, copies.reserve(1), peer))
            self.back.append(copies.make(self.summed, self.summed, copies.reserve(1), peer))
        for offset, peer in x_peers:
            self.along.append(copies.make(self.land_x.at[0], self.land_x.at[offset], copies.reserve(1), peer))
        whole = rows(self.result, core * half, half)
        self.give = copies.make(whole, whole, copies.reserve(1), mate)

    def steps(self):
        self.swap.start()
        yield
        self.swap.wait_recv()
        self.mine[...] += self.land_core[...]
        for copy in self.there:
            copy.start()
        yield
        value = self.own[...]
        for offset, copy in enumerate(self.there, 1):
            copy.wait_recv()
            value = value + self.land_plane[offset]
        self.land_x[0] = value
        for copy in self.along:
            copy.start()
        yield
        for copy in self.along:
            copy.wait_recv()
        value = self.land_x[self.x % 4]
        for at in range(1, 4):
            value = value + self.land_x[(self.x + 4 - at) % 4]
        self.summed[...] = value
        for copy in self.back:
            copy.start()
        yield
        for copy in self.back:
            copy.wait_recv()
        self.give.start()
        for copy in (self.swap, *self.there, *self.along, *self.back):
            copy.wait_send()
        yield
        self.give.wait()


STREAMS = 2


def whole_kernel(
    count, interval_ref, block_ref, start_ref, basis_ref, projected_ref, residual_ref,
    block, other, high, low, rows, row_parts, cols, col_parts, vec,
    land_big, land_small, land_col, row_prev, col_prev, first_part,
    start_land, first_land, last_land, image_land, slab_ref, image_ref, before_ref, inverse_ref,
    *rest,
):
    sum_buffers = [rest[5 * k : 5 * k + 5] for k in range(3)]
    tile, pend_left, pend_right, send, recv, local_sem = rest[15:]
    r, c = lax.axis_index("row"), lax.axis_index("col")
    core, x, y, z = r % 2, r // 2, c % 4, c // 4
    copies = Copies(send, recv)

    def device(x, core, y, z):
        return (2 * x + core, 4 * z + y)

    mate = device(x, 1 - core, y, z)
    ring_x = device((x + 3) % 4, core, y, z), device((x + 1) % 4, core, y, z)
    ring_y = device(x, core, (y + 3) % 4, z), device(x, core, (y + 1) % 4, z)
    ring_z = device(x, core, y, (z + 3) % 4), device(x, core, y, (z + 1) % 4)
    crossed = x != z

    local = pltpu.make_async_copy(block_ref, block, local_sem)
    local.start()
    barrier = pltpu.get_barrier_semaphore()

    def greet(who):
        pl.semaphore_signal(barrier, inc=1, device_id=who, device_id_type=MESH)

    peers = [(offset, (r, (c + offset) % 16)) for offset in range(1, 16)]
    x_peers = [(offset, ((r + 2 * offset) % 8, c)) for offset in range(1, 4)]
    for who in (mate, *(peer for _, peer in x_peers), *(peer for _, peer in peers)):
        greet(who)

    @pl.when(crossed)
    def _():
        greet(device(z, core, y, x))
        greet(device(z, 1 - core, y, x))

    pl.semaphore_wait(barrier, jnp.where(crossed, 21, 19))

    block_rows, block_cols = block.shape
    slab = start_ref.shape[0]
    width = start_ref.shape[1] // 2
    mine_cols = pl.ds(pl.multiple_of(core * width, width), width)
    mate_cols = pl.ds(pl.multiple_of((1 - core) * width, width), width)

    start_copy = copies.make(start_ref.at[:, mate_cols], start_land, copies.reserve(1), mate)
    start_copy.start()
    block_copy = copies.make(block_ref, other, copies.reserve(1), mate)
    block_copy.start()

    lower_end = jnp.full((1, block_cols), interval_ref[0], jnp.float32)
    upper_end = jnp.full((1, block_cols), interval_ref[1], jnp.float32)
    center = 0.5 * (lower_end + upper_end)
    inverse_width = 1.0 / (0.5 * (upper_end - lower_end))

    def prepare(source, which):
        base = which * block_rows
        step = 256

        @pl.loop(0, block_rows // step)
        def _(i):
            at = pl.multiple_of(i * step, step)
            value = source[pl.ds(at, step), :]
            row = lax.broadcasted_iota(jnp.int32, value.shape, 0) + (2 * x * block_rows + base + at)
            col = lax.broadcasted_iota(jnp.int32, value.shape, 1) + c * block_cols
            value = jnp.where(row == col, value - center, value) * inverse_width
            big, small = split(value)
            to = pl.ds(pl.multiple_of(base + at, step), step)
            high[to, :] = big
            low[to, :] = small

    start_copy.wait_recv()
    own = start_ref[:, mine_cols]
    theirs = start_land[...]
    lower = jnp.where(core == 0, own, theirs)
    upper = jnp.where(core == 0, theirs, own)
    piece = jnp.concatenate([lower, upper], axis=0).T
    cols[x] = piece
    col_prev[...] = piece

    places = {"y": y, "z": z}
    rings = {"y": ring_y, "z": ring_z}
    orders = (("z", "y"), ("y", "z"))
    share = width // STREAMS
    half = share // 2

    class Stream:
        def __init__(self, index):
            self.base = index * share
            self.at_first = self.at_last = False
            self.all = pl.ds(self.base, share)
            slots = [[copies.reserve(6) for _ in range(2)] for _ in range(2)]
            self.scatters = [[self.scatter(index, u, stage, slots[u][stage]) for stage in range(2)] for u in range(2)]
            slots = [[copies.reserve(4) for _ in range(2)] for _ in range(2)]
            self.gathers = [[self.gather(u, stage, slots[u][stage]) for stage in range(2)] for u in range(2)]
            self.col_scatter = Scatter(
                copies, copies.reserve(6), x, ring_x, self.col_slice(col_parts), lambda i: land_col.at[index, i]
            )
            self.col_gather = Gather(copies, copies.reserve(4), x, ring_x, self.col_slice(cols))

        def span(self, colour, side):
            size = half if side is None else half // 2
            return pl.ds(self.base + colour * half + (0 if side is None else side * size), size)

        def col_slice(self, ref):
            def part(t, side):
                return ref.at[t, self.all if side is None else self.span(side, None), :]
            return part

        def plane(self, ref, colour, axis):
            def part(t, side):
                at = self.span(colour, side)
                return ref.at[:, t, at, :] if axis == "z" else ref.at[t, :, at, :]
            return part

        def line(self, ref, colour, axis):
            def part(t, side):
                at = self.span(colour, side)
                return ref.at[y, t, at, :] if axis == "z" else ref.at[t, z, at, :]
            return part

        def scatter(self, index, colour, stage, slot):
            axis = orders[colour][stage]
            part = (self.plane if stage == 0 else self.line)(row_parts, colour, axis)
            landing = land_big if stage == 0 else land_small
            return Scatter(copies, slot, places[axis], rings[axis], part, lambda i: landing.at[index, colour, i])

        def gather(self, colour, stage, slot):
            axis = orders[colour][1 - stage]
            part = (self.line if stage == 0 else self.plane)(rows, colour, axis)
            return Gather(copies, slot, places[axis], rings[axis], part)

        def multiply(self):
            for q in range(4):
                big, small = split(cols[q, self.all, :])
                vec[:share, q * CHUNK : (q + 1) * CHUNK] = big
                vec[share:, q * CHUNK : (q + 1) * CHUNK] = small

            @pl.loop(0, 8, unroll=4)
            def _(i):
                at = pl.ds(pl.multiple_of(i * 256, 256), 256)
                out = three_pass(vec[...], (high[at, :], low[at, :]), ((1,), (1,)))
                row_parts[i // 2, 2 * (i % 2), self.all, :] = out[:, :CHUNK]
                row_parts[i // 2, 2 * (i % 2) + 1, self.all, :] = out[:, CHUNK:]

        def multiply_turned(self):
            def one(i):
                at = pl.ds(pl.multiple_of(i * 1024, 1024), 1024)
                wide = jnp.concatenate([rows[2 * i + k // 4, k % 4, self.all, :] for k in range(8)], axis=1)
                left = jnp.concatenate(split(wide), axis=0)
                return three_pass(left, (high[at, :], low[at, :]), ((1,), (0,)))

            out = one(0) + one(1)
            for q in range(4):
                col_parts[q, self.all, :] = out[:, q * CHUNK : (q + 1) * CHUNK]

        def to_rows(self):
            self.multiply()
            firsts = [self.scatters[0][0], self.scatters[1][0]]
            seconds = [self.scatters[0][1], self.scatters[1][1]]
            for first in firsts:
                first.start()
            yield
            for first in firsts:
                first.relay()
            yield
            for first, second in zip(firsts, seconds):
                first.finish()
                second.start()
            yield
            for second in seconds:
                second.relay()
            yield

        def run(self):
            for step in range(3):
                yield from self.to_rows()
                for colour in range(2):
                    self.scatters[colour][1].finish()
                    at = self.span(colour, None)
                    value = row_parts[y, z, at, :]
                    if step > 0:
                        value = 2.0 * value - row_prev[at, :]
                    rows[y, z, at, :] = value
                    row_prev[at, :] = value
                    if step == 1:
                        first_part[at, :] = value
                    self.gathers[colour][0].start()
                self.at_first = step >= 1
                yield
                for colour in range(2):
                    self.gathers[colour][0].forward()
                yield
                for colour in range(2):
                    self.gathers[colour][0].finish()
                    self.gathers[colour][1].start()
                yield
                for colour in range(2):
                    self.gathers[colour][1].forward()
                yield
                for colour in range(2):
                    self.gathers[colour][1].finish()
                self.multiply_turned()
                self.col_scatter.start()
                yield
                self.col_scatter.relay()
                yield
                self.col_scatter.finish()
                value = col_parts[x, self.all, :]
                if step != 1:
                    value = 2.0 * value - col_prev[self.all, :]
                cols[x, self.all, :] = value
                col_prev[self.all, :] = value
                self.col_gather.start()
                self.at_last = step == 2
                yield
                self.col_gather.forward()
                yield
                self.col_gather.finish()
            yield from self.to_rows()
            for colour in range(2):
                self.scatters[colour][1].finish()

    streams = [Stream(index) for index in range(STREAMS)]
    for stream in streams:
        stream.col_gather.start()
    local.wait()
    prepare(block, core)
    for stream in streams:
        stream.col_gather.forward()
    start_copy.wait_send()
    block_copy.wait_recv()
    prepare(other, 1 - core)
    block_copy.wait_send()
    for stream in streams:
        stream.col_gather.finish()

    keep = pl.ds(pl.multiple_of(core * slab, slab), slab)
    give = pl.ds(pl.multiple_of((1 - core) * slab, slab), slab)
    top = pl.ds(0, slab)
    sums = [TotalSum(copies, (core, x, c), mate, peers, x_peers, buffers) for buffers in sum_buffers]

    def trade(piece, land, target):
        land[1] = piece.T
        copy = copies.make(land.at[1, give, :], land.at[0, give, :], copies.reserve(1), mate)
        copy.start()
        yield
        copy.wait()
        target[:, mine_cols] = land[1, keep, :]
        target[:, mate_cols] = land[0, keep, :]

    def first_chain():
        yield from trade(first_part[...], first_land, slab_ref)
        sums[0].total[...] = contract(slab_ref[...], slab_ref[...], 0, 0)
        yield from sums[0].steps()
        sums[0].total[...] = sums[0].result[...] / count
        yield from factor_steps(2, sums[0].total, before_ref, tile, pend_left, pend_right)

    def last_chain():
        yield from trade(col_prev[...], last_land, slab_ref)
        slab_ref[...] = contract(slab_ref[...], before_ref[...], 1, 1)
        sums[1].total[...] = contract(slab_ref[...], slab_ref[...], 0, 0)
        yield from sums[1].steps()
        sums[1].total[...] = sums[1].result[...] / count
        yield from factor_steps(2, sums[1].total, inverse_ref, tile, pend_left, pend_right)
        basis_ref[...] = contract(slab_ref[...], inverse_ref[...], 1, 1)

    def image_chain():
        image_land[2, :, :] = row_parts[y, z].T
        slots = copies.reserve(2)
        same = copies.make(image_land.at[2, keep, :], image_land.at[0, top, :], slots, device(z, core, y, x))
        cross = copies.make(image_land.at[2, give, :], image_land.at[1, top, :], slots + 1, device(z, 1 - core, y, x))
        cross.start()

        @pl.when(crossed)
        def _():
            same.start()

        yield

        @pl.when(crossed)
        def _():
            same.wait()

        @pl.when(jnp.logical_not(crossed))
        def _():
            image_land[0, top, :] = image_land[2, keep, :]

        cross.wait()
        image_ref[:, mine_cols] = image_land[0, top, :]
        image_ref[:, mate_cols] = image_land[1, top, :]
        image_ref[...] = contract(image_ref[...], before_ref[...], 1, 1)
        sums[2].total[...] = contract(slab_ref[...], image_ref[...], 0, 0)
        yield from sums[2].steps()

    def advance(chain):
        return next(chain, "end") != "end"

    runs = [stream.run() for stream in streams]
    chains, begun = [], 0
    going = True
    while going:
        going = False
        for run in runs:
            going = advance(run) or going
            if chains and not advance(chains[0]):
                chains.pop(0)
        if begun == 0 and all(stream.at_first for stream in streams):
            chains.append(first_chain())
            begun = 1
        if begun == 1 and all(stream.at_last for stream in streams):
            chains.append(last_chain())
            begun = 2
    while len(chains) > 1:
        if not advance(chains[0]):
            chains.pop(0)
    image = image_chain()
    ending, closing = True, True
    while ending or closing:
        ending = ending and advance(image)
        for _ in range(2):
            closing = closing and advance(chains[0])

    inverse = inverse_ref[...]
    basis = basis_ref[...]
    projected = contract(product(inverse, sums[2].result[...] / count), inverse, 1, 1)
    projected_ref[...] = projected
    residual_ref[...] = contract(image_ref[...], inverse, 1, 1) - product(basis, projected)


def on_device(matrix, start_vectors, interval):
    block_rows, block_cols = matrix.shape
    slab, vectors = start_vectors.shape
    total_rows = slab * lax.axis_size("row") * lax.axis_size("col")
    width = vectors // 2
    share = width // STREAMS
    f32, bf16 = jnp.float32, jnp.bfloat16
    vmem = pl.BlockSpec(memory_space=pltpu.VMEM)
    tall = jax.ShapeDtypeStruct((slab, vectors), f32)
    square = jax.ShapeDtypeStruct((vectors, vectors), f32)
    one_sum = [
        pltpu.VMEM((vectors, vectors), f32),
        pltpu.VMEM((vectors, vectors), f32),
        pltpu.VMEM((vectors // 2, vectors), f32),
        pltpu.VMEM((16, vectors // 32, vectors), f32),
        pltpu.VMEM((4, vectors // 32, vectors), f32),
    ]
    return pl.pallas_call(
        functools.partial(whole_kernel, total_rows),
        out_shape=(tall, square, tall),
        in_specs=[pl.BlockSpec(memory_space=pltpu.SMEM), pl.BlockSpec(memory_space=pl.ANY), vmem],
        out_specs=(vmem,) * 3,
        scratch_shapes=[
            pltpu.VMEM((block_rows, block_cols), f32),
            pltpu.VMEM((block_rows, block_cols), f32),
            pltpu.VMEM((2 * block_rows, block_cols), bf16),
            pltpu.VMEM((2 * block_rows, block_cols), bf16),
            pltpu.VMEM((4, 4, width, CHUNK), f32),
            pltpu.VMEM((4, 4, width, CHUNK), f32),
            pltpu.VMEM((4, width, CHUNK), f32),
            pltpu.VMEM((4, width, CHUNK), f32),
            pltpu.VMEM((2 * share, block_cols), bf16),
            pltpu.VMEM((STREAMS, 2, 6, 4, share // 4, CHUNK), f32),
            pltpu.VMEM((STREAMS, 2, 6, share // 4, CHUNK), f32),
            pltpu.VMEM((STREAMS, 6, share // 2, CHUNK), f32),
            pltpu.VMEM((width, CHUNK), f32),
            pltpu.VMEM((width, CHUNK), f32),
            pltpu.VMEM((width, CHUNK), f32),
            pltpu.VMEM((slab, width), f32),
            pltpu.VMEM((2, CHUNK, width), f32),
            pltpu.VMEM((2, CHUNK, width), f32),
            pltpu.VMEM((3, CHUNK, width), f32),
            pltpu.VMEM((slab, vectors), f32),
            pltpu.VMEM((slab, vectors), f32),
            pltpu.VMEM((vectors, vectors), f32),
            pltpu.VMEM((vectors, vectors), f32),
            *(one_sum * 3),
            pltpu.VMEM((BLOCK + PANEL, 2 * BLOCK), f32),
            pltpu.VMEM((BLOCK, 6 * PANEL), bf16),
            pltpu.VMEM((6 * PANEL, 2 * BLOCK), bf16),
            pltpu.SemaphoreType.DMA((256,)),
            pltpu.SemaphoreType.DMA((256,)),
            pltpu.SemaphoreType.DMA,
        ],
        compiler_params=pltpu.CompilerParams(
            collective_id=0, has_side_effects=True, vmem_limit_bytes=56 * 2**20
        ),
        cost_estimate=pl.CostEstimate(flops=10**10, bytes_accessed=4 * 10**6, transcendentals=0),
    )(interval, matrix, start_vectors)


def solution(mesh):
    return jax.shard_map(
        on_device,
        mesh=mesh,
        in_specs=(P("row", "col"), P(("col", "row"), None), P()),
        out_specs=(P(("col", "row"), None), P(), P(("col", "row"), None)),
        check_vma=False,
    )
```

```python
import functools

import jax
import jax.numpy as jnp
from jax import lax
from jax.experimental import pallas as pl
from jax.experimental.pallas import tpu as pltpu
from jax.sharding import PartitionSpec as P

FILTER_DEG = 3
OUTER = 2
PANEL = 16
BLOCK = 128
MESH = pl.DeviceIdType.MESH
CHUNK = 128


def product(left, right, precision=lax.Precision.HIGHEST):
    return jnp.dot(left, right, precision=precision, preferred_element_type=jnp.float32)


def contract(left, right, left_dim, right_dim):
    return lax.dot_general(
        left,
        right,
        (((left_dim,), (right_dim,)), ((), ())),
        precision=lax.Precision.HIGHEST,
        preferred_element_type=jnp.float32,
    )


def lane_columns(rows, first):
    narrow = rows[:, :128]
    lanes = jnp.zeros(narrow.shape, jnp.int32) + first
    return [jnp.take_along_axis(narrow, lanes + j, axis=1) for j in range(PANEL)]


def row_of(value, step):
    return jnp.broadcast_to(value[step : step + 1, :], value.shape)


def three_parts(value):
    high = value.astype(jnp.bfloat16).astype(jnp.float32)
    rest = value - high
    middle = rest.astype(jnp.bfloat16).astype(jnp.float32)
    return high, middle, rest - middle


def factor_panels(tile, pend_left, pend_right, begin, end):
    block = tile.shape[1] // 2
    sub = lax.broadcasted_iota(jnp.int32, (PANEL, 128), 0)
    lane = lax.broadcasted_iota(jnp.int32, (PANEL, block), 1)

    def panel(p, carry):
        first = pl.multiple_of(p * PANEL, PANEL)
        here, after = pl.ds(first, PANEL), pl.ds(pl.multiple_of(first + PANEL, PANEL), PANEL)
        rows = tile[here, :]
        tile[:block, :] -= jnp.dot(pend_left[...], pend_right[...], preferred_element_type=jnp.float32)

        columns = lane_columns(rows, first)
        left, right = rows[:, :block], rows[:, block:]
        inverses = []
        pivots = jnp.ones((PANEL, 128), jnp.float32)
        for s in range(PANEL):
            pivot = row_of(columns[s], s)
            pivots = jnp.where(sub == s, pivot, pivots)
            inverse = 1.0 / pivot
            inverses.append(inverse)
            if s < PANEL - 1:
                ratio = jnp.where(sub > s, columns[s] * inverse, 0.0)
                for j in range(s + 1, PANEL):
                    columns[j] = columns[j] - ratio * row_of(columns[j], s)
                left = left - ratio * row_of(left, s)
                right = right - ratio * row_of(right, s)

        scale = lax.rsqrt(pivots)
        done_left, done_right = left * scale, right * scale
        tile[here, :block] = done_left
        tile[here, block:] = done_right
        a = three_parts(jnp.where(lane >= first + 2 * PANEL, done_left, 0.0))
        pend_left[...] = jnp.concatenate([a[0], a[0], a[1], a[1], a[0], a[2]], axis=0).T.astype(jnp.bfloat16)
        b = three_parts(jnp.concatenate([done_left, done_right], axis=1))
        pend_right[...] = jnp.concatenate([b[0], b[1], b[0], b[1], b[2], b[0]], axis=0).astype(jnp.bfloat16)

        following = tile[after, :]
        others = lane_columns(following, first)
        next_left, next_right = following[:, :block], following[:, block:]
        for s in range(PANEL):
            ratio = others[s] * inverses[s]
            for j in range(s + 1, PANEL):
                others[j] = others[j] - ratio * row_of(columns[j], s)
            next_left = next_left - ratio * row_of(left, s)
            next_right = next_right - ratio * row_of(right, s)
        tile[after, :block] = next_left
        tile[after, block:] = next_right
        return carry

    lax.fori_loop(begin, end, panel, 0)


def factor_steps(pieces, work, inverse_ref, tile, pend_left, pend_right):
    order, block = work.shape[0], BLOCK
    at_row = lax.broadcasted_iota(jnp.int32, (order, order), 0)
    at_col = lax.broadcasted_iota(jnp.int32, (order, order), 1)
    inverse_ref[...] = (at_row == at_col).astype(jnp.float32)
    row = lax.broadcasted_iota(jnp.int32, (block, block), 0)
    col = lax.broadcasted_iota(jnp.int32, (block, block), 1)
    panels = block // PANEL
    for at in range(0, order, block):
        stop = at + block
        tile[:block, :block] = work[at:stop, at:stop]
        tile[:block, block:] = (row == col).astype(jnp.float32)
        tile[block:, :] = jnp.zeros((PANEL, 2 * block), jnp.float32)
        pend_left[...] = jnp.zeros_like(pend_left)
        pend_right[...] = jnp.zeros_like(pend_right)
        for piece in range(pieces):
            factor_panels(tile, pend_left, pend_right, piece * panels // pieces, (piece + 1) * panels // pieces)
            yield
        small = jnp.where(row >= col, tile[:block, block:], 0.0)
        solved = product(small, inverse_ref[at:stop, :stop])
        inverse_ref[at:stop, :stop] = solved
        if stop < order:
            below = contract(work[stop:, at:stop], small, 1, 1)
            work[stop:, stop:] -= contract(below, below, 1, 1)
            inverse_ref[stop:, :stop] -= product(below, solved)
            yield


class Copies:
    def __init__(self, send, recv):
        self.send, self.recv, self.used = send, recv, 0

    def reserve(self, count):
        first = self.used
        self.used += count
        return first

    def make(self, source, target, slot, device):
        return pltpu.make_async_remote_copy(
            src_ref=source,
            dst_ref=target,
            send_sem=self.send.at[slot],
            recv_sem=self.recv.at[slot],
            device_id=device,
            device_id_type=MESH,
        )


class Scatter:
    relays = True

    def __init__(self, copies, slot, place, ring, part, land):
        self.place, self.part, self.land = place, part, land
        left, right = ring[3], ring[1]
        ahead, behind, across = (place + 1) % 4, (place + 3) % 4, (place + 2) % 4
        self.ahead, self.behind = ahead, behind
        plan = (
            (part(across, 0), right),
            (part(across, 1), left),
            (part(ahead, 1), right),
            (part(behind, 0), left),
            (part(ahead, 0), right),
            (part(behind, 1), left),
        )
        self.copies = [
            copies.make(source, land(i), slot + i, device) for i, (source, device) in enumerate(plan)
        ]

    def start(self):
        for copy in self.copies[:4]:
            copy.start()

    def relay(self):
        for first, half, target in ((0, 0, self.ahead), (1, 1, self.behind)):
            self.copies[first].wait_recv()
            mine = self.part(target, half)
            mine[...] += self.land(first)[...]
            self.copies[4 + first].start()

    def finish(self):
        for copy in self.copies[2:]:
            copy.wait_recv()
        for half, terms in ((0, (3, 4)), (1, (2, 5))):
            mine = self.part(self.place, half)
            mine[...] += self.land(terms[0])[...] + self.land(terms[1])[...]
        for copy in self.copies:
            copy.wait_send()


class Gather:
    relays = True

    def __init__(self, copies, slot, place, ring, part):
        left, right = ring[3], ring[1]
        ahead, behind = (place + 1) % 4, (place + 3) % 4
        self.copies = [
            copies.make(part(place, None), part(place, None), slot, right),
            copies.make(part(place, None), part(place, None), slot + 1, left),
            copies.make(part(behind, 0), part(behind, 0), slot + 2, right),
            copies.make(part(ahead, 1), part(ahead, 1), slot + 3, left),
        ]

    def start(self):
        for copy in self.copies[:2]:
            copy.start()

    def forward(self):
        for first in range(2):
            self.copies[first].wait_recv()
            self.copies[2 + first].start()

    def finish(self):
        for copy in self.copies[2:]:
            copy.wait_recv()
        for copy in self.copies:
            copy.wait_send()


class DirectScatter:
    relays = False

    def __init__(self, copies, slot, place, ring, part, land):
        self.mine, self.land = part(place, None), land
        self.copies = [
            copies.make(part((place + offset) % 4, None), land(offset - 1), slot + offset - 1, ring[offset])
            for offset in (2, 1, 3)
        ]

    def start(self):
        for copy in self.copies:
            copy.start()

    def finish(self):
        for copy in self.copies:
            copy.wait_recv()
        self.mine[...] += self.land(0)[...] + (self.land(1)[...] + self.land(2)[...])
        for copy in self.copies:
            copy.wait_send()


class DirectGather:
    relays = False

    def __init__(self, copies, slot, place, ring, part):
        own = part(place, None)
        self.copies = [copies.make(own, own, slot + offset - 1, ring[offset]) for offset in (2, 1, 3)]

    def start(self):
        for copy in self.copies:
            copy.start()

    def finish(self):
        for copy in self.copies:
            copy.wait_recv()
        for copy in self.copies:
            copy.wait_send()


def split(value):
    high = value.astype(jnp.bfloat16)
    return high, (value - high.astype(jnp.float32)).astype(jnp.bfloat16)


def three_pass(left, right, dims):
    def one(a, b):
        return lax.dot_general(a, b, (dims, ((), ())), preferred_element_type=jnp.float32)

    count = left.shape[0] // 2
    both = one(left, right[0])
    return both[:count] + (both[count:] + one(left[:count], right[1]))


class TotalSum:
    def __init__(self, copies, position, mate, peers, x_peers, buffers):
        core, x, c = position
        self.x = x
        self.total, self.result, self.land_core, self.land_plane, self.land_x = buffers
        half = self.total.shape[0] // 2
        size = half // 16

        def rows(ref, first, count):
            return ref.at[pl.ds(pl.multiple_of(first, size), count), :]

        def piece(ref, t):
            return rows(ref, core * half + t * size, size)

        self.mine = rows(self.total, core * half, half)
        self.swap = copies.make(rows(self.total, (1 - core) * half, half), self.land_core, copies.reserve(1), mate)
        self.own, self.summed = piece(self.total, c), piece(self.result, c)
        self.there, self.along, self.back = [], [], []
        for offset, peer in peers:
            source, target = piece(self.total, (c + offset) % 16), self.land_plane.at[offset]
            self.there.append(copies.make(source, target, copies.reserve(1), peer))
            self.back.append(copies.make(self.summed, self.summed, copies.reserve(1), peer))
        for offset, peer in x_peers:
            self.along.append(copies.make(self.land_x.at[0], self.land_x.at[offset], copies.reserve(1), peer))
        whole = rows(self.result, core * half, half)
        self.give = copies.make(whole, whole, copies.reserve(1), mate)

    def steps(self):
        self.swap.start()
        yield
        self.swap.wait_recv()
        self.mine[...] += self.land_core[...]
        for copy in self.there:
            copy.start()
        yield
        value = self.own[...]
        for offset, copy in enumerate(self.there, 1):
            copy.wait_recv()
            value = value + self.land_plane[offset]
        self.land_x[0] = value
        for copy in self.along:
            copy.start()
        yield
        for copy in self.along:
            copy.wait_recv()
        value = self.land_x[self.x % 4]
        for at in range(1, 4):
            value = value + self.land_x[(self.x + 4 - at) % 4]
        self.summed[...] = value
        for copy in self.back:
            copy.start()
        yield
        for copy in self.back:
            copy.wait_recv()
        self.give.start()
        for copy in (self.swap, *self.there, *self.along, *self.back):
            copy.wait_send()
        yield
        self.give.wait()


STREAMS = 2
LEAD = 0
SCATTERS = (Scatter, DirectScatter, DirectScatter)
GATHERS = (DirectGather, Gather, DirectGather)


def whole_kernel(
    count, interval_ref, block_ref, start_ref, basis_ref, projected_ref, residual_ref,
    block, other, high, low, rows, row_parts, cols, col_parts, vec,
    land_big, land_small, land_col, row_prev, col_prev, first_part,
    start_land, first_land, last_land, image_land, slab_ref, image_ref, before_ref, inverse_ref,
    *rest,
):
    sum_buffers = [rest[5 * k : 5 * k + 5] for k in range(3)]
    tile, pend_left, pend_right, send, recv, local_sem = rest[15:]
    r, c = lax.axis_index("row"), lax.axis_index("col")
    core, x, y, z = r % 2, r // 2, c % 4, c // 4
    copies = Copies(send, recv)

    def device(x, core, y, z):
        return (2 * x + core, 4 * z + y)

    mate = device(x, 1 - core, y, z)
    ring_x = {offset: device((x + offset) % 4, core, y, z) for offset in (1, 2, 3)}
    ring_y = {offset: device(x, core, (y + offset) % 4, z) for offset in (1, 2, 3)}
    ring_z = {offset: device(x, core, y, (z + offset) % 4) for offset in (1, 2, 3)}
    crossed = x != z

    local = pltpu.make_async_copy(block_ref, block, local_sem)
    local.start()
    barrier = pltpu.get_barrier_semaphore()

    def greet(who):
        pl.semaphore_signal(barrier, inc=1, device_id=who, device_id_type=MESH)

    peers = [(offset, (r, (c + offset) % 16)) for offset in range(1, 16)]
    x_peers = list(ring_x.items())
    for who in (mate, *(peer for _, peer in x_peers), *(peer for _, peer in peers)):
        greet(who)

    @pl.when(crossed)
    def _():
        greet(device(z, core, y, x))
        greet(device(z, 1 - core, y, x))

    pl.semaphore_wait(barrier, jnp.where(crossed, 21, 19))

    block_rows, block_cols = block.shape
    slab = start_ref.shape[0]
    width = start_ref.shape[1] // 2
    mine_cols = pl.ds(pl.multiple_of(core * width, width), width)
    mate_cols = pl.ds(pl.multiple_of((1 - core) * width, width), width)

    start_copy = copies.make(start_ref.at[:, mate_cols], start_land, copies.reserve(1), mate)
    start_copy.start()
    block_copy = copies.make(block_ref, other, copies.reserve(1), mate)
    block_copy.start()

    lower_end = jnp.full((1, block_cols), interval_ref[0], jnp.float32)
    upper_end = jnp.full((1, block_cols), interval_ref[1], jnp.float32)
    center = 0.5 * (lower_end + upper_end)
    inverse_width = 1.0 / (0.5 * (upper_end - lower_end))

    def prepare(source, which):
        base = which * block_rows
        step = 256

        @pl.loop(0, block_rows // step)
        def _(i):
            at = pl.multiple_of(i * step, step)
            value = source[pl.ds(at, step), :]
            row = lax.broadcasted_iota(jnp.int32, value.shape, 0) + (2 * x * block_rows + base + at)
            col = lax.broadcasted_iota(jnp.int32, value.shape, 1) + c * block_cols
            value = jnp.where(row == col, value - center, value) * inverse_width
            big, small = split(value)
            to = pl.ds(pl.multiple_of(base + at, step), step)
            high[to, :] = big
            low[to, :] = small

    start_copy.wait_recv()
    own = start_ref[:, mine_cols]
    theirs = start_land[...]
    lower = jnp.where(core == 0, own, theirs)
    upper = jnp.where(core == 0, theirs, own)
    piece = jnp.concatenate([lower, upper], axis=0).T
    cols[x] = piece
    col_prev[...] = piece

    places = {"y": y, "z": z}
    rings = {"y": ring_y, "z": ring_z}
    orders = (("z", "y"), ("y", "z"))
    share = width // STREAMS
    half = share // 2

    class Stream:
        def __init__(self, index):
            self.base = index * share
            self.at_first = self.at_last = False
            self.all = pl.ds(self.base, share)
            slots = [[copies.reserve(6) for _ in range(2)] for _ in range(2)]
            self.scatters = [[self.scatter(index, u, stage, slots[u][stage]) for stage in range(2)] for u in range(2)]
            slots = [[copies.reserve(4) for _ in range(2)] for _ in range(2)]
            self.gathers = [[self.gather(u, stage, slots[u][stage]) for stage in range(2)] for u in range(2)]
            self.col_scatter = SCATTERS[2](
                copies, copies.reserve(6), x, ring_x, self.col_slice(col_parts), lambda i: land_col.at[index, i]
            )
            self.col_gather = GATHERS[2](copies, copies.reserve(4), x, ring_x, self.col_slice(cols))

        def span(self, colour, side):
            size = half if side is None else half // 2
            return pl.ds(self.base + colour * half + (0 if side is None else side * size), size)

        def col_slice(self, ref):
            def part(t, side):
                return ref.at[t, self.all if side is None else self.span(side, None), :]
            return part

        def plane(self, ref, colour, axis):
            def part(t, side):
                at = self.span(colour, side)
                return ref.at[:, t, at, :] if axis == "z" else ref.at[t, :, at, :]
            return part

        def line(self, ref, colour, axis):
            def part(t, side):
                at = self.span(colour, side)
                return ref.at[y, t, at, :] if axis == "z" else ref.at[t, z, at, :]
            return part

        def scatter(self, index, colour, stage, slot):
            axis = orders[colour][stage]
            part = (self.plane if stage == 0 else self.line)(row_parts, colour, axis)
            landing = land_big if stage == 0 else land_small
            return SCATTERS[stage](copies, slot, places[axis], rings[axis], part, lambda i: landing.at[index, colour, i])

        def gather(self, colour, stage, slot):
            axis = orders[colour][1 - stage]
            part = (self.line if stage == 0 else self.plane)(rows, colour, axis)
            return GATHERS[stage](copies, slot, places[axis], rings[axis], part)

        def multiply(self):
            for q in range(4):
                big, small = split(cols[q, self.all, :])
                vec[:share, q * CHUNK : (q + 1) * CHUNK] = big
                vec[share:, q * CHUNK : (q + 1) * CHUNK] = small

            @pl.loop(0, 8, unroll=4)
            def _(i):
                at = pl.ds(pl.multiple_of(i * 256, 256), 256)
                out = three_pass(vec[...], (high[at, :], low[at, :]), ((1,), (1,)))
                row_parts[i // 2, 2 * (i % 2), self.all, :] = out[:, :CHUNK]
                row_parts[i // 2, 2 * (i % 2) + 1, self.all, :] = out[:, CHUNK:]

        def multiply_turned(self):
            def one(i):
                at = pl.ds(pl.multiple_of(i * 1024, 1024), 1024)
                wide = jnp.concatenate([rows[2 * i + k // 4, k % 4, self.all, :] for k in range(8)], axis=1)
                left = jnp.concatenate(split(wide), axis=0)
                return three_pass(left, (high[at, :], low[at, :]), ((1,), (0,)))

            out = one(0) + one(1)
            for q in range(4):
                col_parts[q, self.all, :] = out[:, q * CHUNK : (q + 1) * CHUNK]

        def to_rows(self):
            self.multiply()
            firsts = [self.scatters[0][0], self.scatters[1][0]]
            seconds = [self.scatters[0][1], self.scatters[1][1]]
            for first in firsts:
                first.start()
            yield
            if firsts[0].relays:
                for first in firsts:
                    first.relay()
                yield
            for first, second in zip(firsts, seconds):
                first.finish()
                second.start()
            yield
            if seconds[0].relays:
                for second in seconds:
                    second.relay()
                yield

        def gather_rows(self, step):
            for colour in range(2):
                self.scatters[colour][1].finish()
                at = self.span(colour, None)
                value = row_parts[y, z, at, :]
                if step > 0:
                    value = 2.0 * value - row_prev[at, :]
                rows[y, z, at, :] = value
                row_prev[at, :] = value
                if step == 1:
                    first_part[at, :] = value
                self.gathers[colour][0].start()
            self.at_first = step >= 1
            yield
            for stage in range(2):
                pair = [self.gathers[0][stage], self.gathers[1][stage]]
                if pair[0].relays:
                    for one in pair:
                        one.forward()
                    yield
                for colour in range(2):
                    pair[colour].finish()
                    if stage == 0:
                        self.gathers[colour][1].start()
                if stage == 0:
                    yield

        def to_cols(self, step):
            self.multiply_turned()
            self.col_scatter.start()
            yield
            if self.col_scatter.relays:
                self.col_scatter.relay()
                yield
            self.col_scatter.finish()
            value = col_parts[x, self.all, :]
            if step != 1:
                value = 2.0 * value - col_prev[self.all, :]
            cols[x, self.all, :] = value
            col_prev[self.all, :] = value
            self.col_gather.start()
            self.at_last = step == 2
            yield
            if self.col_gather.relays:
                self.col_gather.forward()
                yield
            self.col_gather.finish()

        def run(self):
            for step in range(3):
                yield from self.to_rows()
                yield from self.gather_rows(step)
                yield from self.to_cols(step)
            yield from self.to_rows()
            for colour in range(2):
                self.scatters[colour][1].finish()

    streams = [Stream(index) for index in range(STREAMS)]
    for stream in streams:
        stream.col_gather.start()
    local.wait()
    prepare(block, core)
    for stream in streams:
        if stream.col_gather.relays:
            stream.col_gather.forward()
    start_copy.wait_send()
    block_copy.wait_recv()
    prepare(other, 1 - core)
    block_copy.wait_send()
    for stream in streams:
        stream.col_gather.finish()

    keep = pl.ds(pl.multiple_of(core * slab, slab), slab)
    give = pl.ds(pl.multiple_of((1 - core) * slab, slab), slab)
    top = pl.ds(0, slab)
    sums = [TotalSum(copies, (core, x, c), mate, peers, x_peers, buffers) for buffers in sum_buffers]

    def trade(piece, land, target):
        land[1] = piece.T
        copy = copies.make(land.at[1, give, :], land.at[0, give, :], copies.reserve(1), mate)
        copy.start()
        yield
        copy.wait()
        target[:, mine_cols] = land[1, keep, :]
        target[:, mate_cols] = land[0, keep, :]

    def first_chain():
        yield from trade(first_part[...], first_land, slab_ref)
        sums[0].total[...] = contract(slab_ref[...], slab_ref[...], 0, 0)
        yield from sums[0].steps()
        sums[0].total[...] = sums[0].result[...] / count
        yield from factor_steps(2, sums[0].total, before_ref, tile, pend_left, pend_right)

    def last_chain():
        yield from trade(col_prev[...], last_land, slab_ref)
        slab_ref[...] = contract(slab_ref[...], before_ref[...], 1, 1)
        sums[1].total[...] = contract(slab_ref[...], slab_ref[...], 0, 0)
        yield from sums[1].steps()
        sums[1].total[...] = sums[1].result[...] / count
        yield from factor_steps(2, sums[1].total, inverse_ref, tile, pend_left, pend_right)
        basis_ref[...] = contract(slab_ref[...], inverse_ref[...], 1, 1)

    def image_chain():
        image_land[2, :, :] = row_parts[y, z].T
        slots = copies.reserve(2)
        same = copies.make(image_land.at[2, keep, :], image_land.at[0, top, :], slots, device(z, core, y, x))
        cross = copies.make(image_land.at[2, give, :], image_land.at[1, top, :], slots + 1, device(z, 1 - core, y, x))
        cross.start()

        @pl.when(crossed)
        def _():
            same.start()

        yield

        @pl.when(crossed)
        def _():
            same.wait()

        @pl.when(jnp.logical_not(crossed))
        def _():
            image_land[0, top, :] = image_land[2, keep, :]

        cross.wait()
        image_ref[:, mine_cols] = image_land[0, top, :]
        image_ref[:, mate_cols] = image_land[1, top, :]
        image_ref[...] = contract(image_ref[...], before_ref[...], 1, 1)
        sums[2].total[...] = contract(slab_ref[...], image_ref[...], 0, 0)
        yield from sums[2].steps()

    def advance(chain):
        return next(chain, "end") != "end"

    runs = [stream.run() for stream in streams]
    chains, begun = [], 0
    for _ in range(LEAD):
        advance(runs[0])
    going = True
    while going:
        going = False
        for run in runs:
            going = advance(run) or going
            if chains and not advance(chains[0]):
                chains.pop(0)
        if begun == 0 and all(stream.at_first for stream in streams):
            chains.append(first_chain())
            begun = 1
        if begun == 1 and all(stream.at_last for stream in streams):
            chains.append(last_chain())
            begun = 2
    while len(chains) > 1:
        if not advance(chains[0]):
            chains.pop(0)
    image = image_chain()
    ending, closing = True, True
    while ending or closing:
        ending = ending and advance(image)
        for _ in range(2):
            closing = closing and advance(chains[0])

    inverse = inverse_ref[...]
    basis = basis_ref[...]
    projected = contract(product(inverse, sums[2].result[...] / count), inverse, 1, 1)
    projected_ref[...] = projected
    residual_ref[...] = contract(image_ref[...], inverse, 1, 1) - product(basis, projected)


def on_device(matrix, start_vectors, interval):
    block_rows, block_cols = matrix.shape
    slab, vectors = start_vectors.shape
    total_rows = slab * lax.axis_size("row") * lax.axis_size("col")
    width = vectors // 2
    share = width // STREAMS
    f32, bf16 = jnp.float32, jnp.bfloat16
    vmem = pl.BlockSpec(memory_space=pltpu.VMEM)
    tall = jax.ShapeDtypeStruct((slab, vectors), f32)
    square = jax.ShapeDtypeStruct((vectors, vectors), f32)
    one_sum = [
        pltpu.VMEM((vectors, vectors), f32),
        pltpu.VMEM((vectors, vectors), f32),
        pltpu.VMEM((vectors // 2, vectors), f32),
        pltpu.VMEM((16, vectors // 32, vectors), f32),
        pltpu.VMEM((4, vectors // 32, vectors), f32),
    ]
    return pl.pallas_call(
        functools.partial(whole_kernel, total_rows),
        out_shape=(tall, square, tall),
        in_specs=[pl.BlockSpec(memory_space=pltpu.SMEM), pl.BlockSpec(memory_space=pl.ANY), vmem],
        out_specs=(vmem,) * 3,
        scratch_shapes=[
            pltpu.VMEM((block_rows, block_cols), f32),
            pltpu.VMEM((block_rows, block_cols), f32),
            pltpu.VMEM((2 * block_rows, block_cols), bf16),
            pltpu.VMEM((2 * block_rows, block_cols), bf16),
            pltpu.VMEM((4, 4, width, CHUNK), f32),
            pltpu.VMEM((4, 4, width, CHUNK), f32),
            pltpu.VMEM((4, width, CHUNK), f32),
            pltpu.VMEM((4, width, CHUNK), f32),
            pltpu.VMEM((2 * share, block_cols), bf16),
            pltpu.VMEM((STREAMS, 2, 6, 4, share // 4, CHUNK), f32),
            pltpu.VMEM((STREAMS, 2, 3, share // 2, CHUNK), f32),
            pltpu.VMEM((STREAMS, 3, share, CHUNK), f32),
            pltpu.VMEM((width, CHUNK), f32),
            pltpu.VMEM((width, CHUNK), f32),
            pltpu.VMEM((width, CHUNK), f32),
            pltpu.VMEM((slab, width), f32),
            pltpu.VMEM((2, CHUNK, width), f32),
            pltpu.VMEM((2, CHUNK, width), f32),
            pltpu.VMEM((3, CHUNK, width), f32),
            pltpu.VMEM((slab, vectors), f32),
            pltpu.VMEM((slab, vectors), f32),
            pltpu.VMEM((vectors, vectors), f32),
            pltpu.VMEM((vectors, vectors), f32),
            *(one_sum * 3),
            pltpu.VMEM((BLOCK + PANEL, 2 * BLOCK), f32),
            pltpu.VMEM((BLOCK, 6 * PANEL), bf16),
            pltpu.VMEM((6 * PANEL, 2 * BLOCK), bf16),
            pltpu.SemaphoreType.DMA((256,)),
            pltpu.SemaphoreType.DMA((256,)),
            pltpu.SemaphoreType.DMA,
        ],
        compiler_params=pltpu.CompilerParams(
            collective_id=0, has_side_effects=True, vmem_limit_bytes=56 * 2**20
        ),
        cost_estimate=pl.CostEstimate(flops=10**10, bytes_accessed=4 * 10**6, transcendentals=0),
    )(interval, matrix, start_vectors)


def solution(mesh):
    return jax.shard_map(
        on_device,
        mesh=mesh,
        in_specs=(P("row", "col"), P(("col", "row"), None), P()),
        out_specs=(P(("col", "row"), None), P(), P(("col", "row"), None)),
        check_vma=False,
    )
```

```python
import functools

import jax
import jax.numpy as jnp
from jax import lax
from jax.experimental import pallas as pl
from jax.experimental.pallas import tpu as pltpu
from jax.sharding import PartitionSpec as P

FILTER_DEG = 3
OUTER = 2
PANEL = 16
BLOCK = 128
WORK = "work"
MESH = pl.DeviceIdType.MESH
CHUNK = 128


def product(left, right, precision=lax.Precision.HIGHEST):
    return jnp.dot(left, right, precision=precision, preferred_element_type=jnp.float32)


def contract(left, right, left_dim, right_dim):
    return lax.dot_general(
        left,
        right,
        (((left_dim,), (right_dim,)), ((), ())),
        precision=lax.Precision.HIGHEST,
        preferred_element_type=jnp.float32,
    )


def lane_columns(rows, first):
    narrow = rows[:, :128]
    lanes = jnp.zeros(narrow.shape, jnp.int32) + first
    return [jnp.take_along_axis(narrow, lanes + j, axis=1) for j in range(PANEL)]


def row_of(value, step):
    return jnp.broadcast_to(value[step : step + 1, :], value.shape)


def three_parts(value):
    high = value.astype(jnp.bfloat16).astype(jnp.float32)
    rest = value - high
    middle = rest.astype(jnp.bfloat16).astype(jnp.float32)
    return high, middle, rest - middle


def factor_panels(tile, pend_left, pend_right, begin, end):
    block = tile.shape[1] // 2
    sub = lax.broadcasted_iota(jnp.int32, (PANEL, 128), 0)
    lane = lax.broadcasted_iota(jnp.int32, (PANEL, block), 1)

    def panel(p, carry):
        first = pl.multiple_of(p * PANEL, PANEL)
        here, after = pl.ds(first, PANEL), pl.ds(pl.multiple_of(first + PANEL, PANEL), PANEL)
        rows = tile[here, :]
        tile[:block, :] -= jnp.dot(pend_left[...], pend_right[...], preferred_element_type=jnp.float32)

        columns = lane_columns(rows, first)
        left, right = rows[:, :block], rows[:, block:]
        inverses = []
        pivots = jnp.ones((PANEL, 128), jnp.float32)
        for s in range(PANEL):
            pivot = row_of(columns[s], s)
            pivots = jnp.where(sub == s, pivot, pivots)
            inverse = 1.0 / pivot
            inverses.append(inverse)
            if s < PANEL - 1:
                ratio = jnp.where(sub > s, columns[s] * inverse, 0.0)
                for j in range(s + 1, PANEL):
                    columns[j] = columns[j] - ratio * row_of(columns[j], s)
                left = left - ratio * row_of(left, s)
                right = right - ratio * row_of(right, s)

        scale = lax.rsqrt(pivots)
        done_left, done_right = left * scale, right * scale
        tile[here, :block] = done_left
        tile[here, block:] = done_right
        a = three_parts(jnp.where(lane >= first + 2 * PANEL, done_left, 0.0))
        pend_left[...] = jnp.concatenate([a[0], a[0], a[1], a[1], a[0], a[2]], axis=0).T.astype(jnp.bfloat16)
        b = three_parts(jnp.concatenate([done_left, done_right], axis=1))
        pend_right[...] = jnp.concatenate([b[0], b[1], b[0], b[1], b[2], b[0]], axis=0).astype(jnp.bfloat16)

        following = tile[after, :]
        others = lane_columns(following, first)
        next_left, next_right = following[:, :block], following[:, block:]
        for s in range(PANEL):
            ratio = others[s] * inverses[s]
            for j in range(s + 1, PANEL):
                others[j] = others[j] - ratio * row_of(columns[j], s)
            next_left = next_left - ratio * row_of(left, s)
            next_right = next_right - ratio * row_of(right, s)
        tile[after, :block] = next_left
        tile[after, block:] = next_right
        return carry

    lax.fori_loop(begin, end, panel, 0)


def factor_steps(pieces, work, inverse_ref, tile, pend_left, pend_right):
    order, block = work.shape[0], BLOCK
    at_row = lax.broadcasted_iota(jnp.int32, (order, order), 0)
    at_col = lax.broadcasted_iota(jnp.int32, (order, order), 1)
    inverse_ref[...] = (at_row == at_col).astype(jnp.float32)
    row = lax.broadcasted_iota(jnp.int32, (block, block), 0)
    col = lax.broadcasted_iota(jnp.int32, (block, block), 1)
    panels = block // PANEL
    for at in range(0, order, block):
        stop = at + block
        tile[:block, :block] = work[at:stop, at:stop]
        tile[:block, block:] = (row == col).astype(jnp.float32)
        tile[block:, :] = jnp.zeros((PANEL, 2 * block), jnp.float32)
        pend_left[...] = jnp.zeros_like(pend_left)
        pend_right[...] = jnp.zeros_like(pend_right)
        for piece in range(pieces):
            factor_panels(tile, pend_left, pend_right, piece * panels // pieces, (piece + 1) * panels // pieces)
            yield WORK
        small = jnp.where(row >= col, tile[:block, block:], 0.0)
        solved = product(small, inverse_ref[at:stop, :stop])
        inverse_ref[at:stop, :stop] = solved
        if stop < order:
            below = contract(work[stop:, at:stop], small, 1, 1)
            work[stop:, stop:] -= contract(below, below, 1, 1)
            inverse_ref[stop:, :stop] -= product(below, solved)
            yield WORK


class Copies:
    def __init__(self, send, recv):
        self.send, self.recv, self.used = send, recv, 0

    def reserve(self, count):
        first = self.used
        self.used += count
        return first

    def make(self, source, target, slot, device):
        return pltpu.make_async_remote_copy(
            src_ref=source,
            dst_ref=target,
            send_sem=self.send.at[slot],
            recv_sem=self.recv.at[slot],
            device_id=device,
            device_id_type=MESH,
        )


class Scatter:
    relays = True

    def __init__(self, copies, slot, place, ring, part, land):
        self.place, self.part, self.land = place, part, land
        left, right = ring[3], ring[1]
        ahead, behind, across = (place + 1) % 4, (place + 3) % 4, (place + 2) % 4
        self.ahead, self.behind = ahead, behind
        plan = (
            (part(across, 0), right),
            (part(across, 1), left),
            (part(ahead, 1), right),
            (part(behind, 0), left),
            (part(ahead, 0), right),
            (part(behind, 1), left),
        )
        self.copies = [
            copies.make(source, land(i), slot + i, device) for i, (source, device) in enumerate(plan)
        ]

    def start(self):
        for copy in self.copies[:4]:
            copy.start()

    def relay(self):
        for first, half, target in ((0, 0, self.ahead), (1, 1, self.behind)):
            self.copies[first].wait_recv()
            mine = self.part(target, half)
            mine[...] += self.land(first)[...]
            self.copies[4 + first].start()

    def finish(self):
        for copy in self.copies[2:]:
            copy.wait_recv()
        for half, terms in ((0, (3, 4)), (1, (2, 5))):
            mine = self.part(self.place, half)
            mine[...] += self.land(terms[0])[...] + self.land(terms[1])[...]
        for copy in self.copies:
            copy.wait_send()


class Gather:
    relays = True

    def __init__(self, copies, slot, place, ring, part):
        left, right = ring[3], ring[1]
        ahead, behind = (place + 1) % 4, (place + 3) % 4
        self.copies = [
            copies.make(part(place, None), part(place, None), slot, right),
            copies.make(part(place, None), part(place, None), slot + 1, left),
            copies.make(part(behind, 0), part(behind, 0), slot + 2, right),
            copies.make(part(ahead, 1), part(ahead, 1), slot + 3, left),
        ]

    def start(self):
        for copy in self.copies[:2]:
            copy.start()

    def forward(self):
        for first in range(2):
            self.copies[first].wait_recv()
            self.copies[2 + first].start()

    def finish(self):
        for copy in self.copies[2:]:
            copy.wait_recv()
        for copy in self.copies:
            copy.wait_send()


class DirectScatter:
    relays = False

    def __init__(self, copies, slot, place, ring, part, land):
        self.mine, self.land = part(place, None), land
        self.copies = [
            copies.make(part((place + offset) % 4, None), land(offset - 1), slot + offset - 1, ring[offset])
            for offset in (2, 1, 3)
        ]

    def start(self):
        for copy in self.copies:
            copy.start()

    def finish(self):
        for copy in self.copies:
            copy.wait_recv()
        self.mine[...] += self.land(0)[...] + (self.land(1)[...] + self.land(2)[...])
        for copy in self.copies:
            copy.wait_send()


class DirectGather:
    relays = False

    def __init__(self, copies, slot, place, ring, part):
        own = part(place, None)
        self.copies = [copies.make(own, own, slot + offset - 1, ring[offset]) for offset in (2, 1, 3)]

    def start(self):
        for copy in self.copies:
            copy.start()

    def finish(self):
        for copy in self.copies:
            copy.wait_recv()
        for copy in self.copies:
            copy.wait_send()


def split(value):
    high = value.astype(jnp.bfloat16)
    return high, (value - high.astype(jnp.float32)).astype(jnp.bfloat16)


def three_pass(left, right, dims):
    def one(a, b):
        return lax.dot_general(a, b, (dims, ((), ())), preferred_element_type=jnp.float32)

    count = left.shape[0] // 2
    both = one(left, right[0])
    return both[:count] + (both[count:] + one(left[:count], right[1]))


class TotalSum:
    def __init__(self, copies, position, mate, peers, x_peers, buffers):
        core, x, c = position
        self.x = x
        self.total, self.result, self.land_core, self.land_plane, self.land_x = buffers
        half = self.total.shape[0] // 2
        size = half // 16

        def rows(ref, first, count):
            return ref.at[pl.ds(pl.multiple_of(first, size), count), :]

        def piece(ref, t):
            return rows(ref, core * half + t * size, size)

        self.mine = rows(self.total, core * half, half)
        self.swap = copies.make(rows(self.total, (1 - core) * half, half), self.land_core, copies.reserve(1), mate)
        self.own, self.summed = piece(self.total, c), piece(self.result, c)
        self.there, self.along, self.back = [], [], []
        for offset, peer in peers:
            source, target = piece(self.total, (c + offset) % 16), self.land_plane.at[offset]
            self.there.append(copies.make(source, target, copies.reserve(1), peer))
            self.back.append(copies.make(self.summed, self.summed, copies.reserve(1), peer))
        for offset, peer in x_peers:
            self.along.append(copies.make(self.land_x.at[0], self.land_x.at[offset], copies.reserve(1), peer))
        whole = rows(self.result, core * half, half)
        self.give = copies.make(whole, whole, copies.reserve(1), mate)

    def steps(self):
        self.swap.start()
        yield
        self.swap.wait_recv()
        self.mine[...] += self.land_core[...]
        for copy in self.there:
            copy.start()
        yield
        value = self.own[...]
        for offset, copy in enumerate(self.there, 1):
            copy.wait_recv()
            value = value + self.land_plane[offset]
        self.land_x[0] = value
        for copy in self.along:
            copy.start()
        yield
        for copy in self.along:
            copy.wait_recv()
        value = self.land_x[self.x % 4]
        for at in range(1, 4):
            value = value + self.land_x[(self.x + 4 - at) % 4]
        self.summed[...] = value
        for copy in self.back:
            copy.start()
        yield
        for copy in self.back:
            copy.wait_recv()
        self.give.start()
        for copy in (self.swap, *self.there, *self.along, *self.back):
            copy.wait_send()
        yield
        self.give.wait()


STREAMS = 2
PIECES_A_WAIT = 3
SCATTERS = (Scatter, DirectScatter, DirectScatter)
GATHERS = (DirectGather, Gather, DirectGather)


def whole_kernel(
    count, interval_ref, block_ref, start_ref, basis_ref, projected_ref, residual_ref,
    block, other, high, low, rows, row_parts, cols, col_parts, vec,
    land_big, land_small, land_col, row_prev, col_prev, first_part,
    start_land, first_land, last_land, image_land, slab_ref, image_ref, before_ref, inverse_ref,
    *rest,
):
    sum_buffers = [rest[5 * k : 5 * k + 5] for k in range(3)]
    tile, pend_left, pend_right, send, recv, local_sem = rest[15:]
    r, c = lax.axis_index("row"), lax.axis_index("col")
    core, x, y, z = r % 2, r // 2, c % 4, c // 4
    copies = Copies(send, recv)

    def device(x, core, y, z):
        return (2 * x + core, 4 * z + y)

    mate = device(x, 1 - core, y, z)
    ring_x = {offset: device((x + offset) % 4, core, y, z) for offset in (1, 2, 3)}
    ring_y = {offset: device(x, core, (y + offset) % 4, z) for offset in (1, 2, 3)}
    ring_z = {offset: device(x, core, y, (z + offset) % 4) for offset in (1, 2, 3)}
    crossed = x != z

    local = pltpu.make_async_copy(block_ref, block, local_sem)
    local.start()
    barrier = pltpu.get_barrier_semaphore()

    def greet(who):
        pl.semaphore_signal(barrier, inc=1, device_id=who, device_id_type=MESH)

    peers = [(offset, (r, (c + offset) % 16)) for offset in range(1, 16)]
    x_peers = list(ring_x.items())
    for who in (mate, *(peer for _, peer in x_peers), *(peer for _, peer in peers)):
        greet(who)

    @pl.when(crossed)
    def _():
        greet(device(z, core, y, x))
        greet(device(z, 1 - core, y, x))

    pl.semaphore_wait(barrier, jnp.where(crossed, 21, 19))

    block_rows, block_cols = block.shape
    slab = start_ref.shape[0]
    width = start_ref.shape[1] // 2
    mine_cols = pl.ds(pl.multiple_of(core * width, width), width)
    mate_cols = pl.ds(pl.multiple_of((1 - core) * width, width), width)

    start_copy = copies.make(start_ref.at[:, mate_cols], start_land, copies.reserve(1), mate)
    start_copy.start()
    block_copy = copies.make(block_ref, other, copies.reserve(1), mate)
    block_copy.start()

    lower_end = jnp.full((1, block_cols), interval_ref[0], jnp.float32)
    upper_end = jnp.full((1, block_cols), interval_ref[1], jnp.float32)
    center = 0.5 * (lower_end + upper_end)
    inverse_width = 1.0 / (0.5 * (upper_end - lower_end))

    def prepare(source, which):
        base = which * block_rows
        step = 256

        @pl.loop(0, block_rows // step)
        def _(i):
            at = pl.multiple_of(i * step, step)
            value = source[pl.ds(at, step), :]
            row = lax.broadcasted_iota(jnp.int32, value.shape, 0) + (2 * x * block_rows + base + at)
            col = lax.broadcasted_iota(jnp.int32, value.shape, 1) + c * block_cols
            value = jnp.where(row == col, value - center, value) * inverse_width
            big, small = split(value)
            to = pl.ds(pl.multiple_of(base + at, step), step)
            high[to, :] = big
            low[to, :] = small

    start_copy.wait_recv()
    own = start_ref[:, mine_cols]
    theirs = start_land[...]
    lower = jnp.where(core == 0, own, theirs)
    upper = jnp.where(core == 0, theirs, own)
    piece = jnp.concatenate([lower, upper], axis=0).T
    cols[x] = piece
    col_prev[...] = piece

    places = {"y": y, "z": z}
    rings = {"y": ring_y, "z": ring_z}
    orders = (("z", "y"), ("y", "z"))
    share = width // STREAMS
    half = share // 2

    class Stream:
        def __init__(self, index):
            self.base = index * share
            self.at_first = self.at_last = False
            self.all = pl.ds(self.base, share)
            slots = [[copies.reserve(6) for _ in range(2)] for _ in range(2)]
            self.scatters = [[self.scatter(index, u, stage, slots[u][stage]) for stage in range(2)] for u in range(2)]
            slots = [[copies.reserve(4) for _ in range(2)] for _ in range(2)]
            self.gathers = [[self.gather(u, stage, slots[u][stage]) for stage in range(2)] for u in range(2)]
            self.col_scatter = SCATTERS[2](
                copies, copies.reserve(6), x, ring_x, self.col_slice(col_parts), lambda i: land_col.at[index, i]
            )
            self.col_gather = GATHERS[2](copies, copies.reserve(4), x, ring_x, self.col_slice(cols))

        def span(self, colour, side):
            size = half if side is None else half // 2
            return pl.ds(self.base + colour * half + (0 if side is None else side * size), size)

        def col_slice(self, ref):
            def part(t, side):
                return ref.at[t, self.all if side is None else self.span(side, None), :]
            return part

        def plane(self, ref, colour, axis):
            def part(t, side):
                at = self.span(colour, side)
                return ref.at[:, t, at, :] if axis == "z" else ref.at[t, :, at, :]
            return part

        def line(self, ref, colour, axis):
            def part(t, side):
                at = self.span(colour, side)
                return ref.at[y, t, at, :] if axis == "z" else ref.at[t, z, at, :]
            return part

        def scatter(self, index, colour, stage, slot):
            axis = orders[colour][stage]
            part = (self.plane if stage == 0 else self.line)(row_parts, colour, axis)
            landing = land_big if stage == 0 else land_small
            return SCATTERS[stage](copies, slot, places[axis], rings[axis], part, lambda i: landing.at[index, colour, i])

        def gather(self, colour, stage, slot):
            axis = orders[colour][1 - stage]
            part = (self.line if stage == 0 else self.plane)(rows, colour, axis)
            return GATHERS[stage](copies, slot, places[axis], rings[axis], part)

        def multiply(self):
            for q in range(4):
                big, small = split(cols[q, self.all, :])
                vec[:share, q * CHUNK : (q + 1) * CHUNK] = big
                vec[share:, q * CHUNK : (q + 1) * CHUNK] = small

            @pl.loop(0, 8, unroll=4)
            def _(i):
                at = pl.ds(pl.multiple_of(i * 256, 256), 256)
                out = three_pass(vec[...], (high[at, :], low[at, :]), ((1,), (1,)))
                row_parts[i // 2, 2 * (i % 2), self.all, :] = out[:, :CHUNK]
                row_parts[i // 2, 2 * (i % 2) + 1, self.all, :] = out[:, CHUNK:]

        def multiply_turned(self):
            def one(i):
                at = pl.ds(pl.multiple_of(i * 1024, 1024), 1024)
                wide = jnp.concatenate([rows[2 * i + k // 4, k % 4, self.all, :] for k in range(8)], axis=1)
                left = jnp.concatenate(split(wide), axis=0)
                return three_pass(left, (high[at, :], low[at, :]), ((1,), (0,)))

            out = one(0) + one(1)
            for q in range(4):
                col_parts[q, self.all, :] = out[:, q * CHUNK : (q + 1) * CHUNK]

        def to_rows(self):
            self.multiply()
            firsts = [self.scatters[0][0], self.scatters[1][0]]
            seconds = [self.scatters[0][1], self.scatters[1][1]]
            for first in firsts:
                first.start()
            yield
            if firsts[0].relays:
                for first in firsts:
                    first.relay()
                yield
            for first, second in zip(firsts, seconds):
                first.finish()
                second.start()
            yield
            if seconds[0].relays:
                for second in seconds:
                    second.relay()
                yield

        def gather_rows(self, step):
            for colour in range(2):
                self.scatters[colour][1].finish()
                at = self.span(colour, None)
                value = row_parts[y, z, at, :]
                if step > 0:
                    value = 2.0 * value - row_prev[at, :]
                rows[y, z, at, :] = value
                row_prev[at, :] = value
                if step == 1:
                    first_part[at, :] = value
                self.gathers[colour][0].start()
            self.at_first = step >= 1
            yield
            for stage in range(2):
                pair = [self.gathers[0][stage], self.gathers[1][stage]]
                if pair[0].relays:
                    for one in pair:
                        one.forward()
                    yield
                for colour in range(2):
                    pair[colour].finish()
                    if stage == 0:
                        self.gathers[colour][1].start()
                if stage == 0:
                    yield

        def to_cols(self, step):
            self.multiply_turned()
            self.col_scatter.start()
            yield
            if self.col_scatter.relays:
                self.col_scatter.relay()
                yield
            self.col_scatter.finish()
            value = col_parts[x, self.all, :]
            if step != 1:
                value = 2.0 * value - col_prev[self.all, :]
            cols[x, self.all, :] = value
            col_prev[self.all, :] = value
            self.col_gather.start()
            self.at_last = step == 2
            yield
            if self.col_gather.relays:
                self.col_gather.forward()
                yield
            self.col_gather.finish()

        def run(self):
            for step in range(3):
                yield from self.to_rows()
                yield from self.gather_rows(step)
                yield from self.to_cols(step)
            yield from self.to_rows()
            for colour in range(2):
                self.scatters[colour][1].finish()

    streams = [Stream(index) for index in range(STREAMS)]
    for stream in streams:
        stream.col_gather.start()
    local.wait()
    prepare(block, core)
    for stream in streams:
        if stream.col_gather.relays:
            stream.col_gather.forward()
    start_copy.wait_send()
    block_copy.wait_recv()
    prepare(other, 1 - core)
    block_copy.wait_send()
    for stream in streams:
        stream.col_gather.finish()

    keep = pl.ds(pl.multiple_of(core * slab, slab), slab)
    give = pl.ds(pl.multiple_of((1 - core) * slab, slab), slab)
    top = pl.ds(0, slab)
    sums = [TotalSum(copies, (core, x, c), mate, peers, x_peers, buffers) for buffers in sum_buffers]

    def trade(piece, land, target):
        land[1] = piece.T
        copy = copies.make(land.at[1, give, :], land.at[0, give, :], copies.reserve(1), mate)
        copy.start()
        yield
        copy.wait()
        target[:, mine_cols] = land[1, keep, :]
        target[:, mate_cols] = land[0, keep, :]

    def first_chain():
        yield from trade(first_part[...], first_land, slab_ref)
        sums[0].total[...] = contract(slab_ref[...], slab_ref[...], 0, 0)
        yield from sums[0].steps()
        sums[0].total[...] = sums[0].result[...] / count
        yield from factor_steps(2, sums[0].total, before_ref, tile, pend_left, pend_right)

    def last_chain():
        yield from trade(col_prev[...], last_land, slab_ref)
        slab_ref[...] = contract(slab_ref[...], before_ref[...], 1, 1)
        sums[1].total[...] = contract(slab_ref[...], slab_ref[...], 0, 0)
        yield from sums[1].steps()
        sums[1].total[...] = sums[1].result[...] / count
        yield from factor_steps(2, sums[1].total, inverse_ref, tile, pend_left, pend_right)
        basis_ref[...] = contract(slab_ref[...], inverse_ref[...], 1, 1)

    def image_chain():
        image_land[2, :, :] = row_parts[y, z].T
        slots = copies.reserve(2)
        same = copies.make(image_land.at[2, keep, :], image_land.at[0, top, :], slots, device(z, core, y, x))
        cross = copies.make(image_land.at[2, give, :], image_land.at[1, top, :], slots + 1, device(z, 1 - core, y, x))
        cross.start()

        @pl.when(crossed)
        def _():
            same.start()

        yield

        @pl.when(crossed)
        def _():
            same.wait()

        @pl.when(jnp.logical_not(crossed))
        def _():
            image_land[0, top, :] = image_land[2, keep, :]

        cross.wait()
        image_ref[:, mine_cols] = image_land[0, top, :]
        image_ref[:, mate_cols] = image_land[1, top, :]
        image_ref[...] = contract(image_ref[...], before_ref[...], 1, 1)
        sums[2].total[...] = contract(slab_ref[...], image_ref[...], 0, 0)
        yield from sums[2].steps()

    class Chain:
        def __init__(self, steps):
            self.steps, self.ready, self.ended = steps, False, False

        def advance(self):
            if not self.ended:
                said = next(self.steps, "end")
                self.ready, self.ended = said == WORK, said == "end"

    runs = [Chain(stream.run()) for stream in streams]
    chains, begun = [], 0
    while not all(run.ended for run in runs):
        for index, run in enumerate(runs):
            run.advance()
            if chains and (chains[0].ready or index == len(runs) - 1):
                chains[0].advance()
                if chains[0].ended:
                    chains.pop(0)
        if begun == 0 and all(stream.at_first for stream in streams):
            chains.append(Chain(first_chain()))
            begun = 1
        if begun == 1 and all(stream.at_last for stream in streams):
            chains.append(Chain(last_chain()))
            begun = 2
    image = Chain(image_chain())
    while chains or not image.ended:
        image.advance()
        for turn in range(PIECES_A_WAIT):
            if chains and (chains[0].ready or turn == 0 or image.ended):
                chains[0].advance()
                if chains[0].ended:
                    chains.pop(0)

    inverse = inverse_ref[...]
    basis = basis_ref[...]
    projected = contract(product(inverse, sums[2].result[...] / count), inverse, 1, 1)
    projected_ref[...] = projected
    residual_ref[...] = contract(image_ref[...], inverse, 1, 1) - product(basis, projected)


def on_device(matrix, start_vectors, interval):
    block_rows, block_cols = matrix.shape
    slab, vectors = start_vectors.shape
    total_rows = slab * lax.axis_size("row") * lax.axis_size("col")
    width = vectors // 2
    share = width // STREAMS
    f32, bf16 = jnp.float32, jnp.bfloat16
    vmem = pl.BlockSpec(memory_space=pltpu.VMEM)
    tall = jax.ShapeDtypeStruct((slab, vectors), f32)
    square = jax.ShapeDtypeStruct((vectors, vectors), f32)
    one_sum = [
        pltpu.VMEM((vectors, vectors), f32),
        pltpu.VMEM((vectors, vectors), f32),
        pltpu.VMEM((vectors // 2, vectors), f32),
        pltpu.VMEM((16, vectors // 32, vectors), f32),
        pltpu.VMEM((4, vectors // 32, vectors), f32),
    ]
    return pl.pallas_call(
        functools.partial(whole_kernel, total_rows),
        out_shape=(tall, square, tall),
        in_specs=[pl.BlockSpec(memory_space=pltpu.SMEM), pl.BlockSpec(memory_space=pl.ANY), vmem],
        out_specs=(vmem,) * 3,
        scratch_shapes=[
            pltpu.VMEM((block_rows, block_cols), f32),
            pltpu.VMEM((block_rows, block_cols), f32),
            pltpu.VMEM((2 * block_rows, block_cols), bf16),
            pltpu.VMEM((2 * block_rows, block_cols), bf16),
            pltpu.VMEM((4, 4, width, CHUNK), f32),
            pltpu.VMEM((4, 4, width, CHUNK), f32),
            pltpu.VMEM((4, width, CHUNK), f32),
            pltpu.VMEM((4, width, CHUNK), f32),
            pltpu.VMEM((2 * share, block_cols), bf16),
            pltpu.VMEM((STREAMS, 2, 6, 4, share // 4, CHUNK), f32),
            pltpu.VMEM((STREAMS, 2, 3, share // 2, CHUNK), f32),
            pltpu.VMEM((STREAMS, 3, share, CHUNK), f32),
            pltpu.VMEM((width, CHUNK), f32),
            pltpu.VMEM((width, CHUNK), f32),
            pltpu.VMEM((width, CHUNK), f32),
            pltpu.VMEM((slab, width), f32),
            pltpu.VMEM((2, CHUNK, width), f32),
            pltpu.VMEM((2, CHUNK, width), f32),
            pltpu.VMEM((3, CHUNK, width), f32),
            pltpu.VMEM((slab, vectors), f32),
            pltpu.VMEM((slab, vectors), f32),
            pltpu.VMEM((vectors, vectors), f32),
            pltpu.VMEM((vectors, vectors), f32),
            *(one_sum * 3),
            pltpu.VMEM((BLOCK + PANEL, 2 * BLOCK), f32),
            pltpu.VMEM((BLOCK, 6 * PANEL), bf16),
            pltpu.VMEM((6 * PANEL, 2 * BLOCK), bf16),
            pltpu.SemaphoreType.DMA((256,)),
            pltpu.SemaphoreType.DMA((256,)),
            pltpu.SemaphoreType.DMA,
        ],
        compiler_params=pltpu.CompilerParams(
            collective_id=0, has_side_effects=True, vmem_limit_bytes=56 * 2**20
        ),
        cost_estimate=pl.CostEstimate(flops=10**10, bytes_accessed=4 * 10**6, transcendentals=0),
    )(interval, matrix, start_vectors)


def solution(mesh):
    return jax.shard_map(
        on_device,
        mesh=mesh,
        in_specs=(P("row", "col"), P(("col", "row"), None), P()),
        out_specs=(P(("col", "row"), None), P(), P(("col", "row"), None)),
        check_vma=False,
    )
```

```python
import functools

import jax
import jax.numpy as jnp
from jax import lax
from jax.experimental import pallas as pl
from jax.experimental.pallas import tpu as pltpu
from jax.sharding import PartitionSpec as P

FILTER_DEG = 3
OUTER = 2
PANEL = 16
BLOCK = 128
WORK = "work"
MESH = pl.DeviceIdType.MESH
CHUNK = 128


def product(left, right, precision=lax.Precision.HIGHEST):
    return jnp.dot(left, right, precision=precision, preferred_element_type=jnp.float32)


def contract(left, right, left_dim, right_dim):
    return lax.dot_general(
        left,
        right,
        (((left_dim,), (right_dim,)), ((), ())),
        precision=lax.Precision.HIGHEST,
        preferred_element_type=jnp.float32,
    )


def lane_columns(rows, first):
    narrow = rows[:, :128]
    lanes = jnp.zeros(narrow.shape, jnp.int32) + first
    return [jnp.take_along_axis(narrow, lanes + j, axis=1) for j in range(PANEL)]


def row_of(value, step):
    return jnp.broadcast_to(value[step : step + 1, :], value.shape)


def three_parts(value):
    high = value.astype(jnp.bfloat16).astype(jnp.float32)
    rest = value - high
    middle = rest.astype(jnp.bfloat16).astype(jnp.float32)
    return high, middle, rest - middle


def factor_panels(tile, pend_left, pend_right, begin, end):
    block = tile.shape[1] // 2
    sub = lax.broadcasted_iota(jnp.int32, (PANEL, 128), 0)
    lane = lax.broadcasted_iota(jnp.int32, (PANEL, block), 1)

    def panel(p, carry):
        first = pl.multiple_of(p * PANEL, PANEL)
        here, after = pl.ds(first, PANEL), pl.ds(pl.multiple_of(first + PANEL, PANEL), PANEL)
        rows = tile[here, :]
        tile[:block, :] -= jnp.dot(pend_left[...], pend_right[...], preferred_element_type=jnp.float32)

        columns = lane_columns(rows, first)
        left, right = rows[:, :block], rows[:, block:]
        inverses = []
        pivots = jnp.ones((PANEL, 128), jnp.float32)
        for s in range(PANEL):
            pivot = row_of(columns[s], s)
            pivots = jnp.where(sub == s, pivot, pivots)
            inverse = 1.0 / pivot
            inverses.append(inverse)
            if s < PANEL - 1:
                ratio = jnp.where(sub > s, columns[s] * inverse, 0.0)
                for j in range(s + 1, PANEL):
                    columns[j] = columns[j] - ratio * row_of(columns[j], s)
                left = left - ratio * row_of(left, s)
                right = right - ratio * row_of(right, s)

        scale = lax.rsqrt(pivots)
        done_left, done_right = left * scale, right * scale
        tile[here, :block] = done_left
        tile[here, block:] = done_right
        a = three_parts(jnp.where(lane >= first + 2 * PANEL, done_left, 0.0))
        pend_left[...] = jnp.concatenate([a[0], a[0], a[1], a[1], a[0], a[2]], axis=0).T.astype(jnp.bfloat16)
        b = three_parts(jnp.concatenate([done_left, done_right], axis=1))
        pend_right[...] = jnp.concatenate([b[0], b[1], b[0], b[1], b[2], b[0]], axis=0).astype(jnp.bfloat16)

        following = tile[after, :]
        others = lane_columns(following, first)
        next_left, next_right = following[:, :block], following[:, block:]
        for s in range(PANEL):
            ratio = others[s] * inverses[s]
            for j in range(s + 1, PANEL):
                others[j] = others[j] - ratio * row_of(columns[j], s)
            next_left = next_left - ratio * row_of(left, s)
            next_right = next_right - ratio * row_of(right, s)
        tile[after, :block] = next_left
        tile[after, block:] = next_right
        return carry

    lax.fori_loop(begin, end, panel, 0)


def factor_steps(pieces, work, inverse_ref, tile, pend_left, pend_right):
    order, block = work.shape[0], BLOCK
    at_row = lax.broadcasted_iota(jnp.int32, (order, order), 0)
    at_col = lax.broadcasted_iota(jnp.int32, (order, order), 1)
    inverse_ref[...] = (at_row == at_col).astype(jnp.float32)
    row = lax.broadcasted_iota(jnp.int32, (block, block), 0)
    col = lax.broadcasted_iota(jnp.int32, (block, block), 1)
    panels = block // PANEL
    for at in range(0, order, block):
        stop = at + block
        tile[:block, :block] = work[at:stop, at:stop]
        tile[:block, block:] = (row == col).astype(jnp.float32)
        tile[block:, :] = jnp.zeros((PANEL, 2 * block), jnp.float32)
        pend_left[...] = jnp.zeros_like(pend_left)
        pend_right[...] = jnp.zeros_like(pend_right)
        for piece in range(pieces):
            factor_panels(tile, pend_left, pend_right, piece * panels // pieces, (piece + 1) * panels // pieces)
            yield WORK
        small = jnp.where(row >= col, tile[:block, block:], 0.0)
        solved = product(small, inverse_ref[at:stop, :stop])
        inverse_ref[at:stop, :stop] = solved
        if stop < order:
            below = contract(work[stop:, at:stop], small, 1, 1)
            work[stop:, stop:] -= contract(below, below, 1, 1)
            inverse_ref[stop:, :stop] -= product(below, solved)
            yield WORK


class Copies:
    def __init__(self, send, recv):
        self.send, self.recv, self.used = send, recv, 0

    def reserve(self, count):
        first = self.used
        self.used += count
        return first

    def make(self, source, target, slot, device):
        return pltpu.make_async_remote_copy(
            src_ref=source,
            dst_ref=target,
            send_sem=self.send.at[slot],
            recv_sem=self.recv.at[slot],
            device_id=device,
            device_id_type=MESH,
        )


class Scatter:
    relays = True

    def __init__(self, copies, slot, place, ring, part, land):
        self.place, self.part, self.land = place, part, land
        left, right = ring[3], ring[1]
        ahead, behind, across = (place + 1) % 4, (place + 3) % 4, (place + 2) % 4
        self.ahead, self.behind = ahead, behind
        plan = (
            (part(across, 0), right),
            (part(across, 1), left),
            (part(ahead, 1), right),
            (part(behind, 0), left),
            (part(ahead, 0), right),
            (part(behind, 1), left),
        )
        self.copies = [
            copies.make(source, land(i), slot + i, device) for i, (source, device) in enumerate(plan)
        ]

    def start(self):
        for copy in self.copies[:4]:
            copy.start()

    def relay(self):
        for first, half, target in ((0, 0, self.ahead), (1, 1, self.behind)):
            self.copies[first].wait_recv()
            mine = self.part(target, half)
            mine[...] += self.land(first)[...]
            self.copies[4 + first].start()

    def finish(self):
        for copy in self.copies[2:]:
            copy.wait_recv()
        for half, terms in ((0, (3, 4)), (1, (2, 5))):
            mine = self.part(self.place, half)
            mine[...] += self.land(terms[0])[...] + self.land(terms[1])[...]
        for copy in self.copies:
            copy.wait_send()


class Gather:
    relays = True

    def __init__(self, copies, slot, place, ring, part):
        left, right = ring[3], ring[1]
        ahead, behind = (place + 1) % 4, (place + 3) % 4
        self.copies = [
            copies.make(part(place, None), part(place, None), slot, right),
            copies.make(part(place, None), part(place, None), slot + 1, left),
            copies.make(part(behind, 0), part(behind, 0), slot + 2, right),
            copies.make(part(ahead, 1), part(ahead, 1), slot + 3, left),
        ]

    def start(self):
        for copy in self.copies[:2]:
            copy.start()

    def forward(self):
        for first in range(2):
            self.copies[first].wait_recv()
            self.copies[2 + first].start()

    def finish(self):
        for copy in self.copies[2:]:
            copy.wait_recv()
        for copy in self.copies:
            copy.wait_send()


class DirectScatter:
    relays = False

    def __init__(self, copies, slot, place, ring, part, land):
        self.mine, self.land = part(place, None), land
        self.copies = [
            copies.make(part((place + offset) % 4, None), land(offset - 1), slot + offset - 1, ring[offset])
            for offset in (2, 1, 3)
        ]

    def start(self):
        for copy in self.copies:
            copy.start()

    def finish(self):
        for copy in self.copies:
            copy.wait_recv()
        self.mine[...] += self.land(0)[...] + (self.land(1)[...] + self.land(2)[...])
        for copy in self.copies:
            copy.wait_send()


class DirectGather:
    relays = False

    def __init__(self, copies, slot, place, ring, part):
        own = part(place, None)
        self.copies = [copies.make(own, own, slot + offset - 1, ring[offset]) for offset in (2, 1, 3)]

    def start(self):
        for copy in self.copies:
            copy.start()

    def finish(self):
        for copy in self.copies:
            copy.wait_recv()
        for copy in self.copies:
            copy.wait_send()


def split(value):
    high = value.astype(jnp.bfloat16)
    return high, (value - high.astype(jnp.float32)).astype(jnp.bfloat16)


def three_pass(left, right, dims):
    def one(a, b):
        return lax.dot_general(a, b, (dims, ((), ())), preferred_element_type=jnp.float32)

    count = left.shape[0] // 2
    both = one(left, right[0])
    return both[:count] + (both[count:] + one(left[:count], right[1]))


class TotalSum:
    def __init__(self, copies, position, mate, peers, x_peers, buffers):
        core, x, c = position
        self.x = x
        self.total, self.result, self.land_plane, self.land_x = buffers
        half = self.total.shape[0]
        size = half // 16

        def rows(ref, first, count):
            return ref.at[pl.ds(pl.multiple_of(first, size), count), :]

        self.own, self.summed = rows(self.total, c * size, size), rows(self.result, core * half + c * size, size)
        self.there, self.along, self.back = [], [], []
        for offset, peer in peers:
            source, target = rows(self.total, (c + offset) % 16 * size, size), self.land_plane.at[offset]
            self.there.append(copies.make(source, target, copies.reserve(1), peer))
            self.back.append(copies.make(self.summed, self.summed, copies.reserve(1), peer))
        for offset, peer in x_peers:
            self.along.append(copies.make(self.land_x.at[0], self.land_x.at[offset], copies.reserve(1), peer))
        whole = rows(self.result, core * half, half)
        self.give = copies.make(whole, whole, copies.reserve(1), mate)

    def steps(self):
        for copy in self.there:
            copy.start()
        yield
        value = self.own[...]
        for offset, copy in enumerate(self.there, 1):
            copy.wait_recv()
            value = value + self.land_plane[offset]
        self.land_x[0] = value
        for copy in self.along:
            copy.start()
        yield
        for copy in self.along:
            copy.wait_recv()
        value = self.land_x[self.x % 4]
        for at in range(1, 4):
            value = value + self.land_x[(self.x + 4 - at) % 4]
        self.summed[...] = value
        for copy in self.back:
            copy.start()
        yield
        for copy in self.back:
            copy.wait_recv()
        self.give.start()
        for copy in (*self.there, *self.along, *self.back):
            copy.wait_send()
        yield
        self.give.wait()


STREAMS = 2
PIECES_A_WAIT = 3
SCATTERS = (Scatter, DirectScatter, DirectScatter)
GATHERS = (DirectGather, Gather, DirectGather)


def whole_kernel(
    count, interval_ref, block_ref, start_ref, basis_ref, projected_ref, residual_ref,
    block, other, high, low, rows, row_parts, cols, col_parts, vec,
    land_big, land_small, land_col, row_prev, col_prev, first_part,
    start_land, first_land, last_land, image_land, slab_ref, image_ref, before_ref, inverse_ref,
    *rest,
):
    sum_buffers = [rest[4 * k : 4 * k + 4] for k in range(3)]
    tile, pend_left, pend_right, send, recv, local_sem = rest[12:]
    r, c = lax.axis_index("row"), lax.axis_index("col")
    core, x, y, z = r % 2, r // 2, c % 4, c // 4
    copies = Copies(send, recv)

    def device(x, core, y, z):
        return (2 * x + core, 4 * z + y)

    mate = device(x, 1 - core, y, z)
    ring_x = {offset: device((x + offset) % 4, core, y, z) for offset in (1, 2, 3)}
    ring_y = {offset: device(x, core, (y + offset) % 4, z) for offset in (1, 2, 3)}
    ring_z = {offset: device(x, core, y, (z + offset) % 4) for offset in (1, 2, 3)}
    crossed = x != z

    local = pltpu.make_async_copy(block_ref, block, local_sem)
    local.start()
    barrier = pltpu.get_barrier_semaphore()

    def greet(who):
        pl.semaphore_signal(barrier, inc=1, device_id=who, device_id_type=MESH)

    peers = [(offset, (r, (c + offset) % 16)) for offset in range(1, 16)]
    x_peers = list(ring_x.items())
    across = {offset: device((x + offset) % 4, 1 - core, y, z) for offset in range(4)}
    for who in (*across.values(), *(peer for _, peer in x_peers), *(peer for _, peer in peers)):
        greet(who)

    @pl.when(crossed)
    def _():
        greet(device(z, core, y, x))
        greet(device(z, 1 - core, y, x))

    block_rows, block_cols = block.shape
    slab = start_ref.shape[0]
    width = start_ref.shape[1] // 2
    share = width // STREAMS
    half = share // 2
    mine_cols = pl.ds(pl.multiple_of(core * width, width), width)
    mate_cols = pl.ds(pl.multiple_of((1 - core) * width, width), width)

    lower_end = jnp.full((1, block_cols), interval_ref[0], jnp.float32)
    upper_end = jnp.full((1, block_cols), interval_ref[1], jnp.float32)
    center = 0.5 * (lower_end + upper_end)
    inverse_width = 1.0 / (0.5 * (upper_end - lower_end))

    def prepare(source, which):
        base = which * block_rows
        step = 256

        @pl.loop(0, block_rows // step)
        def _(i):
            at = pl.multiple_of(i * step, step)
            value = source[pl.ds(at, step), :]
            row = lax.broadcasted_iota(jnp.int32, value.shape, 0) + (2 * x * block_rows + base + at)
            col = lax.broadcasted_iota(jnp.int32, value.shape, 1) + c * block_cols
            value = jnp.where(row == col, value - center, value) * inverse_width
            big, small = split(value)
            to = pl.ds(pl.multiple_of(base + at, step), step)
            high[to, :] = big
            low[to, :] = small

    local.wait()
    prepare(block, core)
    start_land[r] = start_ref[:, mine_cols]
    pl.semaphore_wait(barrier, jnp.where(crossed, 24, 22))

    start_copies = []
    for index in range(STREAMS):
        lanes = pl.ds(index * share, share)
        own = start_ref.at[:, pl.ds(pl.multiple_of(core * width + index * share, share), share)]
        theirs = start_ref.at[:, pl.ds(pl.multiple_of((1 - core) * width + index * share, share), share)]
        ways = [(theirs, across[0])]
        for offset in (2, 1, 3):
            ways += [(own, ring_x[offset]), (theirs, across[offset])]
        start_copies.append([
            copies.make(source, start_land.at[r, :, lanes], copies.reserve(1), peer) for source, peer in ways
        ])
    for group in start_copies:
        for copy in group:
            copy.start()
    block_copy = copies.make(block_ref, other, copies.reserve(1), mate)
    block_copy.start()

    places = {"y": y, "z": z}
    rings = {"y": ring_y, "z": ring_z}
    orders = (("z", "y"), ("y", "z"))

    class Stream:
        def __init__(self, index):
            self.base = index * share
            self.at_first = self.at_last = False
            self.all = pl.ds(self.base, share)
            slots = [[copies.reserve(6) for _ in range(2)] for _ in range(2)]
            self.scatters = [[self.scatter(index, u, stage, slots[u][stage]) for stage in range(2)] for u in range(2)]
            slots = [[copies.reserve(4) for _ in range(2)] for _ in range(2)]
            self.gathers = [[self.gather(u, stage, slots[u][stage]) for stage in range(2)] for u in range(2)]
            self.col_scatter = SCATTERS[2](
                copies, copies.reserve(6), x, ring_x, self.col_slice(col_parts), lambda i: land_col.at[index, i]
            )
            self.col_gather = GATHERS[2](copies, copies.reserve(4), x, ring_x, self.col_slice(cols))

        def span(self, colour, side):
            size = half if side is None else half // 2
            return pl.ds(self.base + colour * half + (0 if side is None else side * size), size)

        def col_slice(self, ref):
            def part(t, side):
                return ref.at[t, self.all if side is None else self.span(side, None), :]
            return part

        def plane(self, ref, colour, axis):
            def part(t, side):
                at = self.span(colour, side)
                return ref.at[:, t, at, :] if axis == "z" else ref.at[t, :, at, :]
            return part

        def line(self, ref, colour, axis):
            def part(t, side):
                at = self.span(colour, side)
                return ref.at[y, t, at, :] if axis == "z" else ref.at[t, z, at, :]
            return part

        def scatter(self, index, colour, stage, slot):
            axis = orders[colour][stage]
            part = (self.plane if stage == 0 else self.line)(row_parts, colour, axis)
            landing = land_big if stage == 0 else land_small
            return SCATTERS[stage](copies, slot, places[axis], rings[axis], part, lambda i: landing.at[index, colour, i])

        def gather(self, colour, stage, slot):
            axis = orders[colour][1 - stage]
            part = (self.line if stage == 0 else self.plane)(rows, colour, axis)
            return GATHERS[stage](copies, slot, places[axis], rings[axis], part)

        def multiply(self):
            for q in range(4):
                big, small = split(cols[q, self.all, :])
                vec[:share, q * CHUNK : (q + 1) * CHUNK] = big
                vec[share:, q * CHUNK : (q + 1) * CHUNK] = small

            @pl.loop(0, 8, unroll=4)
            def _(i):
                at = pl.ds(pl.multiple_of(i * 256, 256), 256)
                out = three_pass(vec[...], (high[at, :], low[at, :]), ((1,), (1,)))
                row_parts[i // 2, 2 * (i % 2), self.all, :] = out[:, :CHUNK]
                row_parts[i // 2, 2 * (i % 2) + 1, self.all, :] = out[:, CHUNK:]

        def multiply_turned(self):
            def one(i):
                at = pl.ds(pl.multiple_of(i * 1024, 1024), 1024)
                wide = jnp.concatenate([rows[2 * i + k // 4, k % 4, self.all, :] for k in range(8)], axis=1)
                left = jnp.concatenate(split(wide), axis=0)
                return three_pass(left, (high[at, :], low[at, :]), ((1,), (0,)))

            out = one(0) + one(1)
            for q in range(4):
                col_parts[q, self.all, :] = out[:, q * CHUNK : (q + 1) * CHUNK]

        def to_rows(self):
            self.multiply()
            firsts = [self.scatters[0][0], self.scatters[1][0]]
            seconds = [self.scatters[0][1], self.scatters[1][1]]
            for first in firsts:
                first.start()
            yield
            if firsts[0].relays:
                for first in firsts:
                    first.relay()
                yield
            for first, second in zip(firsts, seconds):
                first.finish()
                second.start()
            yield
            if seconds[0].relays:
                for second in seconds:
                    second.relay()
                yield

        def gather_rows(self, step):
            for colour in range(2):
                self.scatters[colour][1].finish()
                at = self.span(colour, None)
                value = row_parts[y, z, at, :]
                if step > 0:
                    value = 2.0 * value - row_prev[at, :]
                rows[y, z, at, :] = value
                row_prev[at, :] = value
                if step == 1:
                    first_part[at, :] = value
                self.gathers[colour][0].start()
            self.at_first = step >= 1
            yield
            for stage in range(2):
                pair = [self.gathers[0][stage], self.gathers[1][stage]]
                if pair[0].relays:
                    for one in pair:
                        one.forward()
                    yield
                for colour in range(2):
                    pair[colour].finish()
                    if stage == 0:
                        self.gathers[colour][1].start()
                if stage == 0:
                    yield

        def to_cols(self, step):
            self.multiply_turned()
            self.col_scatter.start()
            yield
            if self.col_scatter.relays:
                self.col_scatter.relay()
                yield
            self.col_scatter.finish()
            value = col_parts[x, self.all, :]
            if step != 1:
                value = 2.0 * value - col_prev[self.all, :]
            cols[x, self.all, :] = value
            col_prev[self.all, :] = value
            self.col_gather.start()
            self.at_last = step == 2
            yield
            if self.col_gather.relays:
                self.col_gather.forward()
                yield
            self.col_gather.finish()

        def begin(self):
            lanes = pl.ds(self.base, share)
            for copy in start_copies[self.base // share]:
                copy.wait_recv()
            for q in range(4):
                both = [start_land[2 * q, :, lanes], start_land[2 * q + 1, :, lanes]]
                cols[q, self.all, :] = jnp.concatenate(both, axis=0).T
            col_prev[self.all, :] = cols[x, self.all, :]

        def run(self):
            self.begin()
            for step in range(3):
                yield from self.to_rows()
                yield from self.gather_rows(step)
                yield from self.to_cols(step)
            yield from self.to_rows()
            for colour in range(2):
                self.scatters[colour][1].finish()

    streams = [Stream(index) for index in range(STREAMS)]
    block_copy.wait_recv()
    prepare(other, 1 - core)
    block_copy.wait_send()

    keep = pl.ds(pl.multiple_of(core * slab, slab), slab)
    sums = [TotalSum(copies, (core, x, c), mate, peers, x_peers, buffers) for buffers in sum_buffers]

    def trade(piece, land, target):
        land[1] = piece.T
        copy = copies.make(land.at[1], land.at[0], copies.reserve(1), mate)
        copy.start()
        yield
        copy.wait()
        target[:, mine_cols] = land[1]
        target[:, mate_cols] = land[0]

    def first_chain():
        yield from trade(first_part[...], first_land, slab_ref)
        sums[0].total[...] = contract(slab_ref[:, mine_cols], slab_ref[...], 0, 0)
        yield from sums[0].steps()
        sums[0].result[...] = sums[0].result[...] / count
        yield from factor_steps(2, sums[0].result, before_ref, tile, pend_left, pend_right)

    def last_chain():
        yield from trade(col_prev[...], last_land, slab_ref)
        slab_ref[...] = contract(slab_ref[...], before_ref[...], 1, 1)
        sums[1].total[...] = contract(slab_ref[:, mine_cols], slab_ref[...], 0, 0)
        yield from sums[1].steps()
        sums[1].result[...] = sums[1].result[...] / count
        yield from factor_steps(2, sums[1].result, inverse_ref, tile, pend_left, pend_right)
        basis_ref[...] = contract(slab_ref[keep, :], inverse_ref[...], 1, 1)

    def image_chain():
        image_land[2] = row_parts[y, z].T
        slots = copies.reserve(2)
        same = copies.make(image_land.at[2], image_land.at[0], slots, device(z, core, y, x))
        cross = copies.make(image_land.at[2], image_land.at[1], slots + 1, device(z, 1 - core, y, x))
        cross.start()

        @pl.when(crossed)
        def _():
            same.start()

        yield

        @pl.when(crossed)
        def _():
            same.wait()

        @pl.when(jnp.logical_not(crossed))
        def _():
            image_land[0] = image_land[2]

        cross.wait()
        image_ref[:, mine_cols] = image_land[0]
        image_ref[:, mate_cols] = image_land[1]
        image_ref[...] = contract(image_ref[...], before_ref[...], 1, 1)
        sums[2].total[...] = contract(slab_ref[:, mine_cols], image_ref[...], 0, 0)
        yield from sums[2].steps()

    class Chain:
        def __init__(self, steps):
            self.steps, self.ready, self.ended = steps, False, False

        def advance(self):
            if not self.ended:
                said = next(self.steps, "end")
                self.ready, self.ended = said == WORK, said == "end"

    runs = [Chain(stream.run()) for stream in streams]
    chains, begun = [], 0
    while not all(run.ended for run in runs):
        for index, run in enumerate(runs):
            run.advance()
            if chains and (chains[0].ready or index == len(runs) - 1):
                chains[0].advance()
                if chains[0].ended:
                    chains.pop(0)
        if begun == 0 and all(stream.at_first for stream in streams):
            chains.append(Chain(first_chain()))
            begun = 1
        if begun == 1 and all(stream.at_last for stream in streams):
            chains.append(Chain(last_chain()))
            begun = 2
    image = Chain(image_chain())
    while chains or not image.ended:
        image.advance()
        for turn in range(PIECES_A_WAIT):
            if chains and (chains[0].ready or turn == 0 or image.ended):
                chains[0].advance()
                if chains[0].ended:
                    chains.pop(0)

    for group in start_copies:
        for copy in group:
            copy.wait_send()
    inverse = inverse_ref[...]
    basis = basis_ref[...]
    projected = contract(product(inverse, sums[2].result[...] / count), inverse, 1, 1)
    projected_ref[...] = projected
    residual_ref[...] = contract(image_ref[keep, :], inverse, 1, 1) - product(basis, projected)


def on_device(matrix, start_vectors, interval):
    block_rows, block_cols = matrix.shape
    slab, vectors = start_vectors.shape
    total_rows = slab * lax.axis_size("row") * lax.axis_size("col")
    width = vectors // 2
    share = width // STREAMS
    f32, bf16 = jnp.float32, jnp.bfloat16
    vmem = pl.BlockSpec(memory_space=pltpu.VMEM)
    tall = jax.ShapeDtypeStruct((slab, vectors), f32)
    square = jax.ShapeDtypeStruct((vectors, vectors), f32)
    one_sum = [
        pltpu.VMEM((vectors // 2, vectors), f32),
        pltpu.VMEM((vectors, vectors), f32),
        pltpu.VMEM((16, vectors // 32, vectors), f32),
        pltpu.VMEM((4, vectors // 32, vectors), f32),
    ]
    return pl.pallas_call(
        functools.partial(whole_kernel, total_rows),
        out_shape=(tall, square, tall),
        in_specs=[pl.BlockSpec(memory_space=pltpu.SMEM), pl.BlockSpec(memory_space=pl.ANY), vmem],
        out_specs=(vmem,) * 3,
        scratch_shapes=[
            pltpu.VMEM((block_rows, block_cols), f32),
            pltpu.VMEM((block_rows, block_cols), f32),
            pltpu.VMEM((2 * block_rows, block_cols), bf16),
            pltpu.VMEM((2 * block_rows, block_cols), bf16),
            pltpu.VMEM((4, 4, width, CHUNK), f32),
            pltpu.VMEM((4, 4, width, CHUNK), f32),
            pltpu.VMEM((4, width, CHUNK), f32),
            pltpu.VMEM((4, width, CHUNK), f32),
            pltpu.VMEM((2 * share, block_cols), bf16),
            pltpu.VMEM((STREAMS, 2, 6, 4, share // 4, CHUNK), f32),
            pltpu.VMEM((STREAMS, 2, 3, share // 2, CHUNK), f32),
            pltpu.VMEM((STREAMS, 3, share, CHUNK), f32),
            pltpu.VMEM((width, CHUNK), f32),
            pltpu.VMEM((width, CHUNK), f32),
            pltpu.VMEM((width, CHUNK), f32),
            pltpu.VMEM((8, slab, width), f32),
            pltpu.VMEM((2, CHUNK, width), f32),
            pltpu.VMEM((2, CHUNK, width), f32),
            pltpu.VMEM((3, CHUNK, width), f32),
            pltpu.VMEM((CHUNK, vectors), f32),
            pltpu.VMEM((CHUNK, vectors), f32),
            pltpu.VMEM((vectors, vectors), f32),
            pltpu.VMEM((vectors, vectors), f32),
            *(one_sum * 3),
            pltpu.VMEM((BLOCK + PANEL, 2 * BLOCK), f32),
            pltpu.VMEM((BLOCK, 6 * PANEL), bf16),
            pltpu.VMEM((6 * PANEL, 2 * BLOCK), bf16),
            pltpu.SemaphoreType.DMA((256,)),
            pltpu.SemaphoreType.DMA((256,)),
            pltpu.SemaphoreType.DMA,
        ],
        compiler_params=pltpu.CompilerParams(
            collective_id=0, has_side_effects=True, vmem_limit_bytes=56 * 2**20
        ),
        cost_estimate=pl.CostEstimate(flops=10**10, bytes_accessed=4 * 10**6, transcendentals=0),
    )(interval, matrix, start_vectors)


def solution(mesh):
    return jax.shard_map(
        on_device,
        mesh=mesh,
        in_specs=(P("row", "col"), P(("col", "row"), None), P()),
        out_specs=(P(("col", "row"), None), P(), P(("col", "row"), None)),
        check_vma=False,
    )
```

```python
import functools

import jax
import jax.numpy as jnp
from jax import lax
from jax.experimental import pallas as pl
from jax.experimental.pallas import tpu as pltpu
from jax.sharding import PartitionSpec as P

FILTER_DEG = 3
OUTER = 2
PANEL = 16
BLOCK = 128
WORK = "work"
MESH = pl.DeviceIdType.MESH
CHUNK = 128


def product(left, right, precision=lax.Precision.HIGHEST):
    return jnp.dot(left, right, precision=precision, preferred_element_type=jnp.float32)


def contract(left, right, left_dim, right_dim):
    return lax.dot_general(
        left,
        right,
        (((left_dim,), (right_dim,)), ((), ())),
        precision=lax.Precision.HIGHEST,
        preferred_element_type=jnp.float32,
    )


def lane_columns(rows, first):
    narrow = rows[:, :128]
    lanes = jnp.zeros(narrow.shape, jnp.int32) + first
    return [jnp.take_along_axis(narrow, lanes + j, axis=1) for j in range(PANEL)]


def row_of(value, step):
    return jnp.broadcast_to(value[step : step + 1, :], value.shape)


def three_parts(value):
    high = value.astype(jnp.bfloat16).astype(jnp.float32)
    rest = value - high
    middle = rest.astype(jnp.bfloat16).astype(jnp.float32)
    return high, middle, rest - middle


def factor_panels(tile, pend_left, pend_right, begin, end):
    block = tile.shape[1] // 2
    sub = lax.broadcasted_iota(jnp.int32, (PANEL, 128), 0)
    lane = lax.broadcasted_iota(jnp.int32, (PANEL, block), 1)

    def panel(p, carry):
        first = pl.multiple_of(p * PANEL, PANEL)
        here, after = pl.ds(first, PANEL), pl.ds(pl.multiple_of(first + PANEL, PANEL), PANEL)
        rows = tile[here, :]
        tile[:block, :] -= jnp.dot(pend_left[...], pend_right[...], preferred_element_type=jnp.float32)

        columns = lane_columns(rows, first)
        left, right = rows[:, :block], rows[:, block:]
        inverses = []
        pivots = jnp.ones((PANEL, 128), jnp.float32)
        for s in range(PANEL):
            pivot = row_of(columns[s], s)
            pivots = jnp.where(sub == s, pivot, pivots)
            inverse = 1.0 / pivot
            inverses.append(inverse)
            if s < PANEL - 1:
                ratio = jnp.where(sub > s, columns[s] * inverse, 0.0)
                for j in range(s + 1, PANEL):
                    columns[j] = columns[j] - ratio * row_of(columns[j], s)
                left = left - ratio * row_of(left, s)
                right = right - ratio * row_of(right, s)

        scale = lax.rsqrt(pivots)
        done_left, done_right = left * scale, right * scale
        tile[here, :block] = done_left
        tile[here, block:] = done_right
        a = three_parts(jnp.where(lane >= first + 2 * PANEL, done_left, 0.0))
        pend_left[...] = jnp.concatenate([a[0], a[0], a[1], a[1], a[0], a[2]], axis=0).T.astype(jnp.bfloat16)
        b = three_parts(jnp.concatenate([done_left, done_right], axis=1))
        pend_right[...] = jnp.concatenate([b[0], b[1], b[0], b[1], b[2], b[0]], axis=0).astype(jnp.bfloat16)

        following = tile[after, :]
        others = lane_columns(following, first)
        next_left, next_right = following[:, :block], following[:, block:]
        for s in range(PANEL):
            ratio = others[s] * inverses[s]
            for j in range(s + 1, PANEL):
                others[j] = others[j] - ratio * row_of(columns[j], s)
            next_left = next_left - ratio * row_of(left, s)
            next_right = next_right - ratio * row_of(right, s)
        tile[after, :block] = next_left
        tile[after, block:] = next_right
        return carry

    lax.fori_loop(begin, end, panel, 0)


def factor_steps(pieces, work, inverse_ref, tile, pend_left, pend_right):
    order, block = work.shape[0], BLOCK
    at_row = lax.broadcasted_iota(jnp.int32, (order, order), 0)
    at_col = lax.broadcasted_iota(jnp.int32, (order, order), 1)
    inverse_ref[...] = (at_row == at_col).astype(jnp.float32)
    row = lax.broadcasted_iota(jnp.int32, (block, block), 0)
    col = lax.broadcasted_iota(jnp.int32, (block, block), 1)
    panels = block // PANEL
    for at in range(0, order, block):
        stop = at + block
        tile[:block, :block] = work[at:stop, at:stop]
        tile[:block, block:] = (row == col).astype(jnp.float32)
        tile[block:, :] = jnp.zeros((PANEL, 2 * block), jnp.float32)
        pend_left[...] = jnp.zeros_like(pend_left)
        pend_right[...] = jnp.zeros_like(pend_right)
        for piece in range(pieces):
            factor_panels(tile, pend_left, pend_right, piece * panels // pieces, (piece + 1) * panels // pieces)
            yield WORK
        small = jnp.where(row >= col, tile[:block, block:], 0.0)
        solved = product(small, inverse_ref[at:stop, :stop])
        inverse_ref[at:stop, :stop] = solved
        if stop < order:
            below = contract(work[stop:, at:stop], small, 1, 1)
            work[stop:, stop:] -= contract(below, below, 1, 1)
            inverse_ref[stop:, :stop] -= product(below, solved)
            yield WORK


class Copies:
    def __init__(self, send, recv):
        self.send, self.recv, self.used = send, recv, 0

    def reserve(self, count):
        first = self.used
        self.used += count
        return first

    def make(self, source, target, slot, device):
        return pltpu.make_async_remote_copy(
            src_ref=source,
            dst_ref=target,
            send_sem=self.send.at[slot],
            recv_sem=self.recv.at[slot],
            device_id=device,
            device_id_type=MESH,
        )


class Scatter:
    relays = True

    def __init__(self, copies, slot, place, ring, part, land):
        self.place, self.part, self.land = place, part, land
        left, right = ring[3], ring[1]
        ahead, behind, across = (place + 1) % 4, (place + 3) % 4, (place + 2) % 4
        self.ahead, self.behind = ahead, behind
        plan = (
            (part(across, 0), right),
            (part(across, 1), left),
            (part(ahead, 1), right),
            (part(behind, 0), left),
            (part(ahead, 0), right),
            (part(behind, 1), left),
        )
        self.copies = [
            copies.make(source, land(i), slot + i, device) for i, (source, device) in enumerate(plan)
        ]

    def start(self):
        for copy in self.copies[:4]:
            copy.start()

    def relay(self):
        for first, half, target in ((0, 0, self.ahead), (1, 1, self.behind)):
            self.copies[first].wait_recv()
            mine = self.part(target, half)
            mine[...] += self.land(first)[...]
            self.copies[4 + first].start()

    def finish(self):
        for copy in self.copies[2:]:
            copy.wait_recv()
        for half, terms in ((0, (3, 4)), (1, (2, 5))):
            mine = self.part(self.place, half)
            mine[...] += self.land(terms[0])[...] + self.land(terms[1])[...]
        for copy in self.copies:
            copy.wait_send()


class Gather:
    relays = True

    def __init__(self, copies, slot, place, ring, part):
        left, right = ring[3], ring[1]
        ahead, behind = (place + 1) % 4, (place + 3) % 4
        self.copies = [
            copies.make(part(place, None), part(place, None), slot, right),
            copies.make(part(place, None), part(place, None), slot + 1, left),
            copies.make(part(behind, 0), part(behind, 0), slot + 2, right),
            copies.make(part(ahead, 1), part(ahead, 1), slot + 3, left),
        ]

    def start(self):
        for copy in self.copies[:2]:
            copy.start()

    def forward(self):
        for first in range(2):
            self.copies[first].wait_recv()
            self.copies[2 + first].start()

    def finish(self):
        for copy in self.copies[2:]:
            copy.wait_recv()
        for copy in self.copies:
            copy.wait_send()


class DirectScatter:
    relays = False

    def __init__(self, copies, slot, place, ring, part, land):
        self.mine, self.land = part(place, None), land
        self.copies = [
            copies.make(part((place + offset) % 4, None), land(offset - 1), slot + offset - 1, ring[offset])
            for offset in (2, 1, 3)
        ]

    def start(self):
        for copy in self.copies:
            copy.start()

    def finish(self):
        for copy in self.copies:
            copy.wait_recv()
        self.mine[...] += self.land(0)[...] + (self.land(1)[...] + self.land(2)[...])
        for copy in self.copies:
            copy.wait_send()


class DirectGather:
    relays = False

    def __init__(self, copies, slot, place, ring, part):
        own = part(place, None)
        self.copies = [copies.make(own, own, slot + offset - 1, ring[offset]) for offset in (2, 1, 3)]

    def start(self):
        for copy in self.copies:
            copy.start()

    def finish(self):
        for copy in self.copies:
            copy.wait_recv()
        for copy in self.copies:
            copy.wait_send()


def split(value):
    high = value.astype(jnp.bfloat16)
    return high, (value - high.astype(jnp.float32)).astype(jnp.bfloat16)


def three_pass(left, right, dims):
    def one(a, b):
        return lax.dot_general(a, b, (dims, ((), ())), preferred_element_type=jnp.float32)

    count = left.shape[0] // 2
    both = one(left, right[0])
    return both[:count] + (both[count:] + one(left[:count], right[1]))


def fine(left, right, right_dim):
    return three_pass(jnp.concatenate(split(left), axis=0), split(right), ((1,), (right_dim,)))


class TotalSum:
    def __init__(self, copies, position, mate, peers, x_peers, buffers):
        core, x, c = position
        self.x = x
        self.total, self.result, self.land_plane, self.land_x = buffers
        half = self.total.shape[0]
        size = half // 16

        def rows(ref, first, count):
            return ref.at[pl.ds(pl.multiple_of(first, size), count), :]

        self.own, self.summed = rows(self.total, c * size, size), rows(self.result, core * half + c * size, size)
        self.there, self.along, self.back = [], [], []
        for offset, peer in peers:
            source, target = rows(self.total, (c + offset) % 16 * size, size), self.land_plane.at[offset]
            self.there.append(copies.make(source, target, copies.reserve(1), peer))
            self.back.append(copies.make(self.summed, self.summed, copies.reserve(1), peer))
        for offset, peer in x_peers:
            self.along.append(copies.make(self.land_x.at[0], self.land_x.at[offset], copies.reserve(1), peer))
        whole = rows(self.result, core * half, half)
        self.give = copies.make(whole, whole, copies.reserve(1), mate)

    def steps(self):
        for copy in self.there:
            copy.start()
        yield
        value = self.own[...]
        for offset, copy in enumerate(self.there, 1):
            copy.wait_recv()
            value = value + self.land_plane[offset]
        self.land_x[0] = value
        for copy in self.along:
            copy.start()
        yield
        for copy in self.along:
            copy.wait_recv()
        value = self.land_x[self.x % 4]
        for at in range(1, 4):
            value = value + self.land_x[(self.x + 4 - at) % 4]
        self.summed[...] = value
        for copy in self.back:
            copy.start()
        yield
        for copy in self.back:
            copy.wait_recv()
        self.give.start()
        for copy in (*self.there, *self.along, *self.back):
            copy.wait_send()
        yield
        self.give.wait()


STREAMS = 2
PIECES_A_WAIT = 3
SCATTERS = (Scatter, DirectScatter, DirectScatter)
GATHERS = (DirectGather, Gather, DirectGather)


def whole_kernel(
    count, interval_ref, block_ref, start_ref, basis_ref, projected_ref, residual_ref,
    block, other, high, low, rows, row_parts, cols, col_parts, vec,
    land_big, land_small, land_col, row_prev, col_prev, first_part,
    start_land, first_land, last_land, image_land, slab_ref, image_ref, before_ref, inverse_ref,
    *rest,
):
    sum_buffers = [rest[4 * k : 4 * k + 4] for k in range(3)]
    tile, pend_left, pend_right, send, recv, local_sem = rest[12:]
    r, c = lax.axis_index("row"), lax.axis_index("col")
    core, x, y, z = r % 2, r // 2, c % 4, c // 4
    copies = Copies(send, recv)

    def device(x, core, y, z):
        return (2 * x + core, 4 * z + y)

    mate = device(x, 1 - core, y, z)
    ring_x = {offset: device((x + offset) % 4, core, y, z) for offset in (1, 2, 3)}
    ring_y = {offset: device(x, core, (y + offset) % 4, z) for offset in (1, 2, 3)}
    ring_z = {offset: device(x, core, y, (z + offset) % 4) for offset in (1, 2, 3)}
    crossed = x != z

    local = pltpu.make_async_copy(block_ref, block, local_sem)
    local.start()
    barrier = pltpu.get_barrier_semaphore()

    def greet(who):
        pl.semaphore_signal(barrier, inc=1, device_id=who, device_id_type=MESH)

    peers = [(offset, (r, (c + offset) % 16)) for offset in range(1, 16)]
    x_peers = list(ring_x.items())
    across = {offset: device((x + offset) % 4, 1 - core, y, z) for offset in range(4)}
    for who in (*across.values(), *(peer for _, peer in x_peers), *(peer for _, peer in peers)):
        greet(who)

    @pl.when(crossed)
    def _():
        greet(device(z, core, y, x))
        greet(device(z, 1 - core, y, x))

    block_rows, block_cols = block.shape
    slab = start_ref.shape[0]
    width = start_ref.shape[1] // 2
    share = width // STREAMS
    half = share // 2
    mine_cols = pl.ds(pl.multiple_of(core * width, width), width)
    mate_cols = pl.ds(pl.multiple_of((1 - core) * width, width), width)

    lower_end = jnp.full((1, block_cols), interval_ref[0], jnp.float32)
    upper_end = jnp.full((1, block_cols), interval_ref[1], jnp.float32)
    center = 0.5 * (lower_end + upper_end)
    inverse_width = 1.0 / (0.5 * (upper_end - lower_end))

    def prepare(source, which):
        base = which * block_rows
        step = 256

        @pl.loop(0, block_rows // step)
        def _(i):
            at = pl.multiple_of(i * step, step)
            value = source[pl.ds(at, step), :]
            row = lax.broadcasted_iota(jnp.int32, value.shape, 0) + (2 * x * block_rows + base + at)
            col = lax.broadcasted_iota(jnp.int32, value.shape, 1) + c * block_cols
            value = jnp.where(row == col, value - center, value) * inverse_width
            big, small = split(value)
            to = pl.ds(pl.multiple_of(base + at, step), step)
            high[to, :] = big
            low[to, :] = small

    local.wait()
    prepare(block, core)
    start_land[r] = start_ref[:, mine_cols]
    pl.semaphore_wait(barrier, jnp.where(crossed, 24, 22))

    start_copies = []
    for index in range(STREAMS):
        lanes = pl.ds(index * share, share)
        own = start_ref.at[:, pl.ds(pl.multiple_of(core * width + index * share, share), share)]
        theirs = start_ref.at[:, pl.ds(pl.multiple_of((1 - core) * width + index * share, share), share)]
        ways = [(theirs, across[0])]
        for offset in (2, 1, 3):
            ways += [(own, ring_x[offset]), (theirs, across[offset])]
        start_copies.append([
            copies.make(source, start_land.at[r, :, lanes], copies.reserve(1), peer) for source, peer in ways
        ])
    for group in start_copies:
        for copy in group:
            copy.start()
    block_copy = copies.make(block_ref, other, copies.reserve(1), mate)
    block_copy.start()

    places = {"y": y, "z": z}
    rings = {"y": ring_y, "z": ring_z}
    orders = (("z", "y"), ("y", "z"))

    class Stream:
        def __init__(self, index):
            self.base = index * share
            self.at_first = self.at_last = False
            self.all = pl.ds(self.base, share)
            slots = [[copies.reserve(6) for _ in range(2)] for _ in range(2)]
            self.scatters = [[self.scatter(index, u, stage, slots[u][stage]) for stage in range(2)] for u in range(2)]
            slots = [[copies.reserve(4) for _ in range(2)] for _ in range(2)]
            self.gathers = [[self.gather(u, stage, slots[u][stage]) for stage in range(2)] for u in range(2)]
            self.col_scatter = SCATTERS[2](
                copies, copies.reserve(6), x, ring_x, self.col_slice(col_parts), lambda i: land_col.at[index, i]
            )
            self.col_gather = GATHERS[2](copies, copies.reserve(4), x, ring_x, self.col_slice(cols))

        def span(self, colour, side):
            size = half if side is None else half // 2
            return pl.ds(self.base + colour * half + (0 if side is None else side * size), size)

        def col_slice(self, ref):
            def part(t, side):
                return ref.at[t, self.all if side is None else self.span(side, None), :]
            return part

        def plane(self, ref, colour, axis):
            def part(t, side):
                at = self.span(colour, side)
                return ref.at[:, t, at, :] if axis == "z" else ref.at[t, :, at, :]
            return part

        def line(self, ref, colour, axis):
            def part(t, side):
                at = self.span(colour, side)
                return ref.at[y, t, at, :] if axis == "z" else ref.at[t, z, at, :]
            return part

        def scatter(self, index, colour, stage, slot):
            axis = orders[colour][stage]
            part = (self.plane if stage == 0 else self.line)(row_parts, colour, axis)
            landing = land_big if stage == 0 else land_small
            return SCATTERS[stage](copies, slot, places[axis], rings[axis], part, lambda i: landing.at[index, colour, i])

        def gather(self, colour, stage, slot):
            axis = orders[colour][1 - stage]
            part = (self.line if stage == 0 else self.plane)(rows, colour, axis)
            return GATHERS[stage](copies, slot, places[axis], rings[axis], part)

        def multiply(self):
            for q in range(4):
                big, small = split(cols[q, self.all, :])
                vec[:share, q * CHUNK : (q + 1) * CHUNK] = big
                vec[share:, q * CHUNK : (q + 1) * CHUNK] = small

            @pl.loop(0, 8, unroll=4)
            def _(i):
                at = pl.ds(pl.multiple_of(i * 256, 256), 256)
                out = three_pass(vec[...], (high[at, :], low[at, :]), ((1,), (1,)))
                row_parts[i // 2, 2 * (i % 2), self.all, :] = out[:, :CHUNK]
                row_parts[i // 2, 2 * (i % 2) + 1, self.all, :] = out[:, CHUNK:]

        def multiply_turned(self):
            def one(i):
                at = pl.ds(pl.multiple_of(i * 1024, 1024), 1024)
                wide = jnp.concatenate([rows[2 * i + k // 4, k % 4, self.all, :] for k in range(8)], axis=1)
                left = jnp.concatenate(split(wide), axis=0)
                return three_pass(left, (high[at, :], low[at, :]), ((1,), (0,)))

            out = one(0) + one(1)
            for q in range(4):
                col_parts[q, self.all, :] = out[:, q * CHUNK : (q + 1) * CHUNK]

        def to_rows(self):
            self.multiply()
            firsts = [self.scatters[0][0], self.scatters[1][0]]
            seconds = [self.scatters[0][1], self.scatters[1][1]]
            for first in firsts:
                first.start()
            yield
            if firsts[0].relays:
                for first in firsts:
                    first.relay()
                yield
            for first, second in zip(firsts, seconds):
                first.finish()
                second.start()
            yield
            if seconds[0].relays:
                for second in seconds:
                    second.relay()
                yield

        def gather_rows(self, step):
            for colour in range(2):
                self.scatters[colour][1].finish()
                at = self.span(colour, None)
                value = row_parts[y, z, at, :]
                if step > 0:
                    value = 2.0 * value - row_prev[at, :]
                rows[y, z, at, :] = value
                row_prev[at, :] = value
                if step == 1:
                    first_part[at, :] = value
                self.gathers[colour][0].start()
            self.at_first = step >= 1
            yield
            for stage in range(2):
                pair = [self.gathers[0][stage], self.gathers[1][stage]]
                if pair[0].relays:
                    for one in pair:
                        one.forward()
                    yield
                for colour in range(2):
                    pair[colour].finish()
                    if stage == 0:
                        self.gathers[colour][1].start()
                if stage == 0:
                    yield

        def to_cols(self, step):
            self.multiply_turned()
            self.col_scatter.start()
            yield
            if self.col_scatter.relays:
                self.col_scatter.relay()
                yield
            self.col_scatter.finish()
            value = col_parts[x, self.all, :]
            if step != 1:
                value = 2.0 * value - col_prev[self.all, :]
            cols[x, self.all, :] = value
            col_prev[self.all, :] = value
            self.col_gather.start()
            self.at_last = step == 2
            yield
            if self.col_gather.relays:
                self.col_gather.forward()
                yield
            self.col_gather.finish()

        def begin(self):
            lanes = pl.ds(self.base, share)
            for copy in start_copies[self.base // share]:
                copy.wait_recv()
            for q in range(4):
                both = [start_land[2 * q, :, lanes], start_land[2 * q + 1, :, lanes]]
                cols[q, self.all, :] = jnp.concatenate(both, axis=0).T
            col_prev[self.all, :] = cols[x, self.all, :]

        def run(self):
            self.begin()
            for step in range(3):
                yield from self.to_rows()
                yield from self.gather_rows(step)
                yield from self.to_cols(step)
            yield from self.to_rows()
            for colour in range(2):
                self.scatters[colour][1].finish()

    streams = [Stream(index) for index in range(STREAMS)]
    block_copy.wait_recv()
    prepare(other, 1 - core)
    block_copy.wait_send()

    keep = pl.ds(pl.multiple_of(core * slab, slab), slab)
    sums = [TotalSum(copies, (core, x, c), mate, peers, x_peers, buffers) for buffers in sum_buffers]

    def trade(piece, land, target):
        land[1] = piece.T
        copy = copies.make(land.at[1], land.at[0], copies.reserve(1), mate)
        copy.start()
        yield
        copy.wait()
        target[:, mine_cols] = land[1]
        target[:, mate_cols] = land[0]

    def first_chain():
        yield from trade(first_part[...], first_land, slab_ref)
        sums[0].total[...] = contract(slab_ref[:, mine_cols], slab_ref[...], 0, 0)
        yield from sums[0].steps()
        sums[0].result[...] = sums[0].result[...] / count
        yield from factor_steps(2, sums[0].result, before_ref, tile, pend_left, pend_right)

    def last_chain():
        yield from trade(col_prev[...], last_land, slab_ref)
        slab_ref[...] = fine(slab_ref[...], before_ref[...], 1)
        sums[1].total[...] = contract(slab_ref[:, mine_cols], slab_ref[...], 0, 0)
        yield from sums[1].steps()
        sums[1].result[...] = sums[1].result[...] / count
        yield from factor_steps(2, sums[1].result, inverse_ref, tile, pend_left, pend_right)
        basis_ref[...] = fine(slab_ref[keep, :], inverse_ref[...], 1)

    def image_chain():
        image_land[2] = row_parts[y, z].T
        slots = copies.reserve(2)
        same = copies.make(image_land.at[2], image_land.at[0], slots, device(z, core, y, x))
        cross = copies.make(image_land.at[2], image_land.at[1], slots + 1, device(z, 1 - core, y, x))
        cross.start()

        @pl.when(crossed)
        def _():
            same.start()

        yield

        @pl.when(crossed)
        def _():
            same.wait()

        @pl.when(jnp.logical_not(crossed))
        def _():
            image_land[0] = image_land[2]

        cross.wait()
        image_ref[:, mine_cols] = image_land[0]
        image_ref[:, mate_cols] = image_land[1]
        image_ref[...] = fine(image_ref[...], before_ref[...], 1)
        sums[2].total[...] = contract(slab_ref[:, mine_cols], image_ref[...], 0, 0)
        yield from sums[2].steps()

    class Chain:
        def __init__(self, steps):
            self.steps, self.ready, self.ended = steps, False, False

        def advance(self):
            if not self.ended:
                said = next(self.steps, "end")
                self.ready, self.ended = said == WORK, said == "end"

    runs = [Chain(stream.run()) for stream in streams]
    chains, begun = [], 0
    while not all(run.ended for run in runs):
        for index, run in enumerate(runs):
            run.advance()
            if chains and (begun == 1 and chains[0].ready or index == len(runs) - 1):
                chains[0].advance()
                if chains[0].ended:
                    chains.pop(0)
        if begun == 0 and all(stream.at_first for stream in streams):
            chains.append(Chain(first_chain()))
            begun = 1
        if begun == 1 and all(stream.at_last for stream in streams):
            chains.append(Chain(last_chain()))
            begun = 2
    image = Chain(image_chain())
    while chains or not image.ended:
        image.advance()
        for turn in range(PIECES_A_WAIT):
            if chains and (chains[0].ready or turn == 0 or image.ended):
                chains[0].advance()
                if chains[0].ended:
                    chains.pop(0)

    for group in start_copies:
        for copy in group:
            copy.wait_send()
    inverse = inverse_ref[...]
    basis = basis_ref[...]
    projected = fine(fine(inverse, sums[2].result[...] / count, 0), inverse, 1)
    projected_ref[...] = projected
    residual_ref[...] = fine(image_ref[keep, :], inverse, 1) - fine(basis, projected, 0)


def on_device(matrix, start_vectors, interval):
    block_rows, block_cols = matrix.shape
    slab, vectors = start_vectors.shape
    total_rows = slab * lax.axis_size("row") * lax.axis_size("col")
    width = vectors // 2
    share = width // STREAMS
    f32, bf16 = jnp.float32, jnp.bfloat16
    vmem = pl.BlockSpec(memory_space=pltpu.VMEM)
    tall = jax.ShapeDtypeStruct((slab, vectors), f32)
    square = jax.ShapeDtypeStruct((vectors, vectors), f32)
    one_sum = [
        pltpu.VMEM((vectors // 2, vectors), f32),
        pltpu.VMEM((vectors, vectors), f32),
        pltpu.VMEM((16, vectors // 32, vectors), f32),
        pltpu.VMEM((4, vectors // 32, vectors), f32),
    ]
    return pl.pallas_call(
        functools.partial(whole_kernel, total_rows),
        out_shape=(tall, square, tall),
        in_specs=[pl.BlockSpec(memory_space=pltpu.SMEM), pl.BlockSpec(memory_space=pl.ANY), vmem],
        out_specs=(vmem,) * 3,
        scratch_shapes=[
            pltpu.VMEM((block_rows, block_cols), f32),
            pltpu.VMEM((block_rows, block_cols), f32),
            pltpu.VMEM((2 * block_rows, block_cols), bf16),
            pltpu.VMEM((2 * block_rows, block_cols), bf16),
            pltpu.VMEM((4, 4, width, CHUNK), f32),
            pltpu.VMEM((4, 4, width, CHUNK), f32),
            pltpu.VMEM((4, width, CHUNK), f32),
            pltpu.VMEM((4, width, CHUNK), f32),
            pltpu.VMEM((2 * share, block_cols), bf16),
            pltpu.VMEM((STREAMS, 2, 6, 4, share // 4, CHUNK), f32),
            pltpu.VMEM((STREAMS, 2, 3, share // 2, CHUNK), f32),
            pltpu.VMEM((STREAMS, 3, share, CHUNK), f32),
            pltpu.VMEM((width, CHUNK), f32),
            pltpu.VMEM((width, CHUNK), f32),
            pltpu.VMEM((width, CHUNK), f32),
            pltpu.VMEM((8, slab, width), f32),
            pltpu.VMEM((2, CHUNK, width), f32),
            pltpu.VMEM((2, CHUNK, width), f32),
            pltpu.VMEM((3, CHUNK, width), f32),
            pltpu.VMEM((CHUNK, vectors), f32),
            pltpu.VMEM((CHUNK, vectors), f32),
            pltpu.VMEM((vectors, vectors), f32),
            pltpu.VMEM((vectors, vectors), f32),
            *(one_sum * 3),
            pltpu.VMEM((BLOCK + PANEL, 2 * BLOCK), f32),
            pltpu.VMEM((BLOCK, 6 * PANEL), bf16),
            pltpu.VMEM((6 * PANEL, 2 * BLOCK), bf16),
            pltpu.SemaphoreType.DMA((256,)),
            pltpu.SemaphoreType.DMA((256,)),
            pltpu.SemaphoreType.DMA,
        ],
        compiler_params=pltpu.CompilerParams(
            collective_id=0, has_side_effects=True, vmem_limit_bytes=56 * 2**20
        ),
        cost_estimate=pl.CostEstimate(flops=10**10, bytes_accessed=4 * 10**6, transcendentals=0),
    )(interval, matrix, start_vectors)


def solution(mesh):
    return jax.shard_map(
        on_device,
        mesh=mesh,
        in_specs=(P("row", "col"), P(("col", "row"), None), P()),
        out_specs=(P(("col", "row"), None), P(), P(("col", "row"), None)),
        check_vma=False,
    )
```

```python
import functools

import jax
import jax.numpy as jnp
from jax import lax
from jax.experimental import pallas as pl
from jax.experimental.pallas import tpu as pltpu
from jax.sharding import PartitionSpec as P

FILTER_DEG = 3
OUTER = 2
PANEL = 16
BLOCK = 128
WORK = "work"
MESH = pl.DeviceIdType.MESH
CHUNK = 128


def product(left, right, precision=lax.Precision.HIGHEST):
    return jnp.dot(left, right, precision=precision, preferred_element_type=jnp.float32)


def contract(left, right, left_dim, right_dim):
    return lax.dot_general(
        left,
        right,
        (((left_dim,), (right_dim,)), ((), ())),
        precision=lax.Precision.HIGHEST,
        preferred_element_type=jnp.float32,
    )


def lane_columns(rows, first):
    narrow = rows[:, :128]
    lanes = jnp.zeros(narrow.shape, jnp.int32) + first
    return [jnp.take_along_axis(narrow, lanes + j, axis=1) for j in range(PANEL)]


def row_of(value, step):
    return jnp.broadcast_to(value[step : step + 1, :], value.shape)


def three_parts(value):
    high = value.astype(jnp.bfloat16).astype(jnp.float32)
    rest = value - high
    middle = rest.astype(jnp.bfloat16).astype(jnp.float32)
    return high, middle, rest - middle


def factor_panels(tile, pend_left, pend_right, begin, end):
    block = tile.shape[1] // 2
    sub = lax.broadcasted_iota(jnp.int32, (PANEL, 128), 0)
    lane = lax.broadcasted_iota(jnp.int32, (PANEL, block), 1)

    def panel(p, carry):
        first = pl.multiple_of(p * PANEL, PANEL)
        here, after = pl.ds(first, PANEL), pl.ds(pl.multiple_of(first + PANEL, PANEL), PANEL)
        rows = tile[here, :]
        tile[:block, :] -= jnp.dot(pend_left[...], pend_right[...], preferred_element_type=jnp.float32)

        columns = lane_columns(rows, first)
        left, right = rows[:, :block], rows[:, block:]
        inverses = []
        pivots = jnp.ones((PANEL, 128), jnp.float32)
        for s in range(PANEL):
            pivot = row_of(columns[s], s)
            pivots = jnp.where(sub == s, pivot, pivots)
            inverse = 1.0 / pivot
            inverses.append(inverse)
            if s < PANEL - 1:
                ratio = jnp.where(sub > s, columns[s] * inverse, 0.0)
                for j in range(s + 1, PANEL):
                    columns[j] = columns[j] - ratio * row_of(columns[j], s)
                left = left - ratio * row_of(left, s)
                right = right - ratio * row_of(right, s)

        scale = lax.rsqrt(pivots)
        done_left, done_right = left * scale, right * scale
        tile[here, :block] = done_left
        tile[here, block:] = done_right
        a = three_parts(jnp.where(lane >= first + 2 * PANEL, done_left, 0.0))
        pend_left[...] = jnp.concatenate([a[0], a[0], a[1], a[1], a[0], a[2]], axis=0).T.astype(jnp.bfloat16)
        b = three_parts(jnp.concatenate([done_left, done_right], axis=1))
        pend_right[...] = jnp.concatenate([b[0], b[1], b[0], b[1], b[2], b[0]], axis=0).astype(jnp.bfloat16)

        following = tile[after, :]
        others = lane_columns(following, first)
        next_left, next_right = following[:, :block], following[:, block:]
        for s in range(PANEL):
            ratio = others[s] * inverses[s]
            for j in range(s + 1, PANEL):
                others[j] = others[j] - ratio * row_of(columns[j], s)
            next_left = next_left - ratio * row_of(left, s)
            next_right = next_right - ratio * row_of(right, s)
        tile[after, :block] = next_left
        tile[after, block:] = next_right
        return carry

    lax.fori_loop(begin, end, panel, 0)


def factor_steps(pieces, work, inverse_ref, tile, pend_left, pend_right):
    order, block = work.shape[0], BLOCK
    at_row = lax.broadcasted_iota(jnp.int32, (order, order), 0)
    at_col = lax.broadcasted_iota(jnp.int32, (order, order), 1)
    inverse_ref[...] = (at_row == at_col).astype(jnp.float32)
    row = lax.broadcasted_iota(jnp.int32, (block, block), 0)
    col = lax.broadcasted_iota(jnp.int32, (block, block), 1)
    panels = block // PANEL
    for at in range(0, order, block):
        stop = at + block
        tile[:block, :block] = work[at:stop, at:stop]
        tile[:block, block:] = (row == col).astype(jnp.float32)
        tile[block:, :] = jnp.zeros((PANEL, 2 * block), jnp.float32)
        pend_left[...] = jnp.zeros_like(pend_left)
        pend_right[...] = jnp.zeros_like(pend_right)
        for piece in range(pieces):
            factor_panels(tile, pend_left, pend_right, piece * panels // pieces, (piece + 1) * panels // pieces)
            yield WORK
        small = jnp.where(row >= col, tile[:block, block:], 0.0)
        solved = product(small, inverse_ref[at:stop, :stop])
        inverse_ref[at:stop, :stop] = solved
        if stop < order:
            below = contract(work[stop:, at:stop], small, 1, 1)
            work[stop:, stop:] -= contract(below, below, 1, 1)
            inverse_ref[stop:, :stop] -= product(below, solved)
            yield WORK


class Copies:
    def __init__(self, send, recv):
        self.send, self.recv, self.used = send, recv, 0

    def reserve(self, count):
        first = self.used
        self.used += count
        return first

    def make(self, source, target, slot, device):
        return pltpu.make_async_remote_copy(
            src_ref=source,
            dst_ref=target,
            send_sem=self.send.at[slot],
            recv_sem=self.recv.at[slot],
            device_id=device,
            device_id_type=MESH,
        )


class Scatter:
    relays = True

    def __init__(self, copies, slot, place, ring, part, land):
        self.place, self.part, self.land = place, part, land
        left, right = ring[3], ring[1]
        ahead, behind, across = (place + 1) % 4, (place + 3) % 4, (place + 2) % 4
        self.ahead, self.behind = ahead, behind
        plan = (
            (part(across, 0), right),
            (part(across, 1), left),
            (part(ahead, 1), right),
            (part(behind, 0), left),
            (part(ahead, 0), right),
            (part(behind, 1), left),
        )
        self.copies = [
            copies.make(source, land(i), slot + i, device) for i, (source, device) in enumerate(plan)
        ]

    def start(self):
        for copy in self.copies[:4]:
            copy.start()

    def relay(self):
        for first, half, target in ((0, 0, self.ahead), (1, 1, self.behind)):
            self.copies[first].wait_recv()
            mine = self.part(target, half)
            mine[...] += self.land(first)[...]
            self.copies[4 + first].start()

    def finish(self):
        for copy in self.copies[2:]:
            copy.wait_recv()
        for half, terms in ((0, (3, 4)), (1, (2, 5))):
            mine = self.part(self.place, half)
            mine[...] += self.land(terms[0])[...] + self.land(terms[1])[...]
        for copy in self.copies:
            copy.wait_send()


class Gather:
    relays = True

    def __init__(self, copies, slot, place, ring, part):
        left, right = ring[3], ring[1]
        ahead, behind = (place + 1) % 4, (place + 3) % 4
        self.copies = [
            copies.make(part(place, None), part(place, None), slot, right),
            copies.make(part(place, None), part(place, None), slot + 1, left),
            copies.make(part(behind, 0), part(behind, 0), slot + 2, right),
            copies.make(part(ahead, 1), part(ahead, 1), slot + 3, left),
        ]

    def start(self):
        for copy in self.copies[:2]:
            copy.start()

    def forward(self):
        for first in range(2):
            self.copies[first].wait_recv()
            self.copies[2 + first].start()

    def finish(self):
        for copy in self.copies[2:]:
            copy.wait_recv()
        for copy in self.copies:
            copy.wait_send()


class DirectScatter:
    relays = False

    def __init__(self, copies, slot, place, ring, part, land):
        self.mine, self.land = part(place, None), land
        self.copies = [
            copies.make(part((place + offset) % 4, None), land(offset - 1), slot + offset - 1, ring[offset])
            for offset in (2, 1, 3)
        ]

    def start(self):
        for copy in self.copies:
            copy.start()

    def finish(self):
        for copy in self.copies:
            copy.wait_recv()
        self.mine[...] += self.land(0)[...] + (self.land(1)[...] + self.land(2)[...])
        for copy in self.copies:
            copy.wait_send()


class DirectGather:
    relays = False

    def __init__(self, copies, slot, place, ring, part):
        own = part(place, None)
        self.copies = [copies.make(own, own, slot + offset - 1, ring[offset]) for offset in (2, 1, 3)]

    def start(self):
        for copy in self.copies:
            copy.start()

    def finish(self):
        for copy in self.copies:
            copy.wait_recv()
        for copy in self.copies:
            copy.wait_send()


def split(value):
    high = value.astype(jnp.bfloat16)
    return high, (value - high.astype(jnp.float32)).astype(jnp.bfloat16)


def three_pass(left, right, dims):
    def one(a, b):
        return lax.dot_general(a, b, (dims, ((), ())), preferred_element_type=jnp.float32)

    count = left.shape[0] // 2
    both = one(left, right[0])
    return both[:count] + (both[count:] + one(left[:count], right[1]))


def fine(left, right, right_dim):
    return three_pass(jnp.concatenate(split(left), axis=0), split(right), ((1,), (right_dim,)))


def by_factor(left, inverse_ref):
    half = inverse_ref.shape[0] // 2
    first = fine(left[:, :half], inverse_ref[:half, :half], 1)
    return jnp.concatenate([first, fine(left, inverse_ref[half:, :], 1)], axis=1)


class TotalSum:
    def __init__(self, copies, position, mate, peers, x_peers, buffers):
        core, x, c = position
        self.x = x
        self.total, self.result, self.land_plane, self.land_x = buffers
        half = self.total.shape[0]
        size = half // 16

        def rows(ref, first, count):
            return ref.at[pl.ds(pl.multiple_of(first, size), count), :]

        self.own, self.summed = rows(self.total, c * size, size), rows(self.result, core * half + c * size, size)
        self.there, self.along, self.back = [], [], []
        for offset, peer in peers:
            source, target = rows(self.total, (c + offset) % 16 * size, size), self.land_plane.at[offset]
            self.there.append(copies.make(source, target, copies.reserve(1), peer))
            self.back.append(copies.make(self.summed, self.summed, copies.reserve(1), peer))
        for offset, peer in x_peers:
            self.along.append(copies.make(self.land_x.at[0], self.land_x.at[offset], copies.reserve(1), peer))
        whole = rows(self.result, core * half, half)
        self.give = copies.make(whole, whole, copies.reserve(1), mate)

    def steps(self):
        for copy in self.there:
            copy.start()
        yield
        value = self.own[...]
        for offset, copy in enumerate(self.there, 1):
            copy.wait_recv()
            value = value + self.land_plane[offset]
        self.land_x[0] = value
        for copy in self.along:
            copy.start()
        yield
        for copy in self.along:
            copy.wait_recv()
        value = self.land_x[self.x % 4]
        for at in range(1, 4):
            value = value + self.land_x[(self.x + 4 - at) % 4]
        self.summed[...] = value
        for copy in self.back:
            copy.start()
        yield
        for copy in self.back:
            copy.wait_recv()
        self.give.start()
        for copy in (*self.there, *self.along, *self.back):
            copy.wait_send()
        yield
        self.give.wait()


STREAMS = 2
PIECES_A_WAIT = 3
SCATTERS = (Scatter, DirectScatter, DirectScatter)
GATHERS = (DirectGather, Gather, DirectGather)


def whole_kernel(
    count, interval_ref, block_ref, start_ref, basis_ref, projected_ref, residual_ref,
    block, other, high, low, rows, row_parts, cols, col_parts, vec,
    land_big, land_small, land_col, row_prev, col_prev, first_part,
    start_land, first_land, last_land, image_land, slab_ref, image_ref, before_ref, inverse_ref,
    *rest,
):
    sum_buffers = [rest[4 * k : 4 * k + 4] for k in range(3)]
    tile, pend_left, pend_right, send, recv, local_sem = rest[12:]
    r, c = lax.axis_index("row"), lax.axis_index("col")
    core, x, y, z = r % 2, r // 2, c % 4, c // 4
    copies = Copies(send, recv)

    def device(x, core, y, z):
        return (2 * x + core, 4 * z + y)

    mate = device(x, 1 - core, y, z)
    ring_x = {offset: device((x + offset) % 4, core, y, z) for offset in (1, 2, 3)}
    ring_y = {offset: device(x, core, (y + offset) % 4, z) for offset in (1, 2, 3)}
    ring_z = {offset: device(x, core, y, (z + offset) % 4) for offset in (1, 2, 3)}
    crossed = x != z

    local = pltpu.make_async_copy(block_ref, block, local_sem)
    local.start()
    barrier = pltpu.get_barrier_semaphore()

    def greet(who):
        pl.semaphore_signal(barrier, inc=1, device_id=who, device_id_type=MESH)

    peers = [(offset, (r, (c + offset) % 16)) for offset in range(1, 16)]
    x_peers = list(ring_x.items())
    across = {offset: device((x + offset) % 4, 1 - core, y, z) for offset in range(4)}
    for who in (*across.values(), *(peer for _, peer in x_peers), *(peer for _, peer in peers)):
        greet(who)

    @pl.when(crossed)
    def _():
        greet(device(z, core, y, x))
        greet(device(z, 1 - core, y, x))

    block_rows, block_cols = block.shape
    slab = start_ref.shape[0]
    width = start_ref.shape[1] // 2
    share = width // STREAMS
    half = share // 2
    mine_cols = pl.ds(pl.multiple_of(core * width, width), width)
    mate_cols = pl.ds(pl.multiple_of((1 - core) * width, width), width)

    lower_end = jnp.full((1, block_cols), interval_ref[0], jnp.float32)
    upper_end = jnp.full((1, block_cols), interval_ref[1], jnp.float32)
    center = 0.5 * (lower_end + upper_end)
    inverse_width = 1.0 / (0.5 * (upper_end - lower_end))

    def prepare(source, which):
        base = which * block_rows
        step = 256

        @pl.loop(0, block_rows // step)
        def _(i):
            at = pl.multiple_of(i * step, step)
            value = source[pl.ds(at, step), :]
            row = lax.broadcasted_iota(jnp.int32, value.shape, 0) + (2 * x * block_rows + base + at)
            col = lax.broadcasted_iota(jnp.int32, value.shape, 1) + c * block_cols
            value = jnp.where(row == col, value - center, value) * inverse_width
            big, small = split(value)
            to = pl.ds(pl.multiple_of(base + at, step), step)
            high[to, :] = big
            low[to, :] = small

    local.wait()
    prepare(block, core)
    start_land[r] = start_ref[:, mine_cols]
    pl.semaphore_wait(barrier, jnp.where(crossed, 24, 22))

    start_copies = []
    for index in range(STREAMS):
        lanes = pl.ds(index * share, share)
        own = start_ref.at[:, pl.ds(pl.multiple_of(core * width + index * share, share), share)]
        theirs = start_ref.at[:, pl.ds(pl.multiple_of((1 - core) * width + index * share, share), share)]
        ways = [(theirs, across[0])]
        for offset in (2, 1, 3):
            ways += [(own, ring_x[offset]), (theirs, across[offset])]
        start_copies.append([
            copies.make(source, start_land.at[r, :, lanes], copies.reserve(1), peer) for source, peer in ways
        ])
    for group in start_copies:
        for copy in group:
            copy.start()
    block_copy = copies.make(block_ref, other, copies.reserve(1), mate)
    block_copy.start()

    places = {"y": y, "z": z}
    rings = {"y": ring_y, "z": ring_z}
    orders = (("z", "y"), ("y", "z"))

    class Stream:
        def __init__(self, index):
            self.base = index * share
            self.at_first = self.at_last = False
            self.all = pl.ds(self.base, share)
            slots = [[copies.reserve(6) for _ in range(2)] for _ in range(2)]
            self.scatters = [[self.scatter(index, u, stage, slots[u][stage]) for stage in range(2)] for u in range(2)]
            slots = [[copies.reserve(4) for _ in range(2)] for _ in range(2)]
            self.gathers = [[self.gather(u, stage, slots[u][stage]) for stage in range(2)] for u in range(2)]
            self.col_scatter = SCATTERS[2](
                copies, copies.reserve(6), x, ring_x, self.col_slice(col_parts), lambda i: land_col.at[index, i]
            )
            self.col_gather = GATHERS[2](copies, copies.reserve(4), x, ring_x, self.col_slice(cols))

        def span(self, colour, side):
            size = half if side is None else half // 2
            return pl.ds(self.base + colour * half + (0 if side is None else side * size), size)

        def col_slice(self, ref):
            def part(t, side):
                return ref.at[t, self.all if side is None else self.span(side, None), :]
            return part

        def plane(self, ref, colour, axis):
            def part(t, side):
                at = self.span(colour, side)
                return ref.at[:, t, at, :] if axis == "z" else ref.at[t, :, at, :]
            return part

        def line(self, ref, colour, axis):
            def part(t, side):
                at = self.span(colour, side)
                return ref.at[y, t, at, :] if axis == "z" else ref.at[t, z, at, :]
            return part

        def scatter(self, index, colour, stage, slot):
            axis = orders[colour][stage]
            part = (self.plane if stage == 0 else self.line)(row_parts, colour, axis)
            landing = land_big if stage == 0 else land_small
            return SCATTERS[stage](copies, slot, places[axis], rings[axis], part, lambda i: landing.at[index, colour, i])

        def gather(self, colour, stage, slot):
            axis = orders[colour][1 - stage]
            part = (self.line if stage == 0 else self.plane)(rows, colour, axis)
            return GATHERS[stage](copies, slot, places[axis], rings[axis], part)

        def multiply(self):
            for q in range(4):
                big, small = split(cols[q, self.all, :])
                vec[:share, q * CHUNK : (q + 1) * CHUNK] = big
                vec[share:, q * CHUNK : (q + 1) * CHUNK] = small

            @pl.loop(0, 8, unroll=4)
            def _(i):
                at = pl.ds(pl.multiple_of(i * 256, 256), 256)
                out = three_pass(vec[...], (high[at, :], low[at, :]), ((1,), (1,)))
                row_parts[i // 2, 2 * (i % 2), self.all, :] = out[:, :CHUNK]
                row_parts[i // 2, 2 * (i % 2) + 1, self.all, :] = out[:, CHUNK:]

        def multiply_turned(self):
            def one(i):
                at = pl.ds(pl.multiple_of(i * 1024, 1024), 1024)
                wide = jnp.concatenate([rows[2 * i + k // 4, k % 4, self.all, :] for k in range(8)], axis=1)
                left = jnp.concatenate(split(wide), axis=0)
                return three_pass(left, (high[at, :], low[at, :]), ((1,), (0,)))

            out = one(0) + one(1)
            for q in range(4):
                col_parts[q, self.all, :] = out[:, q * CHUNK : (q + 1) * CHUNK]

        def to_rows(self):
            self.multiply()
            firsts = [self.scatters[0][0], self.scatters[1][0]]
            seconds = [self.scatters[0][1], self.scatters[1][1]]
            for first in firsts:
                first.start()
            yield
            if firsts[0].relays:
                for first in firsts:
                    first.relay()
                yield
            for first, second in zip(firsts, seconds):
                first.finish()
                second.start()
            yield
            if seconds[0].relays:
                for second in seconds:
                    second.relay()
                yield

        def gather_rows(self, step):
            for colour in range(2):
                self.scatters[colour][1].finish()
                at = self.span(colour, None)
                value = row_parts[y, z, at, :]
                if step > 0:
                    value = 2.0 * value - row_prev[at, :]
                rows[y, z, at, :] = value
                row_prev[at, :] = value
                if step == 1:
                    first_part[at, :] = value
                self.gathers[colour][0].start()
            self.at_first = step >= 1
            yield
            for stage in range(2):
                pair = [self.gathers[0][stage], self.gathers[1][stage]]
                if pair[0].relays:
                    for one in pair:
                        one.forward()
                    yield
                for colour in range(2):
                    pair[colour].finish()
                    if stage == 0:
                        self.gathers[colour][1].start()
                if stage == 0:
                    yield

        def to_cols(self, step):
            self.multiply_turned()
            self.col_scatter.start()
            yield
            if self.col_scatter.relays:
                self.col_scatter.relay()
                yield
            self.col_scatter.finish()
            value = col_parts[x, self.all, :]
            if step != 1:
                value = 2.0 * value - col_prev[self.all, :]
            cols[x, self.all, :] = value
            col_prev[self.all, :] = value
            self.col_gather.start()
            self.at_last = step == 2
            yield
            if self.col_gather.relays:
                self.col_gather.forward()
                yield
            self.col_gather.finish()

        def begin(self):
            lanes = pl.ds(self.base, share)
            for copy in start_copies[self.base // share]:
                copy.wait_recv()
            for q in range(4):
                both = [start_land[2 * q, :, lanes], start_land[2 * q + 1, :, lanes]]
                cols[q, self.all, :] = jnp.concatenate(both, axis=0).T
            col_prev[self.all, :] = cols[x, self.all, :]

        def run(self):
            self.begin()
            for step in range(3):
                yield from self.to_rows()
                yield from self.gather_rows(step)
                yield from self.to_cols(step)
            yield from self.to_rows()
            for colour in range(2):
                self.scatters[colour][1].finish()

    streams = [Stream(index) for index in range(STREAMS)]
    block_copy.wait_recv()
    prepare(other, 1 - core)
    block_copy.wait_send()

    keep = pl.ds(pl.multiple_of(core * slab, slab), slab)
    sums = [TotalSum(copies, (core, x, c), mate, peers, x_peers, buffers) for buffers in sum_buffers]

    def trade(piece, land, target):
        land[1] = piece.T
        copy = copies.make(land.at[1], land.at[0], copies.reserve(1), mate)
        copy.start()
        yield
        copy.wait()
        target[:, mine_cols] = land[1]
        target[:, mate_cols] = land[0]

    def first_chain():
        yield from trade(first_part[...], first_land, slab_ref)
        sums[0].total[...] = contract(slab_ref[:, mine_cols], slab_ref[...], 0, 0)
        yield from sums[0].steps()
        sums[0].result[...] = sums[0].result[...] / count
        yield from factor_steps(2, sums[0].result, before_ref, tile, pend_left, pend_right)

    def last_chain():
        yield from trade(col_prev[...], last_land, slab_ref)
        slab_ref[...] = by_factor(slab_ref[...], before_ref)
        sums[1].total[...] = contract(slab_ref[:, mine_cols], slab_ref[...], 0, 0)
        yield from sums[1].steps()
        sums[1].result[...] = sums[1].result[...] / count
        yield from factor_steps(2, sums[1].result, inverse_ref, tile, pend_left, pend_right)
        basis_ref[...] = by_factor(slab_ref[keep, :], inverse_ref)

    def image_chain():
        image_land[2] = row_parts[y, z].T
        slots = copies.reserve(2)
        same = copies.make(image_land.at[2], image_land.at[0], slots, device(z, core, y, x))
        cross = copies.make(image_land.at[2], image_land.at[1], slots + 1, device(z, 1 - core, y, x))
        cross.start()

        @pl.when(crossed)
        def _():
            same.start()

        yield

        @pl.when(crossed)
        def _():
            same.wait()

        @pl.when(jnp.logical_not(crossed))
        def _():
            image_land[0] = image_land[2]

        cross.wait()
        image_ref[:, mine_cols] = image_land[0]
        image_ref[:, mate_cols] = image_land[1]
        image_ref[...] = by_factor(image_ref[...], before_ref)
        sums[2].total[...] = contract(slab_ref[:, mine_cols], image_ref[...], 0, 0)
        yield from sums[2].steps()

    class Chain:
        def __init__(self, steps):
            self.steps, self.ready, self.ended = steps, False, False

        def advance(self):
            if not self.ended:
                said = next(self.steps, "end")
                self.ready, self.ended = said == WORK, said == "end"

    runs = [Chain(stream.run()) for stream in streams]
    chains, begun = [], 0
    while not all(run.ended for run in runs):
        for index, run in enumerate(runs):
            run.advance()
            if chains and (begun == 1 and chains[0].ready or index == len(runs) - 1):
                chains[0].advance()
                if chains[0].ended:
                    chains.pop(0)
        if begun == 0 and all(stream.at_first for stream in streams):
            chains.append(Chain(first_chain()))
            begun = 1
        if begun == 1 and all(stream.at_last for stream in streams):
            chains.append(Chain(last_chain()))
            begun = 2
    image = Chain(image_chain())
    while chains or not image.ended:
        image.advance()
        for turn in range(PIECES_A_WAIT):
            if chains and (chains[0].ready or turn == 0 or image.ended):
                chains[0].advance()
                if chains[0].ended:
                    chains.pop(0)

    for group in start_copies:
        for copy in group:
            copy.wait_send()
    inverse = inverse_ref[...]
    basis = basis_ref[...]
    cross = sums[2].result[...] / count
    order = inverse.shape[0] // 2
    upper = fine(inverse[:order, :order], cross[:order, :], 0)
    lower = fine(inverse[order:, :], cross, 0)
    projected = by_factor(jnp.concatenate([upper, lower], axis=0), inverse_ref)
    projected_ref[...] = projected
    residual_ref[...] = by_factor(image_ref[keep, :], inverse_ref) - fine(basis, projected, 0)


def on_device(matrix, start_vectors, interval):
    block_rows, block_cols = matrix.shape
    slab, vectors = start_vectors.shape
    total_rows = slab * lax.axis_size("row") * lax.axis_size("col")
    width = vectors // 2
    share = width // STREAMS
    f32, bf16 = jnp.float32, jnp.bfloat16
    vmem = pl.BlockSpec(memory_space=pltpu.VMEM)
    tall = jax.ShapeDtypeStruct((slab, vectors), f32)
    square = jax.ShapeDtypeStruct((vectors, vectors), f32)
    one_sum = [
        pltpu.VMEM((vectors // 2, vectors), f32),
        pltpu.VMEM((vectors, vectors), f32),
        pltpu.VMEM((16, vectors // 32, vectors), f32),
        pltpu.VMEM((4, vectors // 32, vectors), f32),
    ]
    return pl.pallas_call(
        functools.partial(whole_kernel, total_rows),
        out_shape=(tall, square, tall),
        in_specs=[pl.BlockSpec(memory_space=pltpu.SMEM), pl.BlockSpec(memory_space=pl.ANY), vmem],
        out_specs=(vmem,) * 3,
        scratch_shapes=[
            pltpu.VMEM((block_rows, block_cols), f32),
            pltpu.VMEM((block_rows, block_cols), f32),
            pltpu.VMEM((2 * block_rows, block_cols), bf16),
            pltpu.VMEM((2 * block_rows, block_cols), bf16),
            pltpu.VMEM((4, 4, width, CHUNK), f32),
            pltpu.VMEM((4, 4, width, CHUNK), f32),
            pltpu.VMEM((4, width, CHUNK), f32),
            pltpu.VMEM((4, width, CHUNK), f32),
            pltpu.VMEM((2 * share, block_cols), bf16),
            pltpu.VMEM((STREAMS, 2, 6, 4, share // 4, CHUNK), f32),
            pltpu.VMEM((STREAMS, 2, 3, share // 2, CHUNK), f32),
            pltpu.VMEM((STREAMS, 3, share, CHUNK), f32),
            pltpu.VMEM((width, CHUNK), f32),
            pltpu.VMEM((width, CHUNK), f32),
            pltpu.VMEM((width, CHUNK), f32),
            pltpu.VMEM((8, slab, width), f32),
            pltpu.VMEM((2, CHUNK, width), f32),
            pltpu.VMEM((2, CHUNK, width), f32),
            pltpu.VMEM((3, CHUNK, width), f32),
            pltpu.VMEM((CHUNK, vectors), f32),
            pltpu.VMEM((CHUNK, vectors), f32),
            pltpu.VMEM((vectors, vectors), f32),
            pltpu.VMEM((vectors, vectors), f32),
            *(one_sum * 3),
            pltpu.VMEM((BLOCK + PANEL, 2 * BLOCK), f32),
            pltpu.VMEM((BLOCK, 6 * PANEL), bf16),
            pltpu.VMEM((6 * PANEL, 2 * BLOCK), bf16),
            pltpu.SemaphoreType.DMA((256,)),
            pltpu.SemaphoreType.DMA((256,)),
            pltpu.SemaphoreType.DMA,
        ],
        compiler_params=pltpu.CompilerParams(
            collective_id=0, has_side_effects=True, vmem_limit_bytes=56 * 2**20
        ),
        cost_estimate=pl.CostEstimate(flops=10**10, bytes_accessed=4 * 10**6, transcendentals=0),
    )(interval, matrix, start_vectors)


def solution(mesh):
    return jax.shard_map(
        on_device,
        mesh=mesh,
        in_specs=(P("row", "col"), P(("col", "row"), None), P()),
        out_specs=(P(("col", "row"), None), P(), P(("col", "row"), None)),
        check_vma=False,
    )
```
